32 devices in a mesh: space: 8 (over y, x, core), member: 4 (over z).
Axes of the slice: x: 2, y: 2, z: 4, core: 2. Of those that a mesh axis runs over, the one named last changes fastest.
Arguments:
- latent: bfloat16 [16, 4096, 1024], P('member', 'space'), may hold values from -6 to 6
- w_in: bfloat16 [1024, 1024], replicated, may hold values from -0.1875 to 0.1875
- b_in: float32 [1024], replicated, may hold values from -3 to 3
- w_out: bfloat16 [1024, 96], replicated, may hold values from -0.1875 to 0.1875
- b_out: float32 [96], replicated, may hold values from -3 to 3
- target: float32 [4096, 96], P('space'), may hold values from -6 to 6
- area: float32 [4096], P('space'), may hold values from 0.5 to 40, as said below
- cell_of: int32 [4096], P('space'), may hold values from 0 to 255, as said below
Outputs:
- latent_grad: bfloat16 [16, 4096, 1024], P('member', 'space')
- scores: float32 [2], replicated
The draws below stay inside these ranges and needn't reach their ends.
Inputs may be any that keep to these rules, and one draw needn't show every extreme that they name: `cell_of`: every node lies in one coarse cell; some cells hold no node. Positive area of each node.
All inputs are finite; a program needn't handle non-finite values.
Results may differ from the reference program's by a relative error of at most 0.03.
Values may be sent and summed in bfloat16 or wider, within the bound.
A program may use at most 64 MiB of HBM per device.

```python
import jax
import jax.numpy as jnp
from jax import lax

D = 1024
UNITS = 1024
VARS = 96
NODE_DEV = 512
CELL_DEV = 32
MEMBERS = 16
NODES = 4096
CELLS = 256
N_SPACE = 8


def draw_area(key, part):
    first = jax.random.fold_in(key, 11)
    position = jnp.arange(NODES, dtype=jnp.float32) / NODES
    ramp = jnp.exp(jnp.log(6.0) * position)
    noise = jnp.exp(jax.random.uniform(first, (NODES,), jnp.float32, jnp.log(0.5), jnp.log(2.0)))
    return ramp * noise


def draw_cell_of(key, part):
    first = jax.random.fold_in(key, 21)
    second = jax.random.fold_in(key, 22)
    third = jax.random.fold_in(key, 23)
    dense = CELLS // 8
    used = CELLS - CELLS // 8
    region = jax.random.randint(first, (NODES,), 0, 2, dtype=jnp.int32)
    in_dense = jax.random.randint(second, (NODES,), 0, dense, dtype=jnp.int32)
    in_sparse = jax.random.randint(third, (NODES,), dense, used, dtype=jnp.int32)
    return jnp.where(region == 0, in_dense, in_sparse)


def block_levels(stream_key, extent, pieces, smallest, high):
    level, own = 1.0, jax.random.fold_in(stream_key, 6)
    for dim, blocks in pieces:
        draws = jnp.exp(jax.random.uniform(jax.random.fold_in(own, dim), (blocks,), jnp.float32, smallest / len(pieces), high / len(pieces)))
        level = level * jnp.repeat(draws, extent[dim] // blocks).reshape([-1 if axis == dim else 1 for axis in range(len(extent))])
    return level


def bell_draw(rng, extent, spread, limit, split=(), kind=jnp.bfloat16):
    drawn = spread * jax.random.normal(rng, extent, jnp.float32)
    if split:
        drawn = drawn * block_levels(rng, extent, split, -0.22, 0.18)
    return jnp.clip(drawn, -limit, limit).astype(kind)


def setup_inputs(seed: int = 0) -> dict:
    splits = jax.random.split(jax.random.key(seed), 9)
    latent = bell_draw(splits[0], (MEMBERS, NODES, D), 1.0, 6.0, ((0, 4), (1, 8)))
    w_in = bell_draw(splits[1], (D, UNITS), D ** -0.5, 0.1875)
    b_in = bell_draw(splits[2], (UNITS,), 0.5, 3.0, (), jnp.float32)
    w_out = bell_draw(splits[3], (UNITS, VARS), UNITS ** -0.5, 0.1875)
    b_out = bell_draw(splits[4], (VARS,), 0.5, 3.0, (), jnp.float32)
    target = bell_draw(splits[5], (NODES, VARS), 1.0, 6.0, ((0, 8),), jnp.float32)
    area = draw_area(jax.random.fold_in(splits[8], 71), 0)
    cell_of = draw_cell_of(jax.random.fold_in(splits[8], 71), 0)
    return dict(latent=latent, w_in=w_in, b_in=b_in, w_out=w_out, b_out=b_out, target=target, area=area, cell_of=cell_of)


epsilon = 1e-05
loss_scale = 4096.0

def silu_slope(preact):
    sigma = jax.nn.sigmoid(preact)
    return sigma * (1.0 + preact * (1.0 - sigma))

def energy(own_part, everyone, truths, weight, own_ids):
    members = everyone.shape[0]
    variables = everyone.shape[1]
    to_truth = own_part - truths[None]
    truth_dist = jnp.sqrt(lax.optimization_barrier(jnp.mean(to_truth * to_truth, axis=1)) + epsilon)
    between = own_part[:, None] - everyone[None]
    pair_dist = jnp.sqrt(lax.optimization_barrier(jnp.mean(between * between, axis=2)) + epsilon)
    distinct = (own_ids[:, None] != jnp.arange(members, dtype=jnp.int32)[None]).astype(own_part.dtype)
    pair_weight = distinct[:, :, None] / pair_dist
    node_loss = weight * (lax.optimization_barrier(jnp.sum(truth_dist, axis=0)) / members - lax.optimization_barrier(jnp.sum(distinct[:, :, None] * pair_dist, axis=(0, 1))) / (2.0 * members * (members - 1)))
    gradient = weight * (to_truth / truth_dist[:, None] / (members * variables) - lax.optimization_barrier(jnp.sum(between * pair_weight[:, :, None], axis=1)) / (members * (members - 1) * variables))
    return (node_loss, gradient)

def reference(latent, w_in, b_in, w_out, b_out, target, area, cell_of):
    members, node_total, latent_width = latent.shape
    variables = w_out.shape[1]

    def forward(member_rows):
        preact = jnp.dot(member_rows, w_in, preferred_element_type=jnp.float32) + b_in
        activation = jax.nn.silu(preact).astype(jnp.bfloat16)
        return (jnp.dot(activation, w_out, preferred_element_type=jnp.float32) + b_out).astype(jnp.bfloat16)
    predictions = lax.map(forward, latent)
    pred_float = predictions.astype(jnp.float32)
    blocks = node_total // NODE_DEV
    blocked = pred_float.reshape(members, blocks, NODE_DEV, variables).transpose(1, 0, 3, 2)
    truth_blocks = target.reshape(blocks, NODE_DEV, variables).transpose(0, 2, 1)
    area_blocks = area.reshape(blocks, NODE_DEV)
    member_ids = jnp.arange(members, dtype=jnp.int32)

    def fine_block(inputs):
        own_part, truths, weight = inputs
        return energy(own_part, own_part, truths, weight, member_ids)
    fine_loss, fine_grad = lax.map(fine_block, (blocked, truth_blocks, area_blocks))
    fine_node = lax.optimization_barrier(fine_grad.astype(jnp.bfloat16))
    fine_node = fine_node.transpose(1, 0, 3, 2).reshape(members, node_total, variables)
    cells = CELL_DEV * N_SPACE
    flattened = pred_float.transpose(1, 0, 2).reshape(node_total, members * variables)
    cell_sum = jax.ops.segment_sum(flattened, cell_of, cells)
    counts = jax.ops.segment_sum(jnp.ones((node_total,), jnp.float32), cell_of, cells)
    cell_area = jax.ops.segment_sum(area, cell_of, cells)
    target_sum = jax.ops.segment_sum(target, cell_of, cells)
    divisor = jnp.maximum(counts, 1.0)
    cell_mean = lax.optimization_barrier((cell_sum / divisor[:, None]).astype(jnp.bfloat16))
    cell_mean = cell_mean.astype(jnp.float32).reshape(cells, members, variables).transpose(1, 2, 0)
    cell_target = (target_sum / divisor[:, None]).T
    coarse_loss, coarse_grad = energy(cell_mean, cell_mean, cell_target, cell_area, member_ids)
    per_cell = lax.optimization_barrier((coarse_grad / divisor[None, None, :]).astype(jnp.bfloat16))
    node_coarse = jnp.take(per_cell, cell_of, axis=2).transpose(0, 2, 1)
    upstream = (fine_node.astype(jnp.float32) + node_coarse.astype(jnp.float32)).astype(jnp.bfloat16)
    total_area = jnp.sum(area)
    factor = loss_scale * node_total / total_area

    def backward(inputs):
        member_rows, member_up = inputs
        preact = jnp.dot(member_rows, w_in, preferred_element_type=jnp.float32) + b_in
        hidden_grad = jnp.dot(member_up, w_out.T, preferred_element_type=jnp.float32)
        preact_grad = (hidden_grad * silu_slope(preact)).astype(jnp.bfloat16)
        return (jnp.dot(preact_grad, w_in.T, preferred_element_type=jnp.float32) * factor).astype(jnp.bfloat16)
    latent_grad = lax.map(backward, (latent, upstream))
    scores = jnp.stack([jnp.sum(fine_loss), jnp.sum(coarse_loss)]) / total_area
    return (latent_grad, scores)
```

```python
import functools

import jax
import jax.numpy as jnp
from jax import lax
from jax.experimental import pallas as pl
from jax.experimental.pallas import tpu as pltpu
from jax.sharding import PartitionSpec as P

CELL_DEV = 32
COLS = 512
LANES = 128

epsilon = 1e-05
loss_scale = 4096.0
bf16, f32 = jnp.bfloat16, jnp.float32
MESH = pl.DeviceIdType.MESH


def in_hbm(value):
    return pltpu.with_memory_space_constraint(value, pltpu.HBM)


def dot_t(a, b):
    return lax.dot_general(a, b, (((1,), (1,)), ((), ())), preferred_element_type=f32)


def halves(value):
    high = value.astype(bf16).astype(f32)
    return high, value - high


def exchange(spaces, places, scaling, latent, w_in, b_in, w_out, b_out, target, area, cell_of,
             early, pg_out, turned, stats_out,
             lat_buf, w_buf, slope_buf, act, psend, precv, p32, grad, gsend, grecv,
             hot, csum, csend, crecv, mrecv, dsend, drecv, pieces, up_buf, lmem, lspace,
             load_sem, ps_sem, pr_sem, gs_sem, gr_sem, cs_sem, cr_sem,
             ms_sem, mr_sem, ds_sem, dr_sem, ls_sem, lr_sem, ts_sem, tr_sem):
    ms = lax.axis_index("space")
    mm = lax.axis_index("member")
    locals_, quarter, width = lat_buf.shape[1:]
    units = w_buf.shape[1]
    variables = w_out.shape[0]
    members = locals_ * places
    cells = CELL_DEV * spaces
    pair_scale = 1.0 / (members * (members - 1))

    def member_peer(o):
        return lax.rem(mm + o, places)

    def space_peer(o):
        return lax.rem(ms + o, spaces)

    def to_member(src, dst, ss, rs, o):
        peer = member_peer(o)
        return pltpu.make_async_remote_copy(
            src_ref=src(peer), dst_ref=dst.at[mm], send_sem=ss.at[peer], recv_sem=rs.at[mm],
            device_id={"member": peer}, device_id_type=MESH)

    def from_member(dst, ss, rs, o):
        peer = member_peer(o)
        return pltpu.make_async_remote_copy(
            src_ref=dst.at[peer], dst_ref=dst.at[peer], send_sem=ss.at[peer], recv_sem=rs.at[peer],
            device_id={"member": peer}, device_id_type=MESH)

    def to_space(src, dst, ss, rs, o):
        peer = space_peer(o)
        return pltpu.make_async_remote_copy(
            src_ref=src(peer), dst_ref=dst.at[ms], send_sem=ss.at[peer], recv_sem=rs.at[ms],
            device_id={"space": peer}, device_id_type=MESH)

    def from_space(dst, ss, rs, o):
        peer = space_peer(o)
        return pltpu.make_async_remote_copy(
            src_ref=dst.at[peer], dst_ref=dst.at[peer], send_sem=ss.at[peer], recv_sem=rs.at[peer],
            device_id={"space": peer}, device_id_type=MESH)

    def nodes_of(q):
        return pl.ds(pl.multiple_of(q * quarter, quarter), quarter)

    def load_chunk(i):
        q = lax.rem(mm + 1 + i, places)
        return pltpu.make_async_copy(latent.at[:, nodes_of(q), :], lat_buf.at[i], load_sem.at[i])

    w_copy = pltpu.make_async_copy(w_in, w_buf, load_sem.at[places])
    w_copy.start()
    for i in range(places):
        load_chunk(i).start()
    barrier = pltpu.get_barrier_semaphore()
    for o in range(1, places):
        pl.semaphore_signal(barrier, inc=1, device_id={"member": member_peer(o)}, device_id_type=MESH)
    for o in range(1, spaces):
        pl.semaphore_signal(barrier, inc=1, device_id={"space": space_peer(o)}, device_id_type=MESH)

    match = lax.broadcasted_iota(jnp.int32, (cells, cell_of.shape[1]), 0) == cell_of[...]
    ones = jnp.where(match, 1.0, 0.0)
    hot[...] = ones.astype(bf16)
    counts = halves(jnp.sum(ones, axis=1, keepdims=True))
    areas = halves(jnp.sum(jnp.where(match, area[...], 0.0), axis=1, keepdims=True))
    whole = halves(jnp.sum(area[...], axis=1, keepdims=True))
    csum[...] = jnp.zeros_like(csum)
    t_high, t_low = halves(target[...])
    csum[locals_, :, :variables] = dot_t(hot[...], t_high.astype(bf16)) + dot_t(hot[...], t_low.astype(bf16))
    lane = lax.broadcasted_iota(jnp.int32, (cells, LANES), 1)
    meta = csum[locals_]
    for n, value in enumerate(counts + areas + whole):
        meta = jnp.where(lane == variables + n, value, meta)
    csum[locals_] = meta

    w_copy.wait()

    def forward(i, carry):
        q = lax.rem(mm + 1 + i, places)
        load_chunk(i).wait()

        def columns(n, inner):
            at = pl.ds(pl.multiple_of(n * COLS, COLS), COLS)
            rows = lat_buf[i].reshape(locals_ * quarter, width)
            x = jnp.dot(rows, w_buf[:, at], preferred_element_type=f32) + b_in[:, at]
            s = 0.5 * jnp.tanh(0.5 * x) + 0.5
            a = x * s
            act[:, at] = a.astype(bf16)
            slope_buf[i, :, at] = (s + a * (1.0 - s)).astype(bf16)
            return inner

        lax.fori_loop(0, units // COLS, columns, 0)
        pred = dot_t(act[...], w_out[...]) + b_out[...]
        rounded = pred.astype(bf16)
        for j in range(locals_):
            block = rounded[j * quarter:(j + 1) * quarter]
            psend[q, j] = block.astype(f32).T.astype(bf16)
            csum[j, :, :variables] += jnp.dot(hot[:, nodes_of(q)], block, preferred_element_type=f32)
        return carry

    def forward_send(i, carry):
        forward(i, carry)

        @pl.when(i == 0)
        def _():
            pl.semaphore_wait(barrier, places + spaces - 2)

        to_member(lambda peer: psend.at[peer], precv, ps_sem, pr_sem, i + 1).start()
        return carry

    lax.fori_loop(0, places - 1, forward_send, 0)
    forward(places - 1, 0)

    for s in range(spaces):
        csend[s] = csum[:, s * CELL_DEV:(s + 1) * CELL_DEV, :].astype(bf16)
    for o in range(1, spaces):
        to_space(lambda peer: csend.at[peer], crecv, cs_sem, cr_sem, o).start()

    def turn(n, carry):
        at = pl.ds(pl.multiple_of(n * COLS, COLS), COLS)
        turned[:, at] = w_buf[at, :].T
        return carry

    lax.fori_loop(0, width // COLS, turn, 0)

    precv[mm] = psend[mm]
    truths = target[:, nodes_of(mm)]
    weight = area[:, nodes_of(mm)]
    for o in range(1, places):
        from_member(precv, ps_sem, pr_sem, o).wait_recv()

    def truth_step(m, total):
        p = precv[lax.div(m, locals_), lax.rem(m, locals_)].astype(f32)
        p32[m] = p
        d = p - truths
        sq = jnp.sum(d * d, axis=0, keepdims=True) * (1.0 / variables) + epsilon
        r = lax.rsqrt(sq)
        grad[m] = d * (r * (1.0 / members))
        return total + sq * r

    def pair_step(m, total):
        pm = p32[m]
        factors = []
        for r in range(1, members // 2 + 1):
            share = 0.5 if 2 * r == members else 1.0
            d = pm - p32[lax.rem(m + r, members)]
            sq = jnp.sum(d * d, axis=0, keepdims=True) * (1.0 / variables) + epsilon
            inv = lax.rsqrt(sq)
            total = total + share * (sq * inv)
            factors.append(inv * (share * pair_scale))
        mine = grad[m]
        for r in range(1, members // 2 + 1):
            k = lax.rem(m + r, members)
            part = (pm - p32[k]) * factors[r - 1]
            mine = mine - part
            grad[k] = grad[k] + part
        grad[m] = mine
        return total

    zero = jnp.zeros((1, quarter), f32)
    truth_total = lax.fori_loop(0, members, truth_step, zero)
    pair_total = lax.fori_loop(0, members // 2, pair_step, zero)

    crecv[ms] = csend[ms]
    for o in range(1, spaces):
        from_space(crecv, cs_sem, cr_sem, o).wait_recv()

    total = crecv[0].astype(f32)
    for s in range(1, spaces):
        total = total + crecv[s].astype(f32)
    meta = total[locals_]
    cell_count = meta[:, variables:variables + 1] + meta[:, variables + 1:variables + 2]
    cell_area = meta[:, variables + 2:variables + 3] + meta[:, variables + 3:variables + 4]
    all_area = meta[0:1, variables + 4:variables + 5] + meta[0:1, variables + 5:variables + 6]
    divisor = jnp.maximum(cell_count, 1.0)
    means = (total[:locals_] / divisor[None]).astype(bf16)
    mrecv[mm] = means
    for o in range(1, places):
        to_member(lambda peer: mrecv.at[mm], mrecv, ms_sem, mr_sem, o).start()

    pair_total = lax.fori_loop(members // 2, members, pair_step, pair_total)
    fine_loss = weight * (truth_total * (1.0 / members) - pair_total * pair_scale)
    scale = weight * (1.0 / variables)

    def send_grads(o):
        peer = member_peer(o)
        for j in range(locals_):
            gsend[peer, j] = (grad[peer * locals_ + j] * scale).astype(bf16)
        to_member(lambda p: gsend.at[p], grecv, gs_sem, gr_sem, o).start()

    send_grads(1)
    for j in range(locals_):
        grecv[mm, j] = (grad[mm * locals_ + j] * scale).astype(bf16)

    for o in range(1, places):
        from_member(mrecv, ms_sem, mr_sem, o).wait_recv()
    rows = locals_ * CELL_DEV
    own = means.astype(f32).reshape(rows, LANES)
    cell_lane = lax.broadcasted_iota(jnp.int32, (CELL_DEV, LANES), 1)
    cell_target = jnp.where(cell_lane < variables, meta / divisor, 0.0)

    def repeat(value):
        return jnp.concatenate([value] * locals_, axis=0)

    d = own - repeat(cell_target)
    sq = jnp.sum(d * d, axis=1, keepdims=True) * (1.0 / variables) + epsilon
    inv = lax.rsqrt(sq)
    coarse = d * (inv * (1.0 / members))
    coarse_dist = sq * inv * (1.0 / members)
    for o in range(places):
        peer = member_peer(o)
        for r in range(locals_):
            if o == 0 and r == 0:
                continue
            other = jnp.concatenate([mrecv[peer, (j + r) % locals_] for j in range(locals_)], axis=0)
            d = own - other.astype(f32)
            sq = jnp.sum(d * d, axis=1, keepdims=True) * (1.0 / variables) + epsilon
            inv = lax.rsqrt(sq)
            coarse = coarse - d * (inv * pair_scale)
            coarse_dist = coarse_dist - sq * inv * (0.5 * pair_scale)
    cell_weight = repeat(cell_area)
    per_cell = (coarse * (cell_weight * (1.0 / variables)) / repeat(divisor)).astype(bf16)
    dsend[...] = per_cell.reshape(locals_, CELL_DEV, LANES)
    for o in range(1, spaces):
        to_space(lambda peer: dsend, drecv, ds_sem, dr_sem, o).start()
    drecv[ms] = per_cell.reshape(locals_, CELL_DEV, LANES)
    coarse_loss = jnp.sum(cell_weight * coarse_dist, axis=0, keepdims=True)

    row = lax.broadcasted_iota(jnp.int32, (8, LANES), 0)
    lmem[mm] = jnp.where(row == 0, jnp.sum(fine_loss, axis=1, keepdims=True), coarse_loss)
    for o in range(1, places):
        to_member(lambda peer: lmem.at[mm], lmem, ls_sem, lr_sem, o).start()
    for o in range(2, places):
        send_grads(o)

    for o in range(1, spaces):
        from_space(drecv, ds_sem, dr_sem, o).wait_recv()
    for j in range(locals_):
        pieces[j] = drecv[:, j].reshape(cells, LANES).astype(f32).T[:variables].astype(bf16)
    factor = scaling / all_area

    def upstream(i):
        q = lax.rem(mm + 1 + i, places)
        for j in range(locals_):
            coarse_part = jnp.dot(pieces[j], hot[:, nodes_of(q)], preferred_element_type=f32)
            both = grecv[q, j].astype(f32) + coarse_part
            up_buf[j * quarter:(j + 1) * quarter, :] = both.T.astype(bf16)

    def hidden_to(pg, i):
        def hidden(n, carry):
            at = pl.ds(pl.multiple_of(n * COLS, COLS), COLS)
            h = jnp.dot(up_buf[...], w_out[:, at], preferred_element_type=f32)
            pg[:, at] = (h * slope_buf[i, :, at].astype(f32)).astype(bf16)
            return carry

        lax.fori_loop(0, units // COLS, hidden, 0)

    def finish(i):
        upstream(i)
        hidden_to(act, i)

        def outputs(n, carry):
            at = pl.ds(pl.multiple_of(n * COLS, COLS), COLS)
            g = jnp.dot(act[...], turned[:, at], preferred_element_type=f32)
            early[i - 1, :, :, at] = (g * factor).astype(bf16).reshape(locals_, quarter, COLS)
            return carry

        lax.fori_loop(0, width // COLS, outputs, 0)

    finish(places - 1)
    for o in range(1, places):
        from_member(lmem, ls_sem, lr_sem, o).wait_recv()
    loss = lmem[0]
    for m in range(1, places):
        loss = loss + lmem[m]
    lspace[ms] = loss
    for o in range(1, spaces):
        to_space(lambda peer: lspace.at[ms], lspace, ts_sem, tr_sem, o).start()

    def arrived(n, carry):
        i = places - 2 - n
        from_member(grecv, gs_sem, gr_sem, i + 1).wait_recv()
        finish(i)
        return carry

    lax.fori_loop(0, places - 2, arrived, 0)
    from_member(grecv, gs_sem, gr_sem, 1).wait_recv()
    upstream(0)
    hidden_to(pg_out, 0)

    for o in range(1, spaces):
        from_space(lspace, ts_sem, tr_sem, o).wait_recv()
    loss = lspace[0]
    for s in range(1, spaces):
        loss = loss + lspace[s]
    stats_out[...] = jnp.where(row == 2, all_area, loss)

    for o in range(1, places):
        to_member(lambda peer: psend.at[peer], precv, ps_sem, pr_sem, o).wait_send()
        to_member(lambda peer: mrecv.at[mm], mrecv, ms_sem, mr_sem, o).wait_send()
        to_member(lambda peer: gsend.at[peer], grecv, gs_sem, gr_sem, o).wait_send()
        to_member(lambda peer: lmem.at[mm], lmem, ls_sem, lr_sem, o).wait_send()
    for o in range(1, spaces):
        to_space(lambda peer: csend.at[peer], crecv, cs_sem, cr_sem, o).wait_send()
        to_space(lambda peer: dsend, drecv, ds_sem, dr_sem, o).wait_send()
        to_space(lambda peer: lspace.at[ms], lspace, ts_sem, tr_sem, o).wait_send()


def backward(places, scaling, early, pg, turned, stats, latent_grad, scores, last, store_sem):
    locals_, quarter, width = last.shape
    mm = lax.axis_index("member")

    def nodes_of(i):
        q = lax.rem(mm + 1 + i, places)
        return pl.ds(pl.multiple_of(q * quarter, quarter), quarter)

    def store(i):
        return pltpu.make_async_copy(early.at[i - 1], latent_grad.at[:, nodes_of(i), :], store_sem.at[i - 1])

    def store_last(n):
        at = pl.ds(pl.multiple_of(n * COLS, COLS), COLS)
        return pltpu.make_async_copy(
            last.at[:, :, at], latent_grad.at[:, nodes_of(0), at], store_sem.at[places - 1 + n])

    for i in range(1, places):
        store(i).start()
    all_area = stats[2:3, 0:1]
    factor = scaling / all_area

    def outputs(n, carry):
        at = pl.ds(pl.multiple_of(n * COLS, COLS), COLS)
        g = jnp.dot(pg[...], turned[:, at], preferred_element_type=f32)
        last[:, :, at] = (g * factor).astype(bf16).reshape(locals_, quarter, COLS)
        store_last(n).start()
        return carry

    lax.fori_loop(0, width // COLS, outputs, 0)
    both = stats[...] / all_area
    scores[0] = both[0, 0]
    scores[1] = both[1, 0]
    for i in range(1, places):
        store(i).wait()
    for n in range(width // COLS):
        store_last(n).wait()


def solution(mesh):
    spaces, places = mesh.shape["space"], mesh.shape["member"]

    def shards(latent, w_in, b_in, w_out, b_out, target, area, cell_of):
        locals_, nodes, width = latent.shape
        units, variables = w_out.shape
        quarter = nodes // places
        cells = CELL_DEV * spaces
        members = locals_ * places
        anywhere = pl.BlockSpec(memory_space=pl.ANY)
        inside = pl.BlockSpec(memory_space=pltpu.VMEM)
        by_member = [pltpu.SemaphoreType.DMA((places,))]
        by_space = [pltpu.SemaphoreType.DMA((spaces,))]
        rows = locals_ * quarter
        scaling = loss_scale * (nodes * spaces)
        early, pg, turned, stats = pl.pallas_call(
            functools.partial(exchange, spaces, places, scaling),
            out_shape=(
                pltpu.VMEM((places - 1, locals_, quarter, width), bf16),
                pltpu.VMEM((rows, units), bf16),
                pltpu.VMEM((units, width), bf16),
                pltpu.VMEM((8, LANES), f32),
            ),
            in_specs=[anywhere, anywhere] + [inside] * 6,
            out_specs=(inside, inside, inside, inside),
            scratch_shapes=[
                pltpu.VMEM((places, locals_, quarter, width), bf16),
                pltpu.VMEM((width, units), bf16),
                pltpu.VMEM((places, rows, units), bf16),
                pltpu.VMEM((rows, units), bf16),
                pltpu.VMEM((places, locals_, variables, quarter), bf16),
                pltpu.VMEM((places, locals_, variables, quarter), bf16),
                pltpu.VMEM((members, variables, quarter), f32),
                pltpu.VMEM((members, variables, quarter), f32),
                pltpu.VMEM((places, locals_, variables, quarter), bf16),
                pltpu.VMEM((places, locals_, variables, quarter), bf16),
                pltpu.VMEM((cells, nodes), bf16),
                pltpu.VMEM((locals_ + 1, cells, LANES), f32),
                pltpu.VMEM((spaces, locals_ + 1, CELL_DEV, LANES), bf16),
                pltpu.VMEM((spaces, locals_ + 1, CELL_DEV, LANES), bf16),
                pltpu.VMEM((places, locals_, CELL_DEV, LANES), bf16),
                pltpu.VMEM((locals_, CELL_DEV, LANES), bf16),
                pltpu.VMEM((spaces, locals_, CELL_DEV, LANES), bf16),
                pltpu.VMEM((locals_, variables, cells), bf16),
                pltpu.VMEM((rows, variables), bf16),
                pltpu.VMEM((places, 8, LANES), f32),
                pltpu.VMEM((spaces, 8, LANES), f32),
                pltpu.SemaphoreType.DMA((places + 1,)),
            ]
            + by_member * 4
            + by_space * 2
            + by_member * 2
            + by_space * 2
            + by_member * 2
            + by_space * 2,
            compiler_params=pltpu.CompilerParams(
                collective_id=0, has_side_effects=True, vmem_limit_bytes=36 * 2**20
            ),
            name="exchange",
        )(in_hbm(latent), in_hbm(w_in), b_in[None], w_out.T, b_out[None], target.T, area[None], cell_of[None])

        latent_grad, scores = pl.pallas_call(
            functools.partial(backward, places, scaling),
            out_shape=(
                jax.ShapeDtypeStruct((locals_, nodes, width), bf16),
                jax.ShapeDtypeStruct((2,), f32),
            ),
            in_specs=[inside] * 4,
            out_specs=(anywhere, pl.BlockSpec(memory_space=pltpu.SMEM)),
            scratch_shapes=[
                pltpu.VMEM((locals_, quarter, width), bf16),
                pltpu.SemaphoreType.DMA((places - 1 + width // COLS,)),
            ],
            compiler_params=pltpu.CompilerParams(vmem_limit_bytes=16 * 2**20),
            name="backward",
        )(early, pg, turned, stats)
        return latent_grad, scores

    in_specs = (
        P("member", "space", None),
        P(),
        P(),
        P(),
        P(),
        P("space", None),
        P("space"),
        P("space"),
    )
    out_specs = (P("member", "space", None), P())
    return jax.shard_map(shards, mesh=mesh, in_specs=in_specs, out_specs=out_specs, check_vma=False)
```

```python
import functools

import jax
import jax.numpy as jnp
from jax import lax
from jax.experimental import pallas as pl
from jax.experimental.pallas import tpu as pltpu
from jax.sharding import PartitionSpec as P

CELL_DEV = 32
COLS = 512
LANES = 128

epsilon = 1e-05
loss_scale = 4096.0
bf16, f32 = jnp.bfloat16, jnp.float32
MESH = pl.DeviceIdType.MESH


def in_hbm(value):
    return pltpu.with_memory_space_constraint(value, pltpu.HBM)


def dot_t(a, b):
    return lax.dot_general(a, b, (((1,), (1,)), ((), ())), preferred_element_type=f32)


def halves(value):
    high = value.astype(bf16).astype(f32)
    return high, value - high


def exchange(spaces, places, scaling, latent, w_in, b_in_far, w_out_far, b_out_far, target_far, area_far,
             cell_of_far,
             early, pg_out, turned, stats_out,
             b_in, w_out, b_out, target, area, cell_of, lat_buf, w_buf, slope_buf, act, psend, precv, p32, grad, gsend, grecv,
             hot, turned_hot, csum, csend, crecv, mrecv, dsend, drecv, pieces, up_buf, lmem, lspace,
             load_sem, small_sem, ps_sem, pr_sem, gs_sem, gr_sem, cs_sem, cr_sem,
             ms_sem, mr_sem, ds_sem, dr_sem, ls_sem, lr_sem, ts_sem, tr_sem):
    ms = lax.axis_index("space")
    mm = lax.axis_index("member")
    locals_, quarter, width = lat_buf.shape[1:]
    units = w_buf.shape[1]
    variables = w_out.shape[0]
    members = locals_ * places
    cells = CELL_DEV * spaces
    pair_scale = 1.0 / (members * (members - 1))

    def member_peer(o):
        return lax.rem(mm + o, places)

    def space_peer(o):
        return lax.rem(ms + o, spaces)

    def to_member(src, dst, ss, rs, o):
        peer = member_peer(o)
        return pltpu.make_async_remote_copy(
            src_ref=src(peer), dst_ref=dst.at[mm], send_sem=ss.at[peer], recv_sem=rs.at[mm],
            device_id={"member": peer}, device_id_type=MESH)

    def from_member(dst, ss, rs, o):
        peer = member_peer(o)
        return pltpu.make_async_remote_copy(
            src_ref=dst.at[peer], dst_ref=dst.at[peer], send_sem=ss.at[peer], recv_sem=rs.at[peer],
            device_id={"member": peer}, device_id_type=MESH)

    def to_space(src, dst, ss, rs, o):
        peer = space_peer(o)
        return pltpu.make_async_remote_copy(
            src_ref=src(peer), dst_ref=dst.at[ms], send_sem=ss.at[peer], recv_sem=rs.at[ms],
            device_id={"space": peer}, device_id_type=MESH)

    def from_space(dst, ss, rs, o):
        peer = space_peer(o)
        return pltpu.make_async_remote_copy(
            src_ref=dst.at[peer], dst_ref=dst.at[peer], send_sem=ss.at[peer], recv_sem=rs.at[peer],
            device_id={"space": peer}, device_id_type=MESH)

    def nodes_of(q):
        return pl.ds(pl.multiple_of(q * quarter, quarter), quarter)

    def load_chunk(i):
        q = lax.rem(mm + 1 + i, places)
        return pltpu.make_async_copy(latent.at[:, nodes_of(q), :], lat_buf.at[i], load_sem.at[i])

    w_copy = pltpu.make_async_copy(w_in, w_buf, load_sem.at[places])
    small = [
        pltpu.make_async_copy(src, dst, small_sem.at[n])
        for n, (src, dst) in enumerate((
            (cell_of_far, cell_of), (area_far, area), (target_far, target),
            (b_in_far, b_in), (w_out_far, w_out), (b_out_far, b_out)))
    ]
    w_copy.start()
    load_chunk(0).start()
    for copy in small:
        copy.start()
    for i in range(1, places):
        load_chunk(i).start()
    barrier = pltpu.get_barrier_semaphore()
    for o in range(1, places):
        pl.semaphore_signal(barrier, inc=1, device_id={"member": member_peer(o)}, device_id_type=MESH)
    for o in range(1, spaces):
        pl.semaphore_signal(barrier, inc=1, device_id={"space": space_peer(o)}, device_id_type=MESH)

    for copy in small[:3]:
        copy.wait()
    match = lax.broadcasted_iota(jnp.int32, (cells, cell_of.shape[1]), 0) == cell_of[...]
    ones = jnp.where(match, 1.0, 0.0)
    hot[...] = ones.astype(bf16)
    counts = halves(jnp.sum(ones, axis=1, keepdims=True))
    areas = halves(jnp.sum(jnp.where(match, area[...], 0.0), axis=1, keepdims=True))
    whole = halves(jnp.sum(area[...], axis=1, keepdims=True))
    csum[...] = jnp.zeros_like(csum)
    t_high, t_low = halves(target[...])
    csum[locals_, :, :variables] = dot_t(hot[...], t_high.astype(bf16)) + dot_t(hot[...], t_low.astype(bf16))
    lane = lax.broadcasted_iota(jnp.int32, (cells, LANES), 1)
    meta = csum[locals_]
    for n, value in enumerate(counts + areas + whole):
        meta = jnp.where(lane == variables + n, value, meta)
    csum[locals_] = meta

    for copy in small[3:]:
        copy.wait()
    w_copy.wait()

    def forward(i, carry):
        q = lax.rem(mm + 1 + i, places)
        load_chunk(i).wait()

        rows = lat_buf[i].reshape(locals_ * quarter, width)
        x = jnp.dot(rows, w_buf[...], preferred_element_type=f32) + b_in[...]
        s = 0.5 * jnp.tanh(0.5 * x) + 0.5
        a = x * s
        act[...] = a.astype(bf16)
        slope_buf[i] = (s + a * (1.0 - s)).astype(bf16)
        pred = dot_t(act[...], w_out[...]) + b_out[...]
        rounded = pred.astype(bf16)
        for j in range(locals_):
            block = rounded[j * quarter:(j + 1) * quarter]
            psend[q, j] = block.astype(f32).T.astype(bf16)
            csum[j, :, :variables] += jnp.dot(hot[:, nodes_of(q)], block, preferred_element_type=f32)
        return carry

    def forward_send(i, carry):
        forward(i, carry)

        @pl.when(i == 0)
        def _():
            pl.semaphore_wait(barrier, places + spaces - 2)

        to_member(lambda peer: psend.at[peer], precv, ps_sem, pr_sem, i + 1).start()
        return carry

    lax.fori_loop(0, places - 1, forward_send, 0)
    forward(places - 1, 0)

    for s in range(spaces):
        csend[s] = csum[:, s * CELL_DEV:(s + 1) * CELL_DEV, :].astype(bf16)
    for o in range(1, spaces):
        to_space(lambda peer: csend.at[peer], crecv, cs_sem, cr_sem, o).start()

    def turn(n, carry):
        at = pl.ds(pl.multiple_of(n * COLS, COLS), COLS)
        turned[:, at] = w_buf[at, :].T
        return carry

    lax.fori_loop(0, width // COLS, turn, 0)
    for q in range(places):
        at = slice(q * quarter, (q + 1) * quarter)
        turned_hot[at, :] = hot[:, at].astype(f32).T.astype(bf16)

    crecv[ms] = csend[ms]
    for o in range(1, spaces):
        from_space(crecv, cs_sem, cr_sem, o).wait_recv()

    total = crecv[0].astype(f32)
    for s in range(1, spaces):
        total = total + crecv[s].astype(f32)
    meta = total[locals_]
    cell_count = meta[:, variables:variables + 1] + meta[:, variables + 1:variables + 2]
    cell_area = meta[:, variables + 2:variables + 3] + meta[:, variables + 3:variables + 4]
    all_area = meta[0:1, variables + 4:variables + 5] + meta[0:1, variables + 5:variables + 6]
    divisor = jnp.maximum(cell_count, 1.0)
    means = (total[:locals_] / divisor[None]).astype(bf16)
    mrecv[mm] = means
    for o in range(1, places):
        to_member(lambda peer: mrecv.at[mm], mrecv, ms_sem, mr_sem, o).start()

    precv[mm] = psend[mm]
    truths = target[:, nodes_of(mm)]
    weight = area[:, nodes_of(mm)]
    for o in range(1, places):
        from_member(precv, ps_sem, pr_sem, o).wait_recv()

    def truth_step(m, total):
        p = precv[lax.div(m, locals_), lax.rem(m, locals_)].astype(f32)
        p32[m] = p
        d = p - truths
        sq = jnp.sum(d * d, axis=0, keepdims=True) * (1.0 / variables) + epsilon
        r = lax.rsqrt(sq)
        grad[m] = d * (r * (1.0 / members))
        return total + sq * r

    def pair_step(m, total):
        pm = p32[m]
        factors = []
        for r in range(1, members // 2 + 1):
            share = 0.5 if 2 * r == members else 1.0
            d = pm - p32[lax.rem(m + r, members)]
            sq = jnp.sum(d * d, axis=0, keepdims=True) * (1.0 / variables) + epsilon
            inv = lax.rsqrt(sq)
            total = total + share * (sq * inv)
            factors.append(inv * (share * pair_scale))
        mine = grad[m]
        for r in range(1, members // 2 + 1):
            k = lax.rem(m + r, members)
            part = (pm - p32[k]) * factors[r - 1]
            mine = mine - part
            grad[k] = grad[k] + part
        grad[m] = mine
        return total

    zero = jnp.zeros((1, quarter), f32)
    truth_total = lax.fori_loop(0, members, truth_step, zero)
    pair_total = lax.fori_loop(0, members, pair_step, zero)
    fine_loss = weight * (truth_total * (1.0 / members) - pair_total * pair_scale)
    scale = weight * (1.0 / variables)

    def send_grads(o):
        peer = member_peer(o)
        for j in range(locals_):
            gsend[peer, j] = (grad[peer * locals_ + j] * scale).astype(bf16)
        to_member(lambda p: gsend.at[p], grecv, gs_sem, gr_sem, o).start()

    send_grads(1)
    for j in range(locals_):
        grecv[mm, j] = (grad[mm * locals_ + j] * scale).astype(bf16)

    for o in range(1, places):
        from_member(mrecv, ms_sem, mr_sem, o).wait_recv()
    rows = locals_ * CELL_DEV
    own = means.astype(f32).reshape(rows, LANES)
    cell_lane = lax.broadcasted_iota(jnp.int32, (CELL_DEV, LANES), 1)
    cell_target = jnp.where(cell_lane < variables, meta / divisor, 0.0)

    def repeat(value):
        return jnp.concatenate([value] * locals_, axis=0)

    d = own - repeat(cell_target)
    sq = jnp.sum(d * d, axis=1, keepdims=True) * (1.0 / variables) + epsilon
    inv = lax.rsqrt(sq)
    coarse = d * (inv * (1.0 / members))
    coarse_dist = sq * inv * (1.0 / members)
    for o in range(places):
        peer = member_peer(o)
        for r in range(locals_):
            if o == 0 and r == 0:
                continue
            other = jnp.concatenate([mrecv[peer, (j + r) % locals_] for j in range(locals_)], axis=0)
            d = own - other.astype(f32)
            sq = jnp.sum(d * d, axis=1, keepdims=True) * (1.0 / variables) + epsilon
            inv = lax.rsqrt(sq)
            coarse = coarse - d * (inv * pair_scale)
            coarse_dist = coarse_dist - sq * inv * (0.5 * pair_scale)
    cell_weight = repeat(cell_area)
    per_cell = (coarse * (cell_weight * (1.0 / variables)) / repeat(divisor)).astype(bf16)
    dsend[...] = per_cell.reshape(locals_, CELL_DEV, LANES)
    for o in range(1, spaces):
        to_space(lambda peer: dsend, drecv, ds_sem, dr_sem, o).start()
    drecv[ms] = per_cell.reshape(locals_, CELL_DEV, LANES)
    coarse_loss = jnp.sum(cell_weight * coarse_dist, axis=0, keepdims=True)

    row = lax.broadcasted_iota(jnp.int32, (8, LANES), 0)
    lmem[mm] = jnp.where(row == 0, jnp.sum(fine_loss, axis=1, keepdims=True), coarse_loss)
    for o in range(1, places):
        to_member(lambda peer: lmem.at[mm], lmem, ls_sem, lr_sem, o).start()
    for o in range(2, places):
        send_grads(o)

    for o in range(1, spaces):
        from_space(drecv, ds_sem, dr_sem, o).wait_recv()
    by_cell = [drecv[:, j].reshape(cells, LANES) for j in range(locals_)]
    for j in range(locals_):
        pieces[:, j * LANES:(j + 1) * LANES] = by_cell[j]
    factor = scaling / all_area

    def upstream(i):
        q = lax.rem(mm + 1 + i, places)
        coarse_part = jnp.dot(turned_hot[nodes_of(q), :], pieces[...], preferred_element_type=f32)
        for j in range(locals_):
            fine = grecv[q, j].astype(f32).T
            up_buf[j * quarter:(j + 1) * quarter, :] = (
                fine + coarse_part[:, j * LANES:j * LANES + variables]).astype(bf16)

    def hidden_to(pg, i):
        h = jnp.dot(up_buf[...], w_out[...], preferred_element_type=f32)
        pg[...] = (h * slope_buf[i].astype(f32)).astype(bf16)

    def finish(i):
        upstream(i)
        hidden_to(act, i)
        g = jnp.dot(act[...], turned[...], preferred_element_type=f32)
        early[i - 1] = (g * factor).astype(bf16).reshape(locals_, quarter, width)

    finish(places - 1)
    for o in range(1, places):
        from_member(lmem, ls_sem, lr_sem, o).wait_recv()
    loss = lmem[0]
    for m in range(1, places):
        loss = loss + lmem[m]
    lspace[ms] = loss
    for o in range(1, spaces):
        to_space(lambda peer: lspace.at[ms], lspace, ts_sem, tr_sem, o).start()

    def arrived(n, carry):
        i = places - 2 - n
        from_member(grecv, gs_sem, gr_sem, i + 1).wait_recv()
        finish(i)
        return carry

    lax.fori_loop(0, places - 2, arrived, 0)
    from_member(grecv, gs_sem, gr_sem, 1).wait_recv()
    upstream(0)
    hidden_to(pg_out, 0)

    for o in range(1, spaces):
        from_space(lspace, ts_sem, tr_sem, o).wait_recv()
    loss = lspace[0]
    for s in range(1, spaces):
        loss = loss + lspace[s]
    stats_out[...] = jnp.where(row == 2, all_area, loss)

    for o in range(1, places):
        to_member(lambda peer: psend.at[peer], precv, ps_sem, pr_sem, o).wait_send()
        to_member(lambda peer: mrecv.at[mm], mrecv, ms_sem, mr_sem, o).wait_send()
        to_member(lambda peer: gsend.at[peer], grecv, gs_sem, gr_sem, o).wait_send()
        to_member(lambda peer: lmem.at[mm], lmem, ls_sem, lr_sem, o).wait_send()
    for o in range(1, spaces):
        to_space(lambda peer: csend.at[peer], crecv, cs_sem, cr_sem, o).wait_send()
        to_space(lambda peer: dsend, drecv, ds_sem, dr_sem, o).wait_send()
        to_space(lambda peer: lspace.at[ms], lspace, ts_sem, tr_sem, o).wait_send()


def backward(places, scaling, early, pg, turned, stats, latent_grad, scores, last, store_sem):
    locals_, quarter, width = last.shape
    mm = lax.axis_index("member")

    def nodes_of(i):
        q = lax.rem(mm + 1 + i, places)
        return pl.ds(pl.multiple_of(q * quarter, quarter), quarter)

    def store(i):
        return pltpu.make_async_copy(early.at[i - 1], latent_grad.at[:, nodes_of(i), :], store_sem.at[i - 1])

    def store_last(n):
        at = pl.ds(pl.multiple_of(n * COLS, COLS), COLS)
        return pltpu.make_async_copy(
            last.at[:, :, at], latent_grad.at[:, nodes_of(0), at], store_sem.at[places - 1 + n])

    for i in range(1, places):
        store(i).start()
    all_area = stats[2:3, 0:1]
    factor = scaling / all_area

    def outputs(n, carry):
        at = pl.ds(pl.multiple_of(n * COLS, COLS), COLS)
        g = jnp.dot(pg[...], turned[:, at], preferred_element_type=f32)
        last[:, :, at] = (g * factor).astype(bf16).reshape(locals_, quarter, COLS)
        store_last(n).start()
        return carry

    lax.fori_loop(0, width // COLS, outputs, 0)
    both = stats[...] / all_area
    scores[0] = both[0, 0]
    scores[1] = both[1, 0]
    for i in range(1, places):
        store(i).wait()
    for n in range(width // COLS):
        store_last(n).wait()


def solution(mesh):
    spaces, places = mesh.shape["space"], mesh.shape["member"]

    def shards(latent, w_in, b_in, w_out, b_out, target, area, cell_of):
        locals_, nodes, width = latent.shape
        units, variables = w_out.shape
        quarter = nodes // places
        cells = CELL_DEV * spaces
        members = locals_ * places
        anywhere = pl.BlockSpec(memory_space=pl.ANY)
        inside = pl.BlockSpec(memory_space=pltpu.VMEM)
        by_member = [pltpu.SemaphoreType.DMA((places,))]
        by_space = [pltpu.SemaphoreType.DMA((spaces,))]
        rows = locals_ * quarter
        scaling = loss_scale * (nodes * spaces)
        early, pg, turned, stats = pl.pallas_call(
            functools.partial(exchange, spaces, places, scaling),
            out_shape=(
                pltpu.VMEM((places - 1, locals_, quarter, width), bf16),
                pltpu.VMEM((rows, units), bf16),
                pltpu.VMEM((units, width), bf16),
                pltpu.VMEM((8, LANES), f32),
            ),
            in_specs=[anywhere] * 8,
            out_specs=(inside, inside, inside, inside),
            scratch_shapes=[
                pltpu.VMEM((1, units), f32),
                pltpu.VMEM((variables, units), bf16),
                pltpu.VMEM((1, variables), f32),
                pltpu.VMEM((variables, nodes), f32),
                pltpu.VMEM((1, nodes), f32),
                pltpu.VMEM((1, nodes), jnp.int32),
                pltpu.VMEM((places, locals_, quarter, width), bf16),
                pltpu.VMEM((width, units), bf16),
                pltpu.VMEM((places, rows, units), bf16),
                pltpu.VMEM((rows, units), bf16),
                pltpu.VMEM((places, locals_, variables, quarter), bf16),
                pltpu.VMEM((places, locals_, variables, quarter), bf16),
                pltpu.VMEM((members, variables, quarter), f32),
                pltpu.VMEM((members, variables, quarter), f32),
                pltpu.VMEM((places, locals_, variables, quarter), bf16),
                pltpu.VMEM((places, locals_, variables, quarter), bf16),
                pltpu.VMEM((cells, nodes), bf16),
                pltpu.VMEM((nodes, cells), bf16),
                pltpu.VMEM((locals_ + 1, cells, LANES), f32),
                pltpu.VMEM((spaces, locals_ + 1, CELL_DEV, LANES), bf16),
                pltpu.VMEM((spaces, locals_ + 1, CELL_DEV, LANES), bf16),
                pltpu.VMEM((places, locals_, CELL_DEV, LANES), bf16),
                pltpu.VMEM((locals_, CELL_DEV, LANES), bf16),
                pltpu.VMEM((spaces, locals_, CELL_DEV, LANES), bf16),
                pltpu.VMEM((cells, locals_ * LANES), bf16),
                pltpu.VMEM((rows, variables), bf16),
                pltpu.VMEM((places, 8, LANES), f32),
                pltpu.VMEM((spaces, 8, LANES), f32),
                pltpu.SemaphoreType.DMA((places + 1,)),
                pltpu.SemaphoreType.DMA((6,)),
            ]
            + by_member * 4
            + by_space * 2
            + by_member * 2
            + by_space * 2
            + by_member * 2
            + by_space * 2,
            compiler_params=pltpu.CompilerParams(
                collective_id=0, has_side_effects=True, vmem_limit_bytes=36 * 2**20
            ),
            name="exchange",
        )(*map(in_hbm, (latent, w_in, b_in[None], w_out.T, b_out[None], target.T, area[None], cell_of[None])))

        latent_grad, scores = pl.pallas_call(
            functools.partial(backward, places, scaling),
            out_shape=(
                jax.ShapeDtypeStruct((locals_, nodes, width), bf16),
                jax.ShapeDtypeStruct((2,), f32),
            ),
            in_specs=[inside] * 4,
            out_specs=(anywhere, pl.BlockSpec(memory_space=pltpu.SMEM)),
            scratch_shapes=[
                pltpu.VMEM((locals_, quarter, width), bf16),
                pltpu.SemaphoreType.DMA((places - 1 + width // COLS,)),
            ],
            compiler_params=pltpu.CompilerParams(vmem_limit_bytes=16 * 2**20),
            name="backward",
        )(early, pg, turned, stats)
        return latent_grad, scores

    in_specs = (
        P("member", "space", None),
        P(),
        P(),
        P(),
        P(),
        P("space", None),
        P("space"),
        P("space"),
    )
    out_specs = (P("member", "space", None), P())
    return jax.shard_map(shards, mesh=mesh, in_specs=in_specs, out_specs=out_specs, check_vma=False)
```

```python
import functools

import jax
import jax.numpy as jnp
from jax import lax
from jax.experimental import pallas as pl
from jax.experimental.pallas import tpu as pltpu
from jax.sharding import PartitionSpec as P

CELL_DEV = 32
COLS = 512
SLIM = 256
LANES = 128

epsilon = 1e-05
loss_scale = 4096.0
bf16, f32 = jnp.bfloat16, jnp.float32
MESH = pl.DeviceIdType.MESH


def in_hbm(value):
    return pltpu.with_memory_space_constraint(value, pltpu.HBM)


def dot_t(a, b):
    return lax.dot_general(a, b, (((1,), (1,)), ((), ())), preferred_element_type=f32)


def halves(value):
    high = value.astype(bf16).astype(f32)
    return high, value - high


def exchange(spaces, places, scaling, latent, w_in, b_in_far, w_out_far, b_out_far, target_far, area_far,
             cell_of_far,
             early, pg_out, turned, stats_out,
             b_in, w_out, b_out, target, area, cell_of, lat_buf, w_buf, slope_buf, act,
             psend, precv, p32, grad, gsend, grecv, hot, turned_hot, pcat, qsend, qrecv, csend, crecv,
             mrecv, dsend, drecv, up_buf, lmem, lspace,
             load_sem, small_sem, ps_sem, pr_sem, gs_sem, gr_sem, qs_sem, qr_sem, cs_sem, cr_sem,
             ms_sem, mr_sem, ds_sem, dr_sem, ls_sem, lr_sem, ts_sem, tr_sem):
    ms = lax.axis_index("space")
    mm = lax.axis_index("member")
    locals_, quarter, width = lat_buf.shape[1:]
    units = w_buf.shape[1]
    variables = target.shape[0]
    members = locals_ * places
    cells = CELL_DEV * spaces
    pair_scale = 1.0 / (members * (members - 1))

    def member_peer(o):
        return lax.rem(mm + o, places)

    def space_peer(o):
        return lax.rem(ms + o, spaces)

    def to_member(src, dst, ss, rs, o):
        return pltpu.make_async_remote_copy(
            src_ref=src, dst_ref=dst.at[mm], send_sem=ss, recv_sem=rs,
            device_id={"member": member_peer(o)}, device_id_type=MESH)

    def to_space(src, dst, ss, rs, o):
        return pltpu.make_async_remote_copy(
            src_ref=src, dst_ref=dst.at[ms], send_sem=ss, recv_sem=rs,
            device_id={"space": space_peer(o)}, device_id_type=MESH)

    def all_members(dst, ss, rs):
        part = dst.at[pl.ds(0, places - 1)]
        return pltpu.make_async_remote_copy(
            src_ref=part, dst_ref=part, send_sem=ss, recv_sem=rs,
            device_id={"member": member_peer(1)}, device_id_type=MESH)

    def all_spaces(dst, ss, rs):
        part = dst.at[pl.ds(0, spaces - 1)]
        return pltpu.make_async_remote_copy(
            src_ref=part, dst_ref=part, send_sem=ss, recv_sem=rs,
            device_id={"space": space_peer(1)}, device_id_type=MESH)

    def from_member(dst, ss, rs, o):
        peer = member_peer(o)
        return pltpu.make_async_remote_copy(
            src_ref=dst.at[peer], dst_ref=dst.at[peer], send_sem=ss, recv_sem=rs.at[peer],
            device_id={"member": peer}, device_id_type=MESH)

    def nodes_of(q):
        return pl.ds(pl.multiple_of(q * quarter, quarter), quarter)

    def load_chunk(i):
        q = lax.rem(mm + 1 + i, places)
        return pltpu.make_async_copy(latent.at[:, nodes_of(q), :], lat_buf.at[i], load_sem.at[i])

    w_copy = pltpu.make_async_copy(w_in, w_buf, load_sem.at[places])
    small = [
        pltpu.make_async_copy(src, dst, small_sem.at[n])
        for n, (src, dst) in enumerate((
            (cell_of_far, cell_of), (area_far, area), (target_far, target),
            (b_in_far, b_in), (w_out_far, w_out.at[pl.ds(0, variables)]), (b_out_far, b_out)))
    ]
    for copy in small[:3]:
        copy.start()
    w_copy.start()
    load_chunk(0).start()
    for copy in small[3:]:
        copy.start()
    for i in range(1, places):
        load_chunk(i).start()
    barrier = pltpu.get_barrier_semaphore()
    for o in range(1, places):
        pl.semaphore_signal(barrier, inc=1, device_id={"member": member_peer(o)}, device_id_type=MESH)
    for o in range(1, spaces):
        pl.semaphore_signal(barrier, inc=1, device_id={"space": space_peer(o)}, device_id_type=MESH)

    for copy in small[:3]:
        copy.wait()
    match = lax.broadcasted_iota(jnp.int32, (cells, cell_of.shape[1]), 0) == cell_of[...]
    ones = jnp.where(match, 1.0, 0.0)
    hot[...] = ones.astype(bf16)
    counts = halves(jnp.sum(ones, axis=1, keepdims=True))
    areas = halves(jnp.sum(jnp.where(match, area[...], 0.0), axis=1, keepdims=True))
    whole = halves(jnp.sum(area[...], axis=1, keepdims=True))
    spare = LANES - variables
    t_high, t_low = halves(target[...])
    sums = dot_t(hot[...], t_high.astype(bf16)) + dot_t(hot[...], t_low.astype(bf16))
    lane = lax.broadcasted_iota(jnp.int32, (cells, LANES), 1)
    meta = jnp.concatenate([sums, jnp.zeros((cells, spare), f32)], axis=1)
    for n, value in enumerate(counts + areas + whole):
        meta = jnp.where(lane == variables + n, value, meta)
    for s in range(spaces):
        qsend[s] = meta[s * CELL_DEV:(s + 1) * CELL_DEV].astype(bf16)
    w_out[variables:, :] = jnp.zeros((spare, units), bf16)

    for copy in small[3:]:
        copy.wait()
    w_copy.wait()

    def forward(i, carry):
        q = lax.rem(mm + 1 + i, places)
        load_chunk(i).wait()

        rows = lat_buf[i].reshape(locals_ * quarter, width)
        x = jnp.dot(rows, w_buf[...], preferred_element_type=f32) + b_in[...]
        act[...] = (x * (0.5 * jnp.tanh(0.5 * x) + 0.5)).astype(bf16)
        slope_buf[i] = x.astype(bf16)
        bias = jnp.concatenate([b_out[...], jnp.zeros((1, spare), f32)], axis=1)
        rounded = (dot_t(act[...], w_out[...]) + bias).astype(bf16)
        for j in range(locals_):
            block = rounded[j * quarter:(j + 1) * quarter]
            psend[q, j] = block.astype(f32).T[:variables].astype(bf16)
            pcat[nodes_of(q), j * LANES:(j + 1) * LANES] = block
        return carry

    def forward_send(i, carry):
        forward(i, carry)

        @pl.when(i == 0)
        def _():
            pl.semaphore_wait(barrier, places + spaces - 2)

        to_member(psend.at[member_peer(i + 1)], precv, ps_sem, pr_sem, i + 1).start()

        @pl.when(i == 0)
        def _():
            for o in range(1, spaces):
                to_space(qsend.at[space_peer(o)], qrecv, qs_sem, qr_sem, o).start()

        return carry

    lax.fori_loop(0, places - 1, forward_send, 0)
    forward(places - 1, 0)

    sums = jnp.dot(hot[...], pcat[...], preferred_element_type=f32).astype(bf16)
    for s in range(spaces):
        csend[s] = sums[s * CELL_DEV:(s + 1) * CELL_DEV]
    for o in range(1, spaces):
        to_space(csend.at[space_peer(o)], crecv, cs_sem, cr_sem, o).start()

    def turn(n, carry):
        at = pl.ds(pl.multiple_of(n * COLS, COLS), COLS)
        turned[:, at] = w_buf[at, :].T
        return carry

    lax.fori_loop(0, width // COLS, turn, 0)
    for q in range(places):
        at = slice(q * quarter, (q + 1) * quarter)
        turned_hot[at, :] = hot[:, at].astype(f32).T.astype(bf16)

    qrecv[ms] = qsend[ms]
    all_spaces(qrecv, qs_sem, qr_sem).wait_recv()
    meta = qrecv[0].astype(f32)
    for s in range(1, spaces):
        meta = meta + qrecv[s].astype(f32)
    cell_count = meta[:, variables:variables + 1] + meta[:, variables + 1:variables + 2]
    cell_area = meta[:, variables + 2:variables + 3] + meta[:, variables + 3:variables + 4]
    all_area = meta[0:1, variables + 4:variables + 5] + meta[0:1, variables + 5:variables + 6]
    divisor = jnp.maximum(cell_count, 1.0)
    cell_lane = lax.broadcasted_iota(jnp.int32, (CELL_DEV, LANES), 1)
    facts = jnp.where(cell_lane < variables, meta / divisor, jnp.where(cell_lane == variables, divisor, cell_area))
    facts = jnp.concatenate([facts] * locals_, axis=0).T
    cell_target = facts[:variables]
    lane_divisor = facts[variables:variables + 1]
    cell_weight = facts[variables + 1:variables + 2]

    def slopes(n, carry):
        i, at = lax.div(n, units // SLIM), pl.ds(pl.multiple_of(lax.rem(n, units // SLIM) * SLIM, SLIM), SLIM)
        x = slope_buf[i, :, at].astype(f32)
        s = 0.5 * jnp.tanh(0.5 * x) + 0.5
        slope_buf[i, :, at] = (s + x * s * (1.0 - s)).astype(bf16)
        return carry

    half = places // 2 * (units // SLIM)
    lax.fori_loop(0, half, slopes, 0)

    crecv[ms] = csend[ms]
    all_spaces(crecv, cs_sem, cr_sem).wait_recv()
    total = crecv[0].astype(f32)
    for s in range(1, spaces):
        total = total + crecv[s].astype(f32)
    means = (total / divisor).astype(bf16).astype(f32)
    own = jnp.concatenate([means[:, j * LANES:(j + 1) * LANES] for j in range(locals_)], axis=0).T[:variables]
    mrecv[mm] = own.astype(bf16)
    for o in range(1, places):
        to_member(mrecv.at[mm], mrecv, ms_sem, mr_sem, o).start()

    precv[mm] = psend[mm]
    truths = target[:, nodes_of(mm)]
    weight = area[:, nodes_of(mm)]
    all_members(precv, ps_sem, pr_sem).wait_recv()

    def truth_step(m, total):
        p = precv[lax.div(m, locals_), lax.rem(m, locals_)].astype(f32)
        p32[m] = p
        d = p - truths
        sq = jnp.sum(d * d, axis=0, keepdims=True) * (1.0 / variables) + epsilon
        r = lax.rsqrt(sq)
        grad[m] = d * (r * (1.0 / members))
        return total + sq * r

    def pair_step(m, total):
        pm = p32[m]
        factors = []
        for r in range(1, members // 2 + 1):
            share = 0.5 if 2 * r == members else 1.0
            d = pm - p32[lax.rem(m + r, members)]
            sq = jnp.sum(d * d, axis=0, keepdims=True) * (1.0 / variables) + epsilon
            inv = lax.rsqrt(sq)
            total = total + share * (sq * inv)
            factors.append(inv * (share * pair_scale))
        mine = grad[m]
        for r in range(1, members // 2 + 1):
            k = lax.rem(m + r, members)
            part = (pm - p32[k]) * factors[r - 1]
            mine = mine - part
            grad[k] = grad[k] + part
        grad[m] = mine
        return total

    zero = jnp.zeros((1, quarter), f32)
    truth_total = lax.fori_loop(0, members, truth_step, zero)
    pair_total = lax.fori_loop(0, members, pair_step, zero)
    fine_loss = weight * (truth_total * (1.0 / members) - pair_total * pair_scale)
    scale = weight * (1.0 / variables)

    def send_grads(o):
        peer = member_peer(o)
        for j in range(locals_):
            gsend[peer, j] = (grad[peer * locals_ + j] * scale).astype(bf16)
        to_member(gsend.at[peer], grecv, gs_sem, gr_sem.at[mm], o).start()

    send_grads(1)
    for j in range(locals_):
        grecv[mm, j] = (grad[mm * locals_ + j] * scale).astype(bf16)

    lax.fori_loop(half, places * (units // SLIM), slopes, 0)

    all_members(mrecv, ms_sem, mr_sem).wait_recv()
    d = own - cell_target
    sq = jnp.sum(d * d, axis=0, keepdims=True) * (1.0 / variables) + epsilon
    inv = lax.rsqrt(sq)
    coarse = d * (inv * (1.0 / members))
    coarse_dist = sq * inv * (1.0 / members)
    for o in range(places):
        theirs = mrecv[member_peer(o)].astype(f32)
        for r in range(locals_):
            if o == 0 and r == 0:
                continue
            d = own - (pltpu.roll(theirs, r * CELL_DEV, 1) if r else theirs)
            sq = jnp.sum(d * d, axis=0, keepdims=True) * (1.0 / variables) + epsilon
            inv = lax.rsqrt(sq)
            coarse = coarse - d * (inv * pair_scale)
            coarse_dist = coarse_dist - sq * inv * (0.5 * pair_scale)
    per_cell = coarse * (cell_weight * (1.0 / variables)) / lane_divisor
    per_cell = jnp.concatenate([per_cell, jnp.zeros((spare, locals_ * CELL_DEV), f32)], axis=0).T.astype(bf16)
    for j in range(locals_):
        dsend[:, j * LANES:(j + 1) * LANES] = per_cell[j * CELL_DEV:(j + 1) * CELL_DEV]
    for o in range(1, spaces):
        to_space(dsend, drecv, ds_sem, dr_sem, o).start()
    drecv[ms] = dsend[...]
    coarse_loss = jnp.sum(cell_weight * coarse_dist, axis=1, keepdims=True)

    row = lax.broadcasted_iota(jnp.int32, (8, LANES), 0)
    lmem[mm] = jnp.where(row == 0, jnp.sum(fine_loss, axis=1, keepdims=True), coarse_loss)
    for o in range(1, places):
        to_member(lmem.at[mm], lmem, ls_sem, lr_sem, o).start()
    for o in range(2, places):
        send_grads(o)

    all_spaces(drecv, ds_sem, dr_sem).wait_recv()
    factor = scaling / all_area

    def upstream(i):
        q = lax.rem(mm + 1 + i, places)
        pieces = drecv[...].reshape(cells, locals_ * LANES)
        coarse_part = jnp.dot(turned_hot[nodes_of(q), :], pieces, preferred_element_type=f32)
        blank = jnp.zeros((spare, quarter), f32)
        for j in range(locals_):
            fine = jnp.concatenate([grecv[q, j].astype(f32), blank], axis=0).T
            up_buf[j * quarter:(j + 1) * quarter, :] = (
                fine + coarse_part[:, j * LANES:(j + 1) * LANES]).astype(bf16)

    def hidden_to(pg, i):
        h = jnp.dot(up_buf[...], w_out[...], preferred_element_type=f32)
        pg[...] = (h * slope_buf[i].astype(f32)).astype(bf16)

    def finish(i):
        upstream(i)
        hidden_to(act, i)
        g = jnp.dot(act[...], turned[...], preferred_element_type=f32)
        early[i - 1] = (g * factor).astype(bf16).reshape(locals_, quarter, width)

    finish(places - 1)
    all_members(lmem, ls_sem, lr_sem).wait_recv()
    loss = lmem[0]
    for m in range(1, places):
        loss = loss + lmem[m]
    lspace[ms] = loss
    for o in range(1, spaces):
        to_space(lspace.at[ms], lspace, ts_sem, tr_sem, o).start()

    def arrived(n, carry):
        i = places - 2 - n
        from_member(grecv, gs_sem, gr_sem, i + 1).wait_recv()
        finish(i)
        return carry

    lax.fori_loop(0, places - 2, arrived, 0)
    from_member(grecv, gs_sem, gr_sem, 1).wait_recv()
    upstream(0)
    hidden_to(pg_out, 0)

    all_spaces(lspace, ts_sem, tr_sem).wait_recv()
    loss = lspace[0]
    for s in range(1, spaces):
        loss = loss + lspace[s]
    stats_out[...] = jnp.where(row == 2, all_area, loss)

    all_members(psend, ps_sem, pr_sem).wait_send()
    all_members(mrecv, ms_sem, mr_sem).wait_send()
    all_members(gsend, gs_sem, gr_sem.at[mm]).wait_send()
    all_members(lmem, ls_sem, lr_sem).wait_send()
    all_spaces(qsend, qs_sem, qr_sem).wait_send()
    all_spaces(csend, cs_sem, cr_sem).wait_send()
    all_spaces(drecv, ds_sem, dr_sem).wait_send()
    all_spaces(lspace, ts_sem, tr_sem).wait_send()


def backward(places, scaling, early, pg, turned, stats, latent_grad, scores_out, last, scores, store_sem):
    locals_, quarter, width = last.shape
    mm = lax.axis_index("member")

    def nodes_of(i):
        q = lax.rem(mm + 1 + i, places)
        return pl.ds(pl.multiple_of(q * quarter, quarter), quarter)

    def store(i):
        return pltpu.make_async_copy(early.at[i - 1], latent_grad.at[:, nodes_of(i), :], store_sem.at[i - 1])

    def store_last(n):
        at = pl.ds(pl.multiple_of(n * COLS, COLS), COLS)
        return pltpu.make_async_copy(
            last.at[:, :, at], latent_grad.at[:, nodes_of(0), at], store_sem.at[places - 1 + n])

    for i in range(1, places):
        store(i).start()
    all_area = stats[2:3, 0:1]
    factor = scaling / all_area
    both = stats[...] / all_area
    scores[0] = both[0, 0]
    scores[1] = both[1, 0]
    score_copy = pltpu.make_async_copy(scores, scores_out, store_sem.at[places - 1 + width // COLS])
    score_copy.start()

    def outputs(n, carry):
        at = pl.ds(pl.multiple_of(n * COLS, COLS), COLS)
        g = jnp.dot(pg[...], turned[:, at], preferred_element_type=f32)
        last[:, :, at] = (g * factor).astype(bf16).reshape(locals_, quarter, COLS)
        store_last(n).start()
        return carry

    lax.fori_loop(0, width // COLS, outputs, 0)
    score_copy.wait()
    for i in range(1, places):
        store(i).wait()
    for n in range(width // COLS):
        store_last(n).wait()


def solution(mesh):
    spaces, places = mesh.shape["space"], mesh.shape["member"]

    def shards(latent, w_in, b_in, w_out, b_out, target, area, cell_of):
        locals_, nodes, width = latent.shape
        units, variables = w_out.shape
        quarter = nodes // places
        cells = CELL_DEV * spaces
        members = locals_ * places
        anywhere = pl.BlockSpec(memory_space=pl.ANY)
        inside = pl.BlockSpec(memory_space=pltpu.VMEM)
        single = pltpu.SemaphoreType.DMA
        rows = locals_ * quarter
        scaling = loss_scale * (nodes * spaces)
        early, pg, turned, stats = pl.pallas_call(
            functools.partial(exchange, spaces, places, scaling),
            out_shape=(
                pltpu.VMEM((places - 1, locals_, quarter, width), bf16),
                pltpu.VMEM((rows, units), bf16),
                pltpu.VMEM((units, width), bf16),
                pltpu.VMEM((8, LANES), f32),
            ),
            in_specs=[anywhere] * 8,
            out_specs=(inside, inside, inside, inside),
            scratch_shapes=[
                pltpu.VMEM((1, units), f32),
                pltpu.VMEM((LANES, units), bf16),
                pltpu.VMEM((1, variables), f32),
                pltpu.VMEM((variables, nodes), f32),
                pltpu.VMEM((1, nodes), f32),
                pltpu.VMEM((1, nodes), jnp.int32),
                pltpu.VMEM((places, locals_, quarter, width), bf16),
                pltpu.VMEM((width, units), bf16),
                pltpu.VMEM((places, rows, units), bf16),
                pltpu.VMEM((rows, units), bf16),
                pltpu.VMEM((places, locals_, variables, quarter), bf16),
                pltpu.VMEM((places, locals_, variables, quarter), bf16),
                pltpu.VMEM((members, variables, quarter), f32),
                pltpu.VMEM((members, variables, quarter), f32),
                pltpu.VMEM((places, locals_, variables, quarter), bf16),
                pltpu.VMEM((places, locals_, variables, quarter), bf16),
                pltpu.VMEM((cells, nodes), bf16),
                pltpu.VMEM((nodes, cells), bf16),
                pltpu.VMEM((nodes, locals_ * LANES), bf16),
                pltpu.VMEM((spaces, CELL_DEV, LANES), bf16),
                pltpu.VMEM((spaces, CELL_DEV, LANES), bf16),
                pltpu.VMEM((spaces, CELL_DEV, locals_ * LANES), bf16),
                pltpu.VMEM((spaces, CELL_DEV, locals_ * LANES), bf16),
                pltpu.VMEM((places, variables, locals_ * CELL_DEV), bf16),
                pltpu.VMEM((CELL_DEV, locals_ * LANES), bf16),
                pltpu.VMEM((spaces, CELL_DEV, locals_ * LANES), bf16),
                pltpu.VMEM((rows, LANES), bf16),
                pltpu.VMEM((places, 8, LANES), f32),
                pltpu.VMEM((spaces, 8, LANES), f32),
                pltpu.SemaphoreType.DMA((places + 1,)),
                pltpu.SemaphoreType.DMA((6,)),
                single, single, single, pltpu.SemaphoreType.DMA((places,)),
            ]
            + [single] * 12,
            compiler_params=pltpu.CompilerParams(
                collective_id=0, has_side_effects=True, vmem_limit_bytes=36 * 2**20
            ),
            name="exchange",
        )(*map(in_hbm, (latent, w_in, b_in[None], w_out.T, b_out[None], target.T, area[None], cell_of[None])))

        latent_grad, scores = pl.pallas_call(
            functools.partial(backward, places, scaling),
            out_shape=(
                jax.ShapeDtypeStruct((locals_, nodes, width), bf16),
                jax.ShapeDtypeStruct((2,), f32),
            ),
            in_specs=[inside] * 4,
            out_specs=(anywhere, anywhere),
            scratch_shapes=[
                pltpu.VMEM((locals_, quarter, width), bf16),
                pltpu.SMEM((2,), f32),
                pltpu.SemaphoreType.DMA((places + width // COLS,)),
            ],
            compiler_params=pltpu.CompilerParams(vmem_limit_bytes=16 * 2**20),
            name="backward",
        )(early, pg, turned, stats)
        return latent_grad, scores

    in_specs = (
        P("member", "space", None),
        P(),
        P(),
        P(),
        P(),
        P("space", None),
        P("space"),
        P("space"),
    )
    out_specs = (P("member", "space", None), P())
    return jax.shard_map(shards, mesh=mesh, in_specs=in_specs, out_specs=out_specs, check_vma=False)
```

```python
import functools

import jax
import jax.numpy as jnp
from jax import lax
from jax.experimental import pallas as pl
from jax.experimental.pallas import tpu as pltpu
from jax.sharding import PartitionSpec as P

CELL_DEV = 32
COLS = 512
SLIM = 256
LANES = 128

epsilon = 1e-05
loss_scale = 4096.0
bf16, f32 = jnp.bfloat16, jnp.float32
MESH = pl.DeviceIdType.MESH


def in_hbm(value):
    return pltpu.with_memory_space_constraint(value, pltpu.HBM)


def dot_t(a, b):
    return lax.dot_general(a, b, (((1,), (1,)), ((), ())), preferred_element_type=f32)


def halves(value):
    high = value.astype(bf16).astype(f32)
    return high, value - high


def exchange(spaces, places, scaling, latent, w_in, b_in_far, w_out_far, b_out_far, target_far, area_far,
             cell_of_far,
             early, pg_out, turned, stats_out,
             b_in, w_out, b_out, target, area, cell_of, lat_buf, w_buf, slope_buf, act,
             psend, precv, p32, grad, gsend, grecv, hot, turned_hot, pcat, qsend, qrecv, csend, crecv,
             zsend, zrecv, mrecv, nrecv, dsend, drecv, up_buf, lmem, lspace,
             load_sem, small_sem, ps_sem, pr_sem, gs_sem, gr_sem, qs_sem, qr_sem, cs_sem, cr_sem,
             zs_sem, zr_sem, ms_sem, mr_sem, ns_sem, nr_sem, ds_sem, dr_sem, ls_sem, lr_sem, ts_sem, tr_sem):
    ms = lax.axis_index("space")
    mm = lax.axis_index("member")
    locals_, nodes, width = lat_buf.shape
    quarter = nodes // places
    units = w_buf.shape[1]
    variables = target.shape[0]
    members = locals_ * places
    rows = locals_ * quarter
    cells = CELL_DEV * spaces
    pair_scale = 1.0 / (members * (members - 1))

    def member_peer(o):
        return lax.rem(mm + o, places)

    def space_peer(o):
        return lax.rem(ms + o, spaces)

    def to_member(src, dst, ss, rs, o):
        return pltpu.make_async_remote_copy(
            src_ref=src, dst_ref=dst.at[mm], send_sem=ss, recv_sem=rs,
            device_id={"member": member_peer(o)}, device_id_type=MESH)

    def to_space(src, dst, ss, rs, o):
        return pltpu.make_async_remote_copy(
            src_ref=src, dst_ref=dst.at[ms], send_sem=ss, recv_sem=rs,
            device_id={"space": space_peer(o)}, device_id_type=MESH)

    def all_members(dst, ss, rs):
        part = dst.at[pl.ds(0, places - 1)]
        return pltpu.make_async_remote_copy(
            src_ref=part, dst_ref=part, send_sem=ss, recv_sem=rs,
            device_id={"member": member_peer(1)}, device_id_type=MESH)

    def all_spaces(dst, ss, rs):
        part = dst.at[pl.ds(0, spaces - 1)]
        return pltpu.make_async_remote_copy(
            src_ref=part, dst_ref=part, send_sem=ss, recv_sem=rs,
            device_id={"space": space_peer(1)}, device_id_type=MESH)

    def from_member(dst, ss, rs, o):
        peer = member_peer(o)
        return pltpu.make_async_remote_copy(
            src_ref=dst.at[peer], dst_ref=dst.at[peer], send_sem=ss, recv_sem=rs.at[peer],
            device_id={"member": peer}, device_id_type=MESH)

    def nodes_of(q):
        return pl.ds(pl.multiple_of(q * quarter, quarter), quarter)

    def load_chunk(j):
        return pltpu.make_async_copy(latent.at[j], lat_buf.at[j], load_sem.at[j])

    w_copy = pltpu.make_async_copy(w_in, w_buf, load_sem.at[locals_])
    small = [
        pltpu.make_async_copy(src, dst, small_sem.at[n])
        for n, (src, dst) in enumerate((
            (cell_of_far, cell_of), (area_far, area), (target_far, target),
            (b_in_far, b_in), (w_out_far, w_out.at[pl.ds(0, variables)]), (b_out_far, b_out)))
    ]
    for copy in small[:3]:
        copy.start()
    w_copy.start()
    load_chunk(0).start()
    for copy in small[3:]:
        copy.start()
    for j in range(1, locals_):
        load_chunk(j).start()
    barrier = pltpu.get_barrier_semaphore()
    for o in range(1, places):
        pl.semaphore_signal(barrier, inc=1, device_id={"member": member_peer(o)}, device_id_type=MESH)
    for o in range(1, spaces):
        pl.semaphore_signal(barrier, inc=1, device_id={"space": space_peer(o)}, device_id_type=MESH)

    for copy in small[:3]:
        copy.wait()
    spare = LANES - variables
    match = lax.broadcasted_iota(jnp.int32, (cells, nodes), 0) == cell_of[...]
    hot[...] = jnp.where(match, 1.0, 0.0).astype(bf16)
    row = lax.broadcasted_iota(jnp.int32, (spare, nodes), 0)
    t_high, t_low = halves(target[...])
    a_high, a_low = halves(area[...])
    firsts = jnp.where(row == 0, 1.0, jnp.where(row == 1, a_high, 0.0))
    seconds = jnp.where(row == 1, a_low, 0.0)
    sums = dot_t(hot[...], jnp.concatenate([t_high, firsts], axis=0).astype(bf16))
    sums = sums + dot_t(hot[...], jnp.concatenate([t_low, seconds], axis=0).astype(bf16))
    lane = lax.broadcasted_iota(jnp.int32, (cells, LANES), 1)
    lows = pltpu.roll(halves(sums)[1], 2, 1)
    meta = jnp.where(lane < variables + 2, sums, lows)
    for n, value in enumerate(halves(jnp.sum(area[...], axis=1, keepdims=True))):
        meta = jnp.where(lane == variables + 4 + n, value, meta)
    for s in range(spaces):
        qsend[s] = meta[s * CELL_DEV:(s + 1) * CELL_DEV].astype(bf16)
    w_out[variables:, :] = jnp.zeros((spare, units), bf16)

    for copy in small[3:]:
        copy.wait()
    w_copy.wait()

    def forward(j, carry):
        load_chunk(j).wait()
        x = jnp.dot(lat_buf[j], w_buf[...], preferred_element_type=f32) + b_in[...]
        act[...] = (x * (0.5 * jnp.tanh(0.5 * x) + 0.5)).astype(bf16)
        slope_buf[j] = x.astype(bf16)
        bias = jnp.concatenate([b_out[...], jnp.zeros((1, spare), f32)], axis=1)
        rounded = (dot_t(act[...], w_out[...]) + bias).astype(bf16)
        pcat[:, pl.ds(pl.multiple_of(j * LANES, LANES), LANES)] = rounded
        for q in range(places):
            psend[q, j] = rounded[q * quarter:(q + 1) * quarter].astype(f32).T[:variables].astype(bf16)

        @pl.when(j == 0)
        def _():
            pl.semaphore_wait(barrier, places + spaces - 2)

        for o in range(1, places):
            pltpu.make_async_remote_copy(
                src_ref=psend.at[member_peer(o), j], dst_ref=precv.at[mm, j], send_sem=ps_sem, recv_sem=pr_sem,
                device_id={"member": member_peer(o)}, device_id_type=MESH).start()

        @pl.when(j == 0)
        def _():
            for o in range(1, spaces):
                to_space(qsend.at[space_peer(o)], qrecv, qs_sem, qr_sem, o).start()

        return carry

    def spread(src, dst, ss, rs, lanes):
        sums = jnp.dot(hot[...], pcat[:, lanes], preferred_element_type=f32).astype(bf16)
        for s in range(spaces):
            src[s] = sums[s * CELL_DEV:(s + 1) * CELL_DEV]
        for o in range(1, spaces):
            to_space(src.at[space_peer(o)], dst, ss, rs, o).start()

    ahead = (locals_ - 1) * LANES
    lax.fori_loop(0, locals_ - 1, forward, 0)
    spread(csend, crecv, cs_sem, cr_sem, slice(0, ahead))
    forward(locals_ - 1, 0)
    spread(zsend, zrecv, zs_sem, zr_sem, slice(ahead, ahead + LANES))

    def turn(n, carry):
        at = pl.ds(pl.multiple_of(n * COLS, COLS), COLS)
        turned[:, at] = w_buf[at, :].T
        return carry

    lax.fori_loop(0, width // COLS, turn, 0)
    for q in range(places):
        at = slice(q * quarter, (q + 1) * quarter)
        turned_hot[at, :] = hot[:, at].astype(f32).T.astype(bf16)

    qrecv[ms] = qsend[ms]
    all_spaces(qrecv, qs_sem, qr_sem).wait_recv()
    meta = qrecv[0].astype(f32)
    for s in range(1, spaces):
        meta = meta + qrecv[s].astype(f32)
    cell_count = meta[:, variables:variables + 1] + meta[:, variables + 2:variables + 3]
    cell_area = meta[:, variables + 1:variables + 2] + meta[:, variables + 3:variables + 4]
    all_area = meta[0:1, variables + 4:variables + 5] + meta[0:1, variables + 5:variables + 6]
    divisor = jnp.maximum(cell_count, 1.0)
    cell_lane = lax.broadcasted_iota(jnp.int32, (CELL_DEV, LANES), 1)
    facts = jnp.where(cell_lane < variables, meta / divisor, jnp.where(cell_lane == variables, divisor, cell_area))
    facts = jnp.concatenate([facts] * locals_, axis=0).T
    cell_target = facts[:variables]
    lane_divisor = facts[variables:variables + 1]
    cell_weight = facts[variables + 1:variables + 2]

    def slopes(n, carry):
        j, at = lax.div(n, units // SLIM), pl.ds(pl.multiple_of(lax.rem(n, units // SLIM) * SLIM, SLIM), SLIM)
        x = slope_buf[j, :, at].astype(f32)
        s = 0.5 * jnp.tanh(0.5 * x) + 0.5
        slope_buf[j, :, at] = (s + x * s * (1.0 - s)).astype(bf16)
        return carry

    def average(src, near, far, means_buf, ss, rs):
        near[ms] = src[ms]
        far.wait_recv()
        total = near[0].astype(f32)
        for s in range(1, spaces):
            total = total + near[s].astype(f32)
        means_buf[mm] = (total / divisor).astype(bf16)
        for o in range(1, places):
            to_member(means_buf.at[mm], means_buf, ss, rs, o).start()

    average(csend, crecv, all_spaces(crecv, cs_sem, cr_sem), mrecv, ms_sem, mr_sem)
    half = locals_ // 2 * (units // SLIM)
    lax.fori_loop(0, half, slopes, 0)
    average(zsend, zrecv, all_spaces(zrecv, zs_sem, zr_sem), nrecv, ns_sem, nr_sem)

    def members_of(place):
        parts = [mrecv[place, :, j * LANES:(j + 1) * LANES] for j in range(locals_ - 1)] + [nrecv[place]]
        return jnp.concatenate(parts, axis=0).astype(f32).T[:variables]

    precv[mm] = psend[mm]
    truths = target[:, nodes_of(mm)]
    weight = area[:, nodes_of(mm)]
    all_members(precv, ps_sem, pr_sem).wait_recv()

    def truth_step(m, total):
        p = precv[lax.div(m, locals_), lax.rem(m, locals_)].astype(f32)
        p32[m] = p
        d = p - truths
        sq = jnp.sum(d * d, axis=0, keepdims=True) * (1.0 / variables) + epsilon
        r = lax.rsqrt(sq)
        grad[m] = d * (r * (1.0 / members))
        return total + sq * r

    def pair_step(m, total):
        pm = p32[m]
        factors = []
        for r in range(1, members // 2 + 1):
            share = 0.5 if 2 * r == members else 1.0
            d = pm - p32[lax.rem(m + r, members)]
            sq = jnp.sum(d * d, axis=0, keepdims=True) * (1.0 / variables) + epsilon
            inv = lax.rsqrt(sq)
            total = total + share * (sq * inv)
            factors.append(inv * (share * pair_scale))
        mine = grad[m]
        for r in range(1, members // 2 + 1):
            k = lax.rem(m + r, members)
            part = (pm - p32[k]) * factors[r - 1]
            mine = mine - part
            grad[k] = grad[k] + part
        grad[m] = mine
        return total

    zero = jnp.zeros((1, quarter), f32)
    truth_total = lax.fori_loop(0, members, truth_step, zero)
    pair_total = lax.fori_loop(0, members, pair_step, zero)
    fine_loss = weight * (truth_total * (1.0 / members) - pair_total * pair_scale)
    scale = weight * (1.0 / variables)

    def send_grads(o):
        peer = member_peer(o)
        for j in range(locals_):
            gsend[peer, j] = (grad[peer * locals_ + j] * scale).astype(bf16)
        to_member(gsend.at[peer], grecv, gs_sem, gr_sem.at[mm], o).start()

    send_grads(1)
    for j in range(locals_):
        grecv[mm, j] = (grad[mm * locals_ + j] * scale).astype(bf16)

    if places > 2:
        send_grads(2)

    own = members_of(mm)
    all_members(mrecv, ms_sem, mr_sem).wait_recv()
    all_members(nrecv, ns_sem, nr_sem).wait_recv()
    d = own - cell_target
    sq = jnp.sum(d * d, axis=0, keepdims=True) * (1.0 / variables) + epsilon
    inv = lax.rsqrt(sq)
    coarse = d * (inv * (1.0 / members))
    coarse_dist = sq * inv * (1.0 / members)
    for o in range(places):
        theirs = members_of(member_peer(o)) if o else own
        for r in range(locals_):
            if o == 0 and r == 0:
                continue
            d = own - (pltpu.roll(theirs, r * CELL_DEV, 1) if r else theirs)
            sq = jnp.sum(d * d, axis=0, keepdims=True) * (1.0 / variables) + epsilon
            inv = lax.rsqrt(sq)
            coarse = coarse - d * (inv * pair_scale)
            coarse_dist = coarse_dist - sq * inv * (0.5 * pair_scale)
    per_cell = coarse * (cell_weight * (1.0 / variables)) / lane_divisor
    per_cell = jnp.concatenate([per_cell, jnp.zeros((spare, locals_ * CELL_DEV), f32)], axis=0).T.astype(bf16)
    for j in range(locals_):
        dsend[:, j * LANES:(j + 1) * LANES] = per_cell[j * CELL_DEV:(j + 1) * CELL_DEV]
    for o in range(1, spaces):
        to_space(dsend, drecv, ds_sem, dr_sem, o).start()
    drecv[ms] = dsend[...]
    coarse_loss = jnp.sum(cell_weight * coarse_dist, axis=1, keepdims=True)

    row = lax.broadcasted_iota(jnp.int32, (8, LANES), 0)
    lmem[mm] = jnp.where(row == 0, jnp.sum(fine_loss, axis=1, keepdims=True), coarse_loss)
    for o in range(1, places):
        to_member(lmem.at[mm], lmem, ls_sem, lr_sem, o).start()
    for o in range(3, places):
        send_grads(o)
    lax.fori_loop(half, locals_ * (units // SLIM), slopes, 0)

    all_spaces(drecv, ds_sem, dr_sem).wait_recv()
    factor = scaling / all_area

    def upstream(i):
        q = lax.rem(mm + 1 + i, places)
        pieces = drecv[...].reshape(cells, locals_ * LANES)
        coarse_part = jnp.dot(turned_hot[nodes_of(q), :], pieces, preferred_element_type=f32)
        blank = jnp.zeros((spare, quarter), f32)
        for j in range(locals_):
            fine = jnp.concatenate([grecv[q, j].astype(f32), blank], axis=0).T
            up_buf[j * quarter:(j + 1) * quarter, :] = (
                fine + coarse_part[:, j * LANES:(j + 1) * LANES]).astype(bf16)

    def hidden_to(pg, i):
        h = jnp.dot(up_buf[...], w_out[...], preferred_element_type=f32)
        slope = slope_buf[:, nodes_of(lax.rem(mm + 1 + i, places)), :].reshape(rows, units)
        pg[...] = (h * slope.astype(f32)).astype(bf16)

    def finish(i):
        upstream(i)
        hidden_to(act, i)
        g = jnp.dot(act[...], turned[...], preferred_element_type=f32)
        early[i - 1] = (g * factor).astype(bf16).reshape(locals_, quarter, width)

    finish(places - 1)
    all_members(lmem, ls_sem, lr_sem).wait_recv()
    loss = lmem[0]
    for m in range(1, places):
        loss = loss + lmem[m]
    lspace[ms] = loss
    for o in range(1, spaces):
        to_space(lspace.at[ms], lspace, ts_sem, tr_sem, o).start()

    def arrived(n, carry):
        i = places - 2 - n
        from_member(grecv, gs_sem, gr_sem, i + 1).wait_recv()
        finish(i)
        return carry

    lax.fori_loop(0, places - 2, arrived, 0)
    from_member(grecv, gs_sem, gr_sem, 1).wait_recv()
    upstream(0)
    hidden_to(pg_out, 0)

    all_spaces(lspace, ts_sem, tr_sem).wait_recv()
    loss = lspace[0]
    for s in range(1, spaces):
        loss = loss + lspace[s]
    stats_out[...] = jnp.where(row == 2, all_area, loss)

    all_members(psend, ps_sem, pr_sem).wait_send()
    all_members(mrecv, ms_sem, mr_sem).wait_send()
    all_members(nrecv, ns_sem, nr_sem).wait_send()
    all_members(gsend, gs_sem, gr_sem.at[mm]).wait_send()
    all_members(lmem, ls_sem, lr_sem).wait_send()
    all_spaces(qsend, qs_sem, qr_sem).wait_send()
    all_spaces(csend, cs_sem, cr_sem).wait_send()
    all_spaces(zsend, zs_sem, zr_sem).wait_send()
    all_spaces(drecv, ds_sem, dr_sem).wait_send()
    all_spaces(lspace, ts_sem, tr_sem).wait_send()


def backward(places, scaling, early, pg, turned, stats, latent_grad, scores_out, last, scores, store_sem):
    locals_, quarter, width = last.shape
    mm = lax.axis_index("member")

    def nodes_of(i):
        q = lax.rem(mm + 1 + i, places)
        return pl.ds(pl.multiple_of(q * quarter, quarter), quarter)

    def store(i):
        return pltpu.make_async_copy(early.at[i - 1], latent_grad.at[:, nodes_of(i), :], store_sem.at[i - 1])

    def store_last(n):
        at = pl.ds(pl.multiple_of(n * COLS, COLS), COLS)
        return pltpu.make_async_copy(
            last.at[:, :, at], latent_grad.at[:, nodes_of(0), at], store_sem.at[places - 1 + n])

    for i in range(1, places):
        store(i).start()
    all_area = stats[2:3, 0:1]
    factor = scaling / all_area
    both = stats[...] / all_area
    scores[0] = both[0, 0]
    scores[1] = both[1, 0]
    score_copy = pltpu.make_async_copy(scores, scores_out, store_sem.at[places - 1 + width // COLS])
    score_copy.start()

    def outputs(n, carry):
        at = pl.ds(pl.multiple_of(n * COLS, COLS), COLS)
        g = jnp.dot(pg[...], turned[:, at], preferred_element_type=f32)
        last[:, :, at] = (g * factor).astype(bf16).reshape(locals_, quarter, COLS)
        store_last(n).start()
        return carry

    lax.fori_loop(0, width // COLS, outputs, 0)
    score_copy.wait()
    for i in range(1, places):
        store(i).wait()
    for n in range(width // COLS):
        store_last(n).wait()


def solution(mesh):
    spaces, places = mesh.shape["space"], mesh.shape["member"]

    def shards(latent, w_in, b_in, w_out, b_out, target, area, cell_of):
        locals_, nodes, width = latent.shape
        units, variables = w_out.shape
        quarter = nodes // places
        cells = CELL_DEV * spaces
        members = locals_ * places
        anywhere = pl.BlockSpec(memory_space=pl.ANY)
        inside = pl.BlockSpec(memory_space=pltpu.VMEM)
        single = pltpu.SemaphoreType.DMA
        rows = locals_ * quarter
        scaling = loss_scale * (nodes * spaces)
        early, pg, turned, stats = pl.pallas_call(
            functools.partial(exchange, spaces, places, scaling),
            out_shape=(
                pltpu.VMEM((places - 1, locals_, quarter, width), bf16),
                pltpu.VMEM((rows, units), bf16),
                pltpu.VMEM((units, width), bf16),
                pltpu.VMEM((8, LANES), f32),
            ),
            in_specs=[anywhere] * 8,
            out_specs=(inside, inside, inside, inside),
            scratch_shapes=[
                pltpu.VMEM((1, units), f32),
                pltpu.VMEM((LANES, units), bf16),
                pltpu.VMEM((1, variables), f32),
                pltpu.VMEM((variables, nodes), f32),
                pltpu.VMEM((1, nodes), f32),
                pltpu.VMEM((1, nodes), jnp.int32),
                pltpu.VMEM((locals_, nodes, width), bf16),
                pltpu.VMEM((width, units), bf16),
                pltpu.VMEM((locals_, nodes, units), bf16),
                pltpu.VMEM((rows, units), bf16),
                pltpu.VMEM((places, locals_, variables, quarter), bf16),
                pltpu.VMEM((places, locals_, variables, quarter), bf16),
                pltpu.VMEM((members, variables, quarter), f32),
                pltpu.VMEM((members, variables, quarter), f32),
                pltpu.VMEM((places, locals_, variables, quarter), bf16),
                pltpu.VMEM((places, locals_, variables, quarter), bf16),
                pltpu.VMEM((cells, nodes), bf16),
                pltpu.VMEM((nodes, cells), bf16),
                pltpu.VMEM((nodes, locals_ * LANES), bf16),
                pltpu.VMEM((spaces, CELL_DEV, LANES), bf16),
                pltpu.VMEM((spaces, CELL_DEV, LANES), bf16),
                pltpu.VMEM((spaces, CELL_DEV, (locals_ - 1) * LANES), bf16),
                pltpu.VMEM((spaces, CELL_DEV, (locals_ - 1) * LANES), bf16),
                pltpu.VMEM((spaces, CELL_DEV, LANES), bf16),
                pltpu.VMEM((spaces, CELL_DEV, LANES), bf16),
                pltpu.VMEM((places, CELL_DEV, (locals_ - 1) * LANES), bf16),
                pltpu.VMEM((places, CELL_DEV, LANES), bf16),
                pltpu.VMEM((CELL_DEV, locals_ * LANES), bf16),
                pltpu.VMEM((spaces, CELL_DEV, locals_ * LANES), bf16),
                pltpu.VMEM((rows, LANES), bf16),
                pltpu.VMEM((places, 8, LANES), f32),
                pltpu.VMEM((spaces, 8, LANES), f32),
                pltpu.SemaphoreType.DMA((locals_ + 1,)),
                pltpu.SemaphoreType.DMA((6,)),
                single, single, single, pltpu.SemaphoreType.DMA((places,)),
            ]
            + [single] * 16,
            compiler_params=pltpu.CompilerParams(
                collective_id=0, has_side_effects=True, vmem_limit_bytes=36 * 2**20
            ),
            name="exchange",
        )(*map(in_hbm, (latent, w_in, b_in[None], w_out.T, b_out[None], target.T, area[None], cell_of[None])))

        latent_grad, scores = pl.pallas_call(
            functools.partial(backward, places, scaling),
            out_shape=(
                jax.ShapeDtypeStruct((locals_, nodes, width), bf16),
                jax.ShapeDtypeStruct((2,), f32),
            ),
            in_specs=[inside] * 4,
            out_specs=(anywhere, anywhere),
            scratch_shapes=[
                pltpu.VMEM((locals_, quarter, width), bf16),
                pltpu.SMEM((2,), f32),
                pltpu.SemaphoreType.DMA((places + width // COLS,)),
            ],
            compiler_params=pltpu.CompilerParams(vmem_limit_bytes=16 * 2**20),
            name="backward",
        )(early, pg, turned, stats)
        return latent_grad, scores

    in_specs = (
        P("member", "space", None),
        P(),
        P(),
        P(),
        P(),
        P("space", None),
        P("space"),
        P("space"),
    )
    out_specs = (P("member", "space", None), P())
    return jax.shard_map(shards, mesh=mesh, in_specs=in_specs, out_specs=out_specs, check_vma=False)
```

```python
import functools

import jax
import jax.numpy as jnp
from jax import lax
from jax.experimental import pallas as pl
from jax.experimental.pallas import tpu as pltpu
from jax.sharding import PartitionSpec as P

CELL_DEV = 32
COLS = 512
SLIM = 256
LANES = 128

epsilon = 1e-05
loss_scale = 4096.0
bf16, f32 = jnp.bfloat16, jnp.float32
MESH = pl.DeviceIdType.MESH


def in_hbm(value):
    return pltpu.with_memory_space_constraint(value, pltpu.HBM)


def dot_t(a, b):
    return lax.dot_general(a, b, (((1,), (1,)), ((), ())), preferred_element_type=f32)


def halves(value):
    high = value.astype(bf16).astype(f32)
    return high, value - high


def exchange(spaces, places, scaling, latent, w_in, b_in_far, w_out_far, b_out_far, target_far, area_far,
             cell_of_far,
             early, pg_out, turned, stats_out,
             b_in, w_out, b_out, target, area, cell_of, lat_buf, w_buf, slope_buf, act,
             psend, precv, p32, grad, gsend, grecv, hot, turned_hot, pcat, qsend, qrecv, csend, crecv,
             zsend, zrecv, mrecv, nrecv, dsend, drecv, up_buf, lmem, lspace,
             load_sem, small_sem, ps_sem, pr_sem, gs_sem, gr_sem, qs_sem, qr_sem, cs_sem, cr_sem,
             zs_sem, zr_sem, ms_sem, mr_sem, ns_sem, nr_sem, ds_sem, dr_sem, ls_sem, lr_sem, ts_sem, tr_sem):
    ms = lax.axis_index("space")
    mm = lax.axis_index("member")
    locals_, nodes, width = lat_buf.shape
    quarter = nodes // places
    units = w_buf.shape[1]
    variables = target.shape[0]
    members = locals_ * places
    rows = locals_ * quarter
    cells = CELL_DEV * spaces
    pair_scale = 1.0 / (members * (members - 1))

    def member_peer(o):
        return lax.rem(mm + o, places)

    def space_peer(o):
        return lax.rem(ms + o, spaces)

    def to_member(src, dst, ss, rs, o):
        return pltpu.make_async_remote_copy(
            src_ref=src, dst_ref=dst.at[mm], send_sem=ss, recv_sem=rs,
            device_id={"member": member_peer(o)}, device_id_type=MESH)

    def to_space(src, dst, ss, rs, o):
        return pltpu.make_async_remote_copy(
            src_ref=src, dst_ref=dst.at[ms], send_sem=ss, recv_sem=rs,
            device_id={"space": space_peer(o)}, device_id_type=MESH)

    def all_members(dst, ss, rs):
        part = dst.at[pl.ds(0, places - 1)]
        return pltpu.make_async_remote_copy(
            src_ref=part, dst_ref=part, send_sem=ss, recv_sem=rs,
            device_id={"member": member_peer(1)}, device_id_type=MESH)

    def all_spaces(dst, ss, rs):
        part = dst.at[pl.ds(0, spaces - 1)]
        return pltpu.make_async_remote_copy(
            src_ref=part, dst_ref=part, send_sem=ss, recv_sem=rs,
            device_id={"space": space_peer(1)}, device_id_type=MESH)

    def from_member(dst, ss, rs, o):
        peer = member_peer(o)
        return pltpu.make_async_remote_copy(
            src_ref=dst.at[peer], dst_ref=dst.at[peer], send_sem=ss, recv_sem=rs.at[peer],
            device_id={"member": peer}, device_id_type=MESH)

    def nodes_of(q):
        return pl.ds(pl.multiple_of(q * quarter, quarter), quarter)

    def load_chunk(j):
        return pltpu.make_async_copy(latent.at[j], lat_buf.at[j], load_sem.at[j])

    w_copy = pltpu.make_async_copy(w_in, w_buf, load_sem.at[locals_])
    small = [
        pltpu.make_async_copy(src, dst, small_sem.at[n])
        for n, (src, dst) in enumerate((
            (cell_of_far, cell_of), (area_far, area), (target_far, target),
            (b_in_far, b_in), (w_out_far, w_out.at[pl.ds(0, variables)]), (b_out_far, b_out)))
    ]
    for copy in small[:3]:
        copy.start()
    w_copy.start()
    load_chunk(0).start()
    for copy in small[3:]:
        copy.start()
    for j in range(1, locals_):
        load_chunk(j).start()
    barrier = pltpu.get_barrier_semaphore()
    for o in range(1, places):
        pl.semaphore_signal(barrier, inc=1, device_id={"member": member_peer(o)}, device_id_type=MESH)
    for o in range(1, spaces):
        pl.semaphore_signal(barrier, inc=1, device_id={"space": space_peer(o)}, device_id_type=MESH)

    for copy in small[:3]:
        copy.wait()
    spare = LANES - variables
    match = lax.broadcasted_iota(jnp.int32, (cells, nodes), 0) == cell_of[...]
    hot[...] = jnp.where(match, 1.0, 0.0).astype(bf16)
    row = lax.broadcasted_iota(jnp.int32, (spare, nodes), 0)
    t_high, t_low = halves(target[...])
    a_high, a_low = halves(area[...])
    firsts = jnp.where(row == 0, 1.0, jnp.where(row == 1, a_high, 0.0))
    seconds = jnp.where(row == 1, a_low, 0.0)
    sums = dot_t(hot[...], jnp.concatenate([t_high, firsts], axis=0).astype(bf16))
    sums = sums + dot_t(hot[...], jnp.concatenate([t_low, seconds], axis=0).astype(bf16))
    lane = lax.broadcasted_iota(jnp.int32, (cells, LANES), 1)
    lows = pltpu.roll(halves(sums)[1], 2, 1)
    meta = jnp.where(lane < variables + 2, sums, lows)
    for n, value in enumerate(halves(jnp.sum(area[...], axis=1, keepdims=True))):
        meta = jnp.where(lane == variables + 4 + n, value, meta)
    for s in range(spaces):
        qsend[s] = meta[s * CELL_DEV:(s + 1) * CELL_DEV].astype(bf16)
    w_out[variables:, :] = jnp.zeros((spare, units), bf16)

    for copy in small[3:]:
        copy.wait()
    w_copy.wait()

    def forward(j, carry):
        load_chunk(j).wait()
        x = jnp.dot(lat_buf[j], w_buf[...], preferred_element_type=f32) + b_in[...]
        act[...] = (x * (0.5 * jnp.tanh(0.5 * x) + 0.5)).astype(bf16)
        slope_buf[j] = x.astype(bf16)
        bias = jnp.concatenate([b_out[...], jnp.zeros((1, spare), f32)], axis=1)
        rounded = (dot_t(act[...], w_out[...]) + bias).astype(bf16)
        pcat[:, pl.ds(pl.multiple_of(j * LANES, LANES), LANES)] = rounded
        for q in range(places):
            psend[q, j] = rounded[q * quarter:(q + 1) * quarter].astype(f32).T[:variables].astype(bf16)

        @pl.when(j == 0)
        def _():
            pl.semaphore_wait(barrier, places + spaces - 2)

        for o in range(1, places):
            pltpu.make_async_remote_copy(
                src_ref=psend.at[member_peer(o), j], dst_ref=precv.at[mm, j], send_sem=ps_sem, recv_sem=pr_sem,
                device_id={"member": member_peer(o)}, device_id_type=MESH).start()

        @pl.when(j == 0)
        def _():
            for o in range(1, spaces):
                to_space(qsend.at[space_peer(o)], qrecv, qs_sem, qr_sem, o).start()

        return carry

    def spread(src, dst, ss, rs, lanes):
        sums = jnp.dot(hot[...], pcat[:, lanes], preferred_element_type=f32).astype(bf16)
        for s in range(spaces):
            src[s] = sums[s * CELL_DEV:(s + 1) * CELL_DEV]
        for o in range(1, spaces):
            to_space(src.at[space_peer(o)], dst, ss, rs, o).start()

    ahead = (locals_ - 1) * LANES
    lax.fori_loop(0, locals_ - 1, forward, 0)
    spread(csend, crecv, cs_sem, cr_sem, slice(0, ahead))
    forward(locals_ - 1, 0)
    spread(zsend, zrecv, zs_sem, zr_sem, slice(ahead, ahead + LANES))

    def turn(n, carry):
        at = pl.ds(pl.multiple_of(n * COLS, COLS), COLS)
        turned[:, at] = w_buf[at, :].T
        return carry

    lax.fori_loop(0, width // COLS, turn, 0)
    for q in range(places):
        at = slice(q * quarter, (q + 1) * quarter)
        turned_hot[at, :] = hot[:, at].astype(f32).T.astype(bf16)

    qrecv[ms] = qsend[ms]
    all_spaces(qrecv, qs_sem, qr_sem).wait_recv()
    meta = qrecv[0].astype(f32)
    for s in range(1, spaces):
        meta = meta + qrecv[s].astype(f32)
    cell_count = meta[:, variables:variables + 1] + meta[:, variables + 2:variables + 3]
    cell_area = meta[:, variables + 1:variables + 2] + meta[:, variables + 3:variables + 4]
    all_area = meta[0:1, variables + 4:variables + 5] + meta[0:1, variables + 5:variables + 6]
    divisor = jnp.maximum(cell_count, 1.0)
    cell_lane = lax.broadcasted_iota(jnp.int32, (CELL_DEV, LANES), 1)
    facts = jnp.where(cell_lane < variables, meta / divisor, jnp.where(cell_lane == variables, divisor, cell_area))
    facts = jnp.concatenate([facts] * locals_, axis=0).T
    cell_target = facts[:variables]
    lane_divisor = facts[variables:variables + 1]
    cell_weight = facts[variables + 1:variables + 2]

    def slopes(n, carry):
        j, at = lax.div(n, units // SLIM), pl.ds(pl.multiple_of(lax.rem(n, units // SLIM) * SLIM, SLIM), SLIM)
        x = slope_buf[j, :, at].astype(f32)
        s = 0.5 * jnp.tanh(0.5 * x) + 0.5
        slope_buf[j, :, at] = (s + x * s * (1.0 - s)).astype(bf16)
        return carry

    def average(src, near, far, means_buf, ss, rs):
        near[ms] = src[ms]
        far.wait_recv()
        total = near[0].astype(f32)
        for s in range(1, spaces):
            total = total + near[s].astype(f32)
        means_buf[mm] = (total / divisor).astype(bf16)
        for o in range(1, places):
            to_member(means_buf.at[mm], means_buf, ss, rs, o).start()

    average(csend, crecv, all_spaces(crecv, cs_sem, cr_sem), mrecv, ms_sem, mr_sem)
    average(zsend, zrecv, all_spaces(zrecv, zs_sem, zr_sem), nrecv, ns_sem, nr_sem)

    def members_of(place):
        parts = [mrecv[place, :, j * LANES:(j + 1) * LANES] for j in range(locals_ - 1)] + [nrecv[place]]
        return jnp.concatenate(parts, axis=0).astype(f32).T[:variables]

    precv[mm] = psend[mm]
    truths = target[:, nodes_of(mm)]
    weight = area[:, nodes_of(mm)]
    all_members(precv, ps_sem, pr_sem).wait_recv()

    def truth_step(m, total):
        p = precv[lax.div(m, locals_), lax.rem(m, locals_)].astype(f32)
        p32[m] = p
        d = p - truths
        sq = jnp.sum(d * d, axis=0, keepdims=True) * (1.0 / variables) + epsilon
        r = lax.rsqrt(sq)
        grad[m] = d * (r * (1.0 / members))
        return total + sq * r

    def pair_step(m, total):
        pm = p32[m]
        factors = []
        for r in range(1, members // 2 + 1):
            share = 0.5 if 2 * r == members else 1.0
            d = pm - p32[lax.rem(m + r, members)]
            sq = jnp.sum(d * d, axis=0, keepdims=True) * (1.0 / variables) + epsilon
            inv = lax.rsqrt(sq)
            total = total + share * (sq * inv)
            factors.append(inv * (share * pair_scale))
        mine = grad[m]
        for r in range(1, members // 2 + 1):
            k = lax.rem(m + r, members)
            part = (pm - p32[k]) * factors[r - 1]
            mine = mine - part
            grad[k] = grad[k] + part
        grad[m] = mine
        return total

    zero = jnp.zeros((1, quarter), f32)
    truth_total = lax.fori_loop(0, members, truth_step, zero)
    pair_total = lax.fori_loop(0, members, pair_step, zero)
    fine_loss = weight * (truth_total * (1.0 / members) - pair_total * pair_scale)
    scale = weight * (1.0 / variables)

    def send_grads(o):
        peer = member_peer(o)
        for j in range(locals_):
            gsend[peer, j] = (grad[peer * locals_ + j] * scale).astype(bf16)
        to_member(gsend.at[peer], grecv, gs_sem, gr_sem.at[mm], o).start()

    send_grads(1)
    for j in range(locals_):
        grecv[mm, j] = (grad[mm * locals_ + j] * scale).astype(bf16)

    if places > 2:
        send_grads(2)

    own = members_of(mm)
    all_members(mrecv, ms_sem, mr_sem).wait_recv()
    all_members(nrecv, ns_sem, nr_sem).wait_recv()
    d = own - cell_target
    sq = jnp.sum(d * d, axis=0, keepdims=True) * (1.0 / variables) + epsilon
    inv = lax.rsqrt(sq)
    coarse = d * (inv * (1.0 / members))
    coarse_dist = sq * inv * (1.0 / members)
    for o in range(places):
        theirs = members_of(member_peer(o)) if o else own
        for r in range(locals_):
            if o == 0 and r == 0:
                continue
            d = own - (pltpu.roll(theirs, r * CELL_DEV, 1) if r else theirs)
            sq = jnp.sum(d * d, axis=0, keepdims=True) * (1.0 / variables) + epsilon
            inv = lax.rsqrt(sq)
            coarse = coarse - d * (inv * pair_scale)
            coarse_dist = coarse_dist - sq * inv * (0.5 * pair_scale)
    per_cell = coarse * (cell_weight * (1.0 / variables)) / lane_divisor
    per_cell = jnp.concatenate([per_cell, jnp.zeros((spare, locals_ * CELL_DEV), f32)], axis=0).T.astype(bf16)
    for j in range(locals_):
        dsend[:, j * LANES:(j + 1) * LANES] = per_cell[j * CELL_DEV:(j + 1) * CELL_DEV]
    for o in range(1, spaces):
        to_space(dsend, drecv, ds_sem, dr_sem, o).start()
    drecv[ms] = dsend[...]
    coarse_loss = jnp.sum(cell_weight * coarse_dist, axis=1, keepdims=True)

    row = lax.broadcasted_iota(jnp.int32, (8, LANES), 0)
    lspace[ms] = jnp.where(row == 0, jnp.sum(fine_loss, axis=1, keepdims=True), coarse_loss)
    for o in range(1, spaces):
        to_space(lspace.at[ms], lspace, ts_sem, tr_sem, o).start()
    for o in range(3, places):
        send_grads(o)
    lax.fori_loop(0, locals_ * (units // SLIM), slopes, 0)

    all_spaces(drecv, ds_sem, dr_sem).wait_recv()
    factor = scaling / all_area

    def upstream(i):
        q = lax.rem(mm + 1 + i, places)
        pieces = drecv[...].reshape(cells, locals_ * LANES)
        coarse_part = jnp.dot(turned_hot[nodes_of(q), :], pieces, preferred_element_type=f32)
        blank = jnp.zeros((spare, quarter), f32)
        for j in range(locals_):
            fine = jnp.concatenate([grecv[q, j].astype(f32), blank], axis=0).T
            up_buf[j * quarter:(j + 1) * quarter, :] = (
                fine + coarse_part[:, j * LANES:(j + 1) * LANES]).astype(bf16)

    def hidden_to(pg, i):
        h = jnp.dot(up_buf[...], w_out[...], preferred_element_type=f32)
        slope = slope_buf[:, nodes_of(lax.rem(mm + 1 + i, places)), :].reshape(rows, units)
        pg[...] = (h * slope.astype(f32)).astype(bf16)

    def finish(i):
        upstream(i)
        hidden_to(act, i)
        g = jnp.dot(act[...], turned[...], preferred_element_type=f32)
        early[i - 1] = (g * factor).astype(bf16).reshape(locals_, quarter, width)

    all_spaces(lspace, ts_sem, tr_sem).wait_recv()
    loss = lspace[0]
    for s in range(1, spaces):
        loss = loss + lspace[s]
    lmem[mm] = loss
    for o in range(1, places):
        to_member(lmem.at[mm], lmem, ls_sem, lr_sem, o).start()
    finish(places - 1)

    def arrived(n, carry):
        i = places - 2 - n
        from_member(grecv, gs_sem, gr_sem, i + 1).wait_recv()
        finish(i)
        return carry

    lax.fori_loop(0, places - 2, arrived, 0)
    from_member(grecv, gs_sem, gr_sem, 1).wait_recv()
    upstream(0)
    hidden_to(pg_out, 0)

    all_members(lmem, ls_sem, lr_sem).wait_recv()
    loss = lmem[0]
    for m in range(1, places):
        loss = loss + lmem[m]
    stats_out[...] = jnp.where(row == 2, all_area, loss)

    all_members(psend, ps_sem, pr_sem).wait_send()
    all_members(mrecv, ms_sem, mr_sem).wait_send()
    all_members(nrecv, ns_sem, nr_sem).wait_send()
    all_members(gsend, gs_sem, gr_sem.at[mm]).wait_send()
    all_members(lmem, ls_sem, lr_sem).wait_send()
    all_spaces(qsend, qs_sem, qr_sem).wait_send()
    all_spaces(csend, cs_sem, cr_sem).wait_send()
    all_spaces(zsend, zs_sem, zr_sem).wait_send()
    all_spaces(drecv, ds_sem, dr_sem).wait_send()
    all_spaces(lspace, ts_sem, tr_sem).wait_send()


def backward(places, scaling, early, pg, turned, stats, latent_grad, scores_out, last, scores, store_sem):
    locals_, quarter, width = last.shape
    mm = lax.axis_index("member")

    def nodes_of(i):
        q = lax.rem(mm + 1 + i, places)
        return pl.ds(pl.multiple_of(q * quarter, quarter), quarter)

    def store(i):
        return pltpu.make_async_copy(early.at[i - 1], latent_grad.at[:, nodes_of(i), :], store_sem.at[i - 1])

    def store_last(n):
        at = pl.ds(pl.multiple_of(n * COLS, COLS), COLS)
        return pltpu.make_async_copy(
            last.at[:, :, at], latent_grad.at[:, nodes_of(0), at], store_sem.at[places - 1 + n])

    for i in range(1, places):
        store(i).start()
    all_area = stats[2:3, 0:1]
    factor = scaling / all_area
    both = stats[...] / all_area
    scores[0] = both[0, 0]
    scores[1] = both[1, 0]
    score_copy = pltpu.make_async_copy(scores, scores_out, store_sem.at[places - 1 + width // COLS])
    score_copy.start()

    def outputs(n, carry):
        at = pl.ds(pl.multiple_of(n * COLS, COLS), COLS)
        g = jnp.dot(pg[...], turned[:, at], preferred_element_type=f32)
        last[:, :, at] = (g * factor).astype(bf16).reshape(locals_, quarter, COLS)
        store_last(n).start()
        return carry

    lax.fori_loop(0, width // COLS, outputs, 0)
    score_copy.wait()
    for i in range(1, places):
        store(i).wait()
    for n in range(width // COLS):
        store_last(n).wait()


def solution(mesh):
    spaces, places = mesh.shape["space"], mesh.shape["member"]

    def shards(latent, w_in, b_in, w_out, b_out, target, area, cell_of):
        locals_, nodes, width = latent.shape
        units, variables = w_out.shape
        quarter = nodes // places
        cells = CELL_DEV * spaces
        members = locals_ * places
        anywhere = pl.BlockSpec(memory_space=pl.ANY)
        inside = pl.BlockSpec(memory_space=pltpu.VMEM)
        single = pltpu.SemaphoreType.DMA
        rows = locals_ * quarter
        scaling = loss_scale * (nodes * spaces)
        early, pg, turned, stats = pl.pallas_call(
            functools.partial(exchange, spaces, places, scaling),
            out_shape=(
                pltpu.VMEM((places - 1, locals_, quarter, width), bf16),
                pltpu.VMEM((rows, units), bf16),
                pltpu.VMEM((units, width), bf16),
                pltpu.VMEM((8, LANES), f32),
            ),
            in_specs=[anywhere] * 8,
            out_specs=(inside, inside, inside, inside),
            scratch_shapes=[
                pltpu.VMEM((1, units), f32),
                pltpu.VMEM((LANES, units), bf16),
                pltpu.VMEM((1, variables), f32),
                pltpu.VMEM((variables, nodes), f32),
                pltpu.VMEM((1, nodes), f32),
                pltpu.VMEM((1, nodes), jnp.int32),
                pltpu.VMEM((locals_, nodes, width), bf16),
                pltpu.VMEM((width, units), bf16),
                pltpu.VMEM((locals_, nodes, units), bf16),
                pltpu.VMEM((rows, units), bf16),
                pltpu.VMEM((places, locals_, variables, quarter), bf16),
                pltpu.VMEM((places, locals_, variables, quarter), bf16),
                pltpu.VMEM((members, variables, quarter), f32),
                pltpu.VMEM((members, variables, quarter), f32),
                pltpu.VMEM((places, locals_, variables, quarter), bf16),
                pltpu.VMEM((places, locals_, variables, quarter), bf16),
                pltpu.VMEM((cells, nodes), bf16),
                pltpu.VMEM((nodes, cells), bf16),
                pltpu.VMEM((nodes, locals_ * LANES), bf16),
                pltpu.VMEM((spaces, CELL_DEV, LANES), bf16),
                pltpu.VMEM((spaces, CELL_DEV, LANES), bf16),
                pltpu.VMEM((spaces, CELL_DEV, (locals_ - 1) * LANES), bf16),
                pltpu.VMEM((spaces, CELL_DEV, (locals_ - 1) * LANES), bf16),
                pltpu.VMEM((spaces, CELL_DEV, LANES), bf16),
                pltpu.VMEM((spaces, CELL_DEV, LANES), bf16),
                pltpu.VMEM((places, CELL_DEV, (locals_ - 1) * LANES), bf16),
                pltpu.VMEM((places, CELL_DEV, LANES), bf16),
                pltpu.VMEM((CELL_DEV, locals_ * LANES), bf16),
                pltpu.VMEM((spaces, CELL_DEV, locals_ * LANES), bf16),
                pltpu.VMEM((rows, LANES), bf16),
                pltpu.VMEM((places, 8, LANES), f32),
                pltpu.VMEM((spaces, 8, LANES), f32),
                pltpu.SemaphoreType.DMA((locals_ + 1,)),
                pltpu.SemaphoreType.DMA((6,)),
                single, single, single, pltpu.SemaphoreType.DMA((places,)),
            ]
            + [single] * 16,
            compiler_params=pltpu.CompilerParams(
                collective_id=0, has_side_effects=True, vmem_limit_bytes=36 * 2**20
            ),
            name="exchange",
        )(*map(in_hbm, (latent, w_in, b_in[None], w_out.T, b_out[None], target.T, area[None], cell_of[None])))

        latent_grad, scores = pl.pallas_call(
            functools.partial(backward, places, scaling),
            out_shape=(
                jax.ShapeDtypeStruct((locals_, nodes, width), bf16),
                jax.ShapeDtypeStruct((2,), f32),
            ),
            in_specs=[inside] * 4,
            out_specs=(anywhere, anywhere),
            scratch_shapes=[
                pltpu.VMEM((locals_, quarter, width), bf16),
                pltpu.SMEM((2,), f32),
                pltpu.SemaphoreType.DMA((places + width // COLS,)),
            ],
            compiler_params=pltpu.CompilerParams(vmem_limit_bytes=16 * 2**20),
            name="backward",
        )(early, pg, turned, stats)
        return latent_grad, scores

    in_specs = (
        P("member", "space", None),
        P(),
        P(),
        P(),
        P(),
        P("space", None),
        P("space"),
        P("space"),
    )
    out_specs = (P("member", "space", None), P())
    return jax.shard_map(shards, mesh=mesh, in_specs=in_specs, out_specs=out_specs, check_vma=False)
```

```python
import functools

import jax
import jax.numpy as jnp
from jax import lax
from jax.experimental import pallas as pl
from jax.experimental.pallas import tpu as pltpu
from jax.sharding import PartitionSpec as P

CELL_DEV = 32
COLS = 512
SLIM = 256
LANES = 128

epsilon = 1e-05
loss_scale = 4096.0
bf16, f32 = jnp.bfloat16, jnp.float32
MESH = pl.DeviceIdType.MESH


def in_hbm(value):
    return pltpu.with_memory_space_constraint(value, pltpu.HBM)


def dot_t(a, b):
    return lax.dot_general(a, b, (((1,), (1,)), ((), ())), preferred_element_type=f32)


def halves(value):
    high = value.astype(bf16).astype(f32)
    return high, value - high


def exchange(spaces, places, scaling, latent, w_in, b_in_far, w_out_far, b_out_far, target_far, area_far,
             cell_of_far,
             early, pg_out, turned, stats_out,
             b_in, w_out, b_out, target, area, cell_of, lat_buf, w_buf, slope_buf, act,
             psend, precv, p32, grad, gsend, grecv, hot, turned_hot, pcat, qsend, qrecv, csend, crecv,
             zsend, zrecv, mrecv, nrecv, dsend, drecv, up_buf, lmem, lspace,
             load_sem, small_sem, ps_sem, pr_sem, gs_sem, gr_sem, qs_sem, qr_sem, cs_sem, cr_sem,
             zs_sem, zr_sem, ms_sem, mr_sem, ns_sem, nr_sem, ds_sem, dr_sem, ls_sem, lr_sem, ts_sem, tr_sem):
    ms = lax.axis_index("space")
    mm = lax.axis_index("member")
    locals_, nodes, width = lat_buf.shape
    quarter = nodes // places
    units = w_buf.shape[1]
    variables = target.shape[0]
    members = locals_ * places
    rows = locals_ * quarter
    cells = CELL_DEV * spaces
    pair_scale = 1.0 / (members * (members - 1))

    def member_peer(o):
        return lax.rem(mm + o, places)

    def space_peer(o):
        return lax.rem(ms + o, spaces)

    def to_member(src, dst, ss, rs, o):
        return pltpu.make_async_remote_copy(
            src_ref=src, dst_ref=dst.at[mm], send_sem=ss, recv_sem=rs,
            device_id={"member": member_peer(o)}, device_id_type=MESH)

    def to_space(src, dst, ss, rs, o):
        return pltpu.make_async_remote_copy(
            src_ref=src, dst_ref=dst.at[ms], send_sem=ss, recv_sem=rs,
            device_id={"space": space_peer(o)}, device_id_type=MESH)

    def all_members(dst, ss, rs):
        part = dst.at[pl.ds(0, places - 1)]
        return pltpu.make_async_remote_copy(
            src_ref=part, dst_ref=part, send_sem=ss, recv_sem=rs,
            device_id={"member": member_peer(1)}, device_id_type=MESH)

    def all_spaces(dst, ss, rs):
        part = dst.at[pl.ds(0, spaces - 1)]
        return pltpu.make_async_remote_copy(
            src_ref=part, dst_ref=part, send_sem=ss, recv_sem=rs,
            device_id={"space": space_peer(1)}, device_id_type=MESH)

    def from_member(dst, ss, rs, o):
        peer = member_peer(o)
        return pltpu.make_async_remote_copy(
            src_ref=dst.at[peer], dst_ref=dst.at[peer], send_sem=ss, recv_sem=rs.at[peer],
            device_id={"member": peer}, device_id_type=MESH)

    def nodes_of(q):
        return pl.ds(pl.multiple_of(q * quarter, quarter), quarter)

    def load_chunk(j):
        return pltpu.make_async_copy(latent.at[j], lat_buf.at[j], load_sem.at[j])

    w_copy = pltpu.make_async_copy(w_in, w_buf, load_sem.at[locals_])
    small = [
        pltpu.make_async_copy(src, dst, small_sem.at[n])
        for n, (src, dst) in enumerate((
            (cell_of_far, cell_of), (area_far, area), (target_far, target),
            (b_in_far, b_in), (w_out_far, w_out.at[pl.ds(0, variables)]), (b_out_far, b_out)))
    ]
    for copy in small[:3]:
        copy.start()
    w_copy.start()
    load_chunk(0).start()
    for copy in small[3:]:
        copy.start()
    for j in range(1, locals_):
        load_chunk(j).start()
    barrier = pltpu.get_barrier_semaphore()
    for o in range(1, places):
        pl.semaphore_signal(barrier, inc=1, device_id={"member": member_peer(o)}, device_id_type=MESH)
    for o in range(1, spaces):
        pl.semaphore_signal(barrier, inc=1, device_id={"space": space_peer(o)}, device_id_type=MESH)

    for copy in small[:3]:
        copy.wait()
    spare = LANES - variables
    match = lax.broadcasted_iota(jnp.int32, (cells, nodes), 0) == cell_of[...]
    hot[...] = jnp.where(match, 1.0, 0.0).astype(bf16)
    row = lax.broadcasted_iota(jnp.int32, (spare, nodes), 0)
    t_high, t_low = halves(target[...])
    a_high, a_low = halves(area[...])
    firsts = jnp.where(row == 0, 1.0, jnp.where(row == 1, a_high, 0.0))
    seconds = jnp.where(row == 1, a_low, 0.0)
    sums = dot_t(hot[...], jnp.concatenate([t_high, firsts, t_low, seconds], axis=0).astype(bf16))
    sums = sums[:, :LANES] + sums[:, LANES:]
    lane = lax.broadcasted_iota(jnp.int32, (cells, LANES), 1)
    lows = pltpu.roll(halves(sums)[1], 2, 1)
    meta = jnp.where(lane < variables + 2, sums, lows)
    for n, value in enumerate(halves(jnp.sum(area[...], axis=1, keepdims=True))):
        meta = jnp.where(lane == variables + 4 + n, value, meta)
    for s in range(spaces):
        qsend[s] = meta[s * CELL_DEV:(s + 1) * CELL_DEV].astype(bf16)
    w_out[variables:, :] = jnp.zeros((spare, units), bf16)

    for copy in small[3:]:
        copy.wait()
    w_copy.wait()

    def forward(j, carry):
        load_chunk(j).wait()
        x = jnp.dot(lat_buf[j], w_buf[...], preferred_element_type=f32) + b_in[...]
        x = x.astype(bf16)
        slope_buf[j] = x
        x = x * 0.5
        act[...] = x * jnp.tanh(x) + x
        bias = jnp.concatenate([b_out[...], jnp.zeros((1, spare), f32)], axis=1)
        rounded = (dot_t(act[...], w_out[...]) + bias).astype(bf16)
        pcat[:, pl.ds(pl.multiple_of(j * LANES, LANES), LANES)] = rounded
        for q in range(places):
            psend[q, j] = rounded[q * quarter:(q + 1) * quarter].astype(f32).T[:variables].astype(bf16)

        @pl.when(j == 0)
        def _():
            pl.semaphore_wait(barrier, places + spaces - 2)

        for o in range(1, places):
            pltpu.make_async_remote_copy(
                src_ref=psend.at[member_peer(o), j], dst_ref=precv.at[mm, j], send_sem=ps_sem, recv_sem=pr_sem,
                device_id={"member": member_peer(o)}, device_id_type=MESH).start()

        @pl.when(j == 0)
        def _():
            for o in range(1, spaces):
                to_space(qsend.at[space_peer(o)], qrecv, qs_sem, qr_sem, o).start()

        return carry

    def spread(src, dst, ss, rs, lanes):
        sums = jnp.dot(hot[...], pcat[:, lanes], preferred_element_type=f32).astype(bf16)
        for s in range(spaces):
            src[s] = sums[s * CELL_DEV:(s + 1) * CELL_DEV]
        for o in range(1, spaces):
            to_space(src.at[space_peer(o)], dst, ss, rs, o).start()

    ahead = (locals_ - 1) * LANES
    lax.fori_loop(0, locals_ - 1, forward, 0)
    spread(csend, crecv, cs_sem, cr_sem, slice(0, ahead))
    forward(locals_ - 1, 0)
    spread(zsend, zrecv, zs_sem, zr_sem, slice(ahead, ahead + LANES))

    def turn(n, carry):
        at = pl.ds(pl.multiple_of(n * COLS, COLS), COLS)
        turned[:, at] = w_buf[at, :].T
        return carry

    lax.fori_loop(0, width // COLS, turn, 0)
    for q in range(places):
        at = slice(q * quarter, (q + 1) * quarter)
        turned_hot[at, :] = hot[:, at].astype(f32).T.astype(bf16)

    qrecv[ms] = qsend[ms]
    all_spaces(qrecv, qs_sem, qr_sem).wait_recv()
    meta = qrecv[0].astype(f32)
    for s in range(1, spaces):
        meta = meta + qrecv[s].astype(f32)
    cell_count = meta[:, variables:variables + 1] + meta[:, variables + 2:variables + 3]
    cell_area = meta[:, variables + 1:variables + 2] + meta[:, variables + 3:variables + 4]
    all_area = meta[0:1, variables + 4:variables + 5] + meta[0:1, variables + 5:variables + 6]
    divisor = jnp.maximum(cell_count, 1.0)
    cell_lane = lax.broadcasted_iota(jnp.int32, (CELL_DEV, LANES), 1)
    facts = jnp.where(cell_lane < variables, meta / divisor, jnp.where(cell_lane == variables, divisor, cell_area))
    facts = jnp.concatenate([facts] * locals_, axis=0).T
    cell_target = facts[:variables]
    lane_divisor = facts[variables:variables + 1]
    cell_weight = facts[variables + 1:variables + 2]

    def slopes(n, carry):
        j, at = lax.div(n, units // SLIM), pl.ds(pl.multiple_of(lax.rem(n, units // SLIM) * SLIM, SLIM), SLIM)
        x = slope_buf[j, :, at].astype(f32)
        s = 0.5 * jnp.tanh(0.5 * x) + 0.5
        slope_buf[j, :, at] = (s + x * s * (1.0 - s)).astype(bf16)
        return carry

    def average(src, near, far, means_buf, ss, rs):
        near[ms] = src[ms]
        far.wait_recv()
        total = near[0].astype(f32)
        for s in range(1, spaces):
            total = total + near[s].astype(f32)
        means_buf[mm] = (total / divisor).astype(bf16)
        for o in range(1, places):
            to_member(means_buf.at[mm], means_buf, ss, rs, o).start()

    average(csend, crecv, all_spaces(crecv, cs_sem, cr_sem), mrecv, ms_sem, mr_sem)
    average(zsend, zrecv, all_spaces(zrecv, zs_sem, zr_sem), nrecv, ns_sem, nr_sem)

    def members_of(place):
        parts = [mrecv[place, :, j * LANES:(j + 1) * LANES] for j in range(locals_ - 1)] + [nrecv[place]]
        return jnp.concatenate(parts, axis=0).astype(f32).T[:variables]

    precv[mm] = psend[mm]
    truths = target[:, nodes_of(mm)]
    weight = area[:, nodes_of(mm)]
    all_members(precv, ps_sem, pr_sem).wait_recv()

    def truth_step(m, total):
        p = precv[lax.div(m, locals_), lax.rem(m, locals_)].astype(f32)
        p32[m] = p
        d = p - truths
        sq = jnp.sum(d * d, axis=0, keepdims=True) * (1.0 / variables) + epsilon
        r = lax.rsqrt(sq)
        grad[m] = d * (r * (1.0 / members))
        return total + sq * r

    def pair_step(m, total):
        pm = p32[m]
        factors = []
        for r in range(1, members // 2 + 1):
            share = 0.5 if 2 * r == members else 1.0
            d = pm - p32[lax.rem(m + r, members)]
            sq = jnp.sum(d * d, axis=0, keepdims=True) * (1.0 / variables) + epsilon
            inv = lax.rsqrt(sq)
            total = total + share * (sq * inv)
            factors.append(inv * (share * pair_scale))
        mine = grad[m]
        for r in range(1, members // 2 + 1):
            k = lax.rem(m + r, members)
            part = (pm - p32[k]) * factors[r - 1]
            mine = mine - part
            grad[k] = grad[k] + part
        grad[m] = mine
        return total

    zero = jnp.zeros((1, quarter), f32)
    truth_total = lax.fori_loop(0, members, truth_step, zero)
    pair_total = lax.fori_loop(0, members, pair_step, zero)
    fine_loss = weight * (truth_total * (1.0 / members) - pair_total * pair_scale)
    scale = weight * (1.0 / variables)

    def send_grads(o):
        peer = member_peer(o)
        for j in range(locals_):
            gsend[peer, j] = (grad[peer * locals_ + j] * scale).astype(bf16)
        to_member(gsend.at[peer], grecv, gs_sem, gr_sem.at[mm], o).start()

    send_grads(1)
    for j in range(locals_):
        grecv[mm, j] = (grad[mm * locals_ + j] * scale).astype(bf16)

    if places > 2:
        send_grads(2)

    own = members_of(mm)
    all_members(mrecv, ms_sem, mr_sem).wait_recv()
    all_members(nrecv, ns_sem, nr_sem).wait_recv()
    d = own - cell_target
    sq = jnp.sum(d * d, axis=0, keepdims=True) * (1.0 / variables) + epsilon
    inv = lax.rsqrt(sq)
    coarse = d * (inv * (1.0 / members))
    coarse_dist = sq * inv * (1.0 / members)
    for o in range(places):
        theirs = members_of(member_peer(o)) if o else own
        for r in range(locals_):
            if o == 0 and r == 0:
                continue
            d = own - (pltpu.roll(theirs, r * CELL_DEV, 1) if r else theirs)
            sq = jnp.sum(d * d, axis=0, keepdims=True) * (1.0 / variables) + epsilon
            inv = lax.rsqrt(sq)
            coarse = coarse - d * (inv * pair_scale)
            coarse_dist = coarse_dist - sq * inv * (0.5 * pair_scale)
    per_cell = coarse * (cell_weight * (1.0 / variables)) / lane_divisor
    per_cell = jnp.concatenate([per_cell, jnp.zeros((spare, locals_ * CELL_DEV), f32)], axis=0).T.astype(bf16)
    for j in range(locals_):
        dsend[:, j * LANES:(j + 1) * LANES] = per_cell[j * CELL_DEV:(j + 1) * CELL_DEV]
    for o in range(1, spaces):
        to_space(dsend, drecv, ds_sem, dr_sem, o).start()
    drecv[ms] = dsend[...]
    coarse_loss = jnp.sum(cell_weight * coarse_dist, axis=1, keepdims=True)

    row = lax.broadcasted_iota(jnp.int32, (8, LANES), 0)
    lspace[ms] = jnp.where(row == 0, jnp.sum(fine_loss, axis=1, keepdims=True), coarse_loss)
    for o in range(1, spaces):
        to_space(lspace.at[ms], lspace, ts_sem, tr_sem, o).start()
    for o in range(3, places):
        send_grads(o)
    lax.fori_loop(0, locals_ * (units // SLIM), slopes, 0)

    all_spaces(drecv, ds_sem, dr_sem).wait_recv()
    factor = scaling / all_area

    def upstream(i):
        q = lax.rem(mm + 1 + i, places)
        pieces = drecv[...].reshape(cells, locals_ * LANES)
        coarse_part = jnp.dot(turned_hot[nodes_of(q), :], pieces, preferred_element_type=f32)
        blank = jnp.zeros((spare, quarter), f32)
        for j in range(locals_):
            fine = jnp.concatenate([grecv[q, j].astype(f32), blank], axis=0).T
            up_buf[j * quarter:(j + 1) * quarter, :] = (
                fine + coarse_part[:, j * LANES:(j + 1) * LANES]).astype(bf16)

    def hidden_to(pg, i):
        h = jnp.dot(up_buf[...], w_out[...], preferred_element_type=f32)
        slope = slope_buf[:, nodes_of(lax.rem(mm + 1 + i, places)), :].reshape(rows, units)
        pg[...] = (h * slope.astype(f32)).astype(bf16)

    def finish(i):
        upstream(i)
        hidden_to(act, i)
        g = jnp.dot(act[...], turned[...], preferred_element_type=f32)
        early[i - 1] = (g * factor).astype(bf16).reshape(locals_, quarter, width)

    finish(places - 1)
    all_spaces(lspace, ts_sem, tr_sem).wait_recv()
    loss = lspace[0]
    for s in range(1, spaces):
        loss = loss + lspace[s]
    lmem[mm] = loss
    for o in range(1, places):
        to_member(lmem.at[mm], lmem, ls_sem, lr_sem, o).start()

    def arrived(n, carry):
        i = places - 2 - n
        from_member(grecv, gs_sem, gr_sem, i + 1).wait_recv()
        finish(i)
        return carry

    lax.fori_loop(0, places - 2, arrived, 0)
    from_member(grecv, gs_sem, gr_sem, 1).wait_recv()
    upstream(0)
    hidden_to(pg_out, 0)

    all_members(lmem, ls_sem, lr_sem).wait_recv()
    loss = lmem[0]
    for m in range(1, places):
        loss = loss + lmem[m]
    stats_out[...] = jnp.where(row == 2, all_area, loss)

    all_members(psend, ps_sem, pr_sem).wait_send()
    all_members(mrecv, ms_sem, mr_sem).wait_send()
    all_members(nrecv, ns_sem, nr_sem).wait_send()
    all_members(gsend, gs_sem, gr_sem.at[mm]).wait_send()
    all_members(lmem, ls_sem, lr_sem).wait_send()
    all_spaces(qsend, qs_sem, qr_sem).wait_send()
    all_spaces(csend, cs_sem, cr_sem).wait_send()
    all_spaces(zsend, zs_sem, zr_sem).wait_send()
    all_spaces(drecv, ds_sem, dr_sem).wait_send()
    all_spaces(lspace, ts_sem, tr_sem).wait_send()


def backward(places, scaling, early, pg, turned, stats, latent_grad, scores_out, last, scores, store_sem):
    locals_, quarter, width = last.shape
    mm = lax.axis_index("member")

    def nodes_of(i):
        q = lax.rem(mm + 1 + i, places)
        return pl.ds(pl.multiple_of(q * quarter, quarter), quarter)

    def store(i):
        return pltpu.make_async_copy(early.at[i - 1], latent_grad.at[:, nodes_of(i), :], store_sem.at[i - 1])

    def store_last(n):
        at = pl.ds(pl.multiple_of(n * COLS, COLS), COLS)
        return pltpu.make_async_copy(
            last.at[:, :, at], latent_grad.at[:, nodes_of(0), at], store_sem.at[places - 1 + n])

    for i in range(1, places):
        store(i).start()
    all_area = stats[2:3, 0:1]
    factor = scaling / all_area
    both = stats[...] / all_area
    scores[0] = both[0, 0]
    scores[1] = both[1, 0]
    score_copy = pltpu.make_async_copy(scores, scores_out, store_sem.at[places - 1 + width // COLS])
    score_copy.start()

    def outputs(n, carry):
        at = pl.ds(pl.multiple_of(n * COLS, COLS), COLS)
        g = jnp.dot(pg[...], turned[:, at], preferred_element_type=f32)
        last[:, :, at] = (g * factor).astype(bf16).reshape(locals_, quarter, COLS)
        store_last(n).start()
        return carry

    lax.fori_loop(0, width // COLS, outputs, 0)
    score_copy.wait()
    for i in range(1, places):
        store(i).wait()
    for n in range(width // COLS):
        store_last(n).wait()


def solution(mesh):
    spaces, places = mesh.shape["space"], mesh.shape["member"]

    def shards(latent, w_in, b_in, w_out, b_out, target, area, cell_of):
        locals_, nodes, width = latent.shape
        units, variables = w_out.shape
        quarter = nodes // places
        cells = CELL_DEV * spaces
        members = locals_ * places
        anywhere = pl.BlockSpec(memory_space=pl.ANY)
        inside = pl.BlockSpec(memory_space=pltpu.VMEM)
        single = pltpu.SemaphoreType.DMA
        rows = locals_ * quarter
        scaling = loss_scale * (nodes * spaces)
        early, pg, turned, stats = pl.pallas_call(
            functools.partial(exchange, spaces, places, scaling),
            out_shape=(
                pltpu.VMEM((places - 1, locals_, quarter, width), bf16),
                pltpu.VMEM((rows, units), bf16),
                pltpu.VMEM((units, width), bf16),
                pltpu.VMEM((8, LANES), f32),
            ),
            in_specs=[anywhere] * 8,
            out_specs=(inside, inside, inside, inside),
            scratch_shapes=[
                pltpu.VMEM((1, units), f32),
                pltpu.VMEM((LANES, units), bf16),
                pltpu.VMEM((1, variables), f32),
                pltpu.VMEM((variables, nodes), f32),
                pltpu.VMEM((1, nodes), f32),
                pltpu.VMEM((1, nodes), jnp.int32),
                pltpu.VMEM((locals_, nodes, width), bf16),
                pltpu.VMEM((width, units), bf16),
                pltpu.VMEM((locals_, nodes, units), bf16),
                pltpu.VMEM((rows, units), bf16),
                pltpu.VMEM((places, locals_, variables, quarter), bf16),
                pltpu.VMEM((places, locals_, variables, quarter), bf16),
                pltpu.VMEM((members, variables, quarter), f32),
                pltpu.VMEM((members, variables, quarter), f32),
                pltpu.VMEM((places, locals_, variables, quarter), bf16),
                pltpu.VMEM((places, locals_, variables, quarter), bf16),
                pltpu.VMEM((cells, nodes), bf16),
                pltpu.VMEM((nodes, cells), bf16),
                pltpu.VMEM((nodes, locals_ * LANES), bf16),
                pltpu.VMEM((spaces, CELL_DEV, LANES), bf16),
                pltpu.VMEM((spaces, CELL_DEV, LANES), bf16),
                pltpu.VMEM((spaces, CELL_DEV, (locals_ - 1) * LANES), bf16),
                pltpu.VMEM((spaces, CELL_DEV, (locals_ - 1) * LANES), bf16),
                pltpu.VMEM((spaces, CELL_DEV, LANES), bf16),
                pltpu.VMEM((spaces, CELL_DEV, LANES), bf16),
                pltpu.VMEM((places, CELL_DEV, (locals_ - 1) * LANES), bf16),
                pltpu.VMEM((places, CELL_DEV, LANES), bf16),
                pltpu.VMEM((CELL_DEV, locals_ * LANES), bf16),
                pltpu.VMEM((spaces, CELL_DEV, locals_ * LANES), bf16),
                pltpu.VMEM((rows, LANES), bf16),
                pltpu.VMEM((places, 8, LANES), f32),
                pltpu.VMEM((spaces, 8, LANES), f32),
                pltpu.SemaphoreType.DMA((locals_ + 1,)),
                pltpu.SemaphoreType.DMA((6,)),
                single, single, single, pltpu.SemaphoreType.DMA((places,)),
            ]
            + [single] * 16,
            compiler_params=pltpu.CompilerParams(
                collective_id=0, has_side_effects=True, vmem_limit_bytes=36 * 2**20
            ),
            name="exchange",
        )(*map(in_hbm, (latent, w_in, b_in[None], w_out.T, b_out[None], target.T, area[None], cell_of[None])))

        latent_grad, scores = pl.pallas_call(
            functools.partial(backward, places, scaling),
            out_shape=(
                jax.ShapeDtypeStruct((locals_, nodes, width), bf16),
                jax.ShapeDtypeStruct((2,), f32),
            ),
            in_specs=[inside] * 4,
            out_specs=(anywhere, anywhere),
            scratch_shapes=[
                pltpu.VMEM((locals_, quarter, width), bf16),
                pltpu.SMEM((2,), f32),
                pltpu.SemaphoreType.DMA((places + width // COLS,)),
            ],
            compiler_params=pltpu.CompilerParams(vmem_limit_bytes=16 * 2**20),
            name="backward",
        )(early, pg, turned, stats)
        return latent_grad, scores

    in_specs = (
        P("member", "space", None),
        P(),
        P(),
        P(),
        P(),
        P("space", None),
        P("space"),
        P("space"),
    )
    out_specs = (P("member", "space", None), P())
    return jax.shard_map(shards, mesh=mesh, in_specs=in_specs, out_specs=out_specs, check_vma=False)
```

```python
import functools

import jax
import jax.numpy as jnp
from jax import lax
from jax.experimental import pallas as pl
from jax.experimental.pallas import tpu as pltpu
from jax.sharding import PartitionSpec as P

CELL_DEV = 32
COLS = 512
SLIM = 256
LANES = 128

epsilon = 1e-05
loss_scale = 4096.0
bf16, f32 = jnp.bfloat16, jnp.float32
MESH = pl.DeviceIdType.MESH


def in_hbm(value):
    return pltpu.with_memory_space_constraint(value, pltpu.HBM)


def dot_t(a, b):
    return lax.dot_general(a, b, (((1,), (1,)), ((), ())), preferred_element_type=f32)


def halves(value):
    high = value.astype(bf16).astype(f32)
    return high, value - high


def exchange(spaces, places, scaling, latent, w_in, b_in_far, w_out_far, b_out_far, target_far, area_far,
             cell_of_far,
             early, pg_out, turned, stats_out,
             b_in, w_out, b_out, target, area, cell_of, lat_buf, w_buf, slope_buf, act,
             psend, precv, p32, grad, gsend, grecv, hot, turned_hot, pcat, qsend, qrecv, csend, crecv,
             zsend, zrecv, mrecv, nrecv, dsend, drecv, up_buf, lmem, lspace,
             load_sem, small_sem, ps_sem, pr_sem, gs_sem, gr_sem, qs_sem, qr_sem, cs_sem, cr_sem,
             zs_sem, zr_sem, ms_sem, mr_sem, ns_sem, nr_sem, ds_sem, dr_sem, ls_sem, lr_sem, ts_sem, tr_sem):
    ms = lax.axis_index("space")
    mm = lax.axis_index("member")
    locals_, nodes, width = lat_buf.shape
    quarter = nodes // places
    units = w_buf.shape[1]
    variables = target.shape[0]
    members = locals_ * places
    rows = locals_ * quarter
    cells = CELL_DEV * spaces
    pair_scale = 1.0 / (members * (members - 1))

    def member_peer(o):
        return lax.rem(mm + o, places)

    def space_peer(o):
        return lax.rem(ms + o, spaces)

    def to_member(src, dst, ss, rs, o):
        return pltpu.make_async_remote_copy(
            src_ref=src, dst_ref=dst.at[mm], send_sem=ss, recv_sem=rs,
            device_id={"member": member_peer(o)}, device_id_type=MESH)

    def to_space(src, dst, ss, rs, o):
        return pltpu.make_async_remote_copy(
            src_ref=src, dst_ref=dst.at[ms], send_sem=ss, recv_sem=rs,
            device_id={"space": space_peer(o)}, device_id_type=MESH)

    def all_members(dst, ss, rs):
        part = dst.at[pl.ds(0, places - 1)]
        return pltpu.make_async_remote_copy(
            src_ref=part, dst_ref=part, send_sem=ss, recv_sem=rs,
            device_id={"member": member_peer(1)}, device_id_type=MESH)

    def all_spaces(dst, ss, rs):
        part = dst.at[pl.ds(0, spaces - 1)]
        return pltpu.make_async_remote_copy(
            src_ref=part, dst_ref=part, send_sem=ss, recv_sem=rs,
            device_id={"space": space_peer(1)}, device_id_type=MESH)

    def from_member(dst, ss, rs, o):
        peer = member_peer(o)
        return pltpu.make_async_remote_copy(
            src_ref=dst.at[peer], dst_ref=dst.at[peer], send_sem=ss, recv_sem=rs.at[peer],
            device_id={"member": peer}, device_id_type=MESH)

    def nodes_of(q):
        return pl.ds(pl.multiple_of(q * quarter, quarter), quarter)

    def load_chunk(j):
        return pltpu.make_async_copy(latent.at[j], lat_buf.at[j], load_sem.at[j])

    w_copy = pltpu.make_async_copy(w_in, w_buf, load_sem.at[locals_])
    small = [
        pltpu.make_async_copy(src, dst, small_sem.at[n])
        for n, (src, dst) in enumerate((
            (cell_of_far, cell_of), (area_far, area), (target_far, target),
            (b_in_far, b_in), (w_out_far, w_out.at[pl.ds(0, variables)]), (b_out_far, b_out)))
    ]
    for copy in small[:3]:
        copy.start()
    w_copy.start()
    load_chunk(0).start()
    for copy in small[3:]:
        copy.start()
    for j in range(1, locals_):
        load_chunk(j).start()
    barrier = pltpu.get_barrier_semaphore()
    for o in range(1, places):
        pl.semaphore_signal(barrier, inc=1, device_id={"member": member_peer(o)}, device_id_type=MESH)
    for o in range(1, spaces):
        pl.semaphore_signal(barrier, inc=1, device_id={"space": space_peer(o)}, device_id_type=MESH)

    for copy in small[:3]:
        copy.wait()
    spare = LANES - variables
    match = lax.broadcasted_iota(jnp.int32, (cells, nodes), 0) == cell_of[...]
    hot[...] = jnp.where(match, 1.0, 0.0).astype(bf16)
    row = lax.broadcasted_iota(jnp.int32, (spare, nodes), 0)
    t_high, t_low = halves(target[...])
    a_high, a_low = halves(area[...])
    firsts = jnp.where(row == 0, 1.0, jnp.where(row == 1, a_high, 0.0))
    seconds = jnp.where(row == 1, a_low, 0.0)
    sums = dot_t(hot[...], jnp.concatenate([t_high, firsts, t_low, seconds], axis=0).astype(bf16))
    sums = sums[:, :LANES] + sums[:, LANES:]
    lane = lax.broadcasted_iota(jnp.int32, (cells, LANES), 1)
    lows = pltpu.roll(halves(sums)[1], 2, 1)
    meta = jnp.where(lane < variables + 2, sums, lows)
    for n, value in enumerate(halves(jnp.sum(area[...], axis=1, keepdims=True))):
        meta = jnp.where(lane == variables + 4 + n, value, meta)
    for s in range(spaces):
        qsend[s] = meta[s * CELL_DEV:(s + 1) * CELL_DEV].astype(bf16)
    w_out[variables:, :] = jnp.zeros((spare, units), bf16)

    for copy in small[3:]:
        copy.wait()
    w_copy.wait()

    def forward(j, carry):
        load_chunk(j).wait()
        x = jnp.dot(lat_buf[j], w_buf[...], preferred_element_type=f32) + b_in[...]
        x = x.astype(bf16)
        slope_buf[j] = x
        x = x * 0.5
        act[...] = x * jnp.tanh(x) + x
        bias = jnp.concatenate([b_out[...], jnp.zeros((1, spare), f32)], axis=1)
        rounded = (dot_t(act[...], w_out[...]) + bias).astype(bf16)
        pcat[:, pl.ds(pl.multiple_of(j * LANES, LANES), LANES)] = rounded
        for q in range(places):
            psend[q, j] = rounded[q * quarter:(q + 1) * quarter].astype(f32).T[:variables].astype(bf16)

        @pl.when(j == 0)
        def _():
            pl.semaphore_wait(barrier, places + spaces - 2)

        for o in range(1, places):
            pltpu.make_async_remote_copy(
                src_ref=psend.at[member_peer(o), j], dst_ref=precv.at[mm, j], send_sem=ps_sem, recv_sem=pr_sem,
                device_id={"member": member_peer(o)}, device_id_type=MESH).start()

        @pl.when(j == 0)
        def _():
            for o in range(1, spaces):
                to_space(qsend.at[space_peer(o)], qrecv, qs_sem, qr_sem, o).start()

        return carry

    def spread(src, dst, ss, rs, lanes):
        sums = jnp.dot(hot[...], pcat[:, lanes], preferred_element_type=f32).astype(bf16)
        for s in range(spaces):
            src[s] = sums[s * CELL_DEV:(s + 1) * CELL_DEV]
        for o in range(1, spaces):
            to_space(src.at[space_peer(o)], dst, ss, rs, o).start()

    ahead = (locals_ - 1) * LANES
    lax.fori_loop(0, locals_ - 1, forward, 0)
    spread(csend, crecv, cs_sem, cr_sem, slice(0, ahead))
    forward(locals_ - 1, 0)
    spread(zsend, zrecv, zs_sem, zr_sem, slice(ahead, ahead + LANES))

    qrecv[ms] = qsend[ms]
    all_spaces(qrecv, qs_sem, qr_sem).wait_recv()
    meta = qrecv[0].astype(f32)
    for s in range(1, spaces):
        meta = meta + qrecv[s].astype(f32)
    cell_count = meta[:, variables:variables + 1] + meta[:, variables + 2:variables + 3]
    cell_area = meta[:, variables + 1:variables + 2] + meta[:, variables + 3:variables + 4]
    all_area = meta[0:1, variables + 4:variables + 5] + meta[0:1, variables + 5:variables + 6]
    divisor = jnp.maximum(cell_count, 1.0)
    cell_lane = lax.broadcasted_iota(jnp.int32, (CELL_DEV, LANES), 1)
    facts = jnp.where(cell_lane < variables, meta / divisor, jnp.where(cell_lane == variables, divisor, cell_area))
    facts = jnp.concatenate([facts] * locals_, axis=0).T
    cell_target = facts[:variables]
    lane_divisor = facts[variables:variables + 1]
    cell_weight = facts[variables + 1:variables + 2]

    def slopes(n, carry):
        j, at = lax.div(n, units // SLIM), pl.ds(pl.multiple_of(lax.rem(n, units // SLIM) * SLIM, SLIM), SLIM)
        x = slope_buf[j, :, at].astype(f32)
        s = 0.5 * jnp.tanh(0.5 * x) + 0.5
        slope_buf[j, :, at] = (s + x * s * (1.0 - s)).astype(bf16)
        return carry

    def average(src, near, far, means_buf, ss, rs):
        near[ms] = src[ms]
        far.wait_recv()
        total = near[0].astype(f32)
        for s in range(1, spaces):
            total = total + near[s].astype(f32)
        means_buf[mm] = (total / divisor).astype(bf16)
        for o in range(1, places):
            to_member(means_buf.at[mm], means_buf, ss, rs, o).start()

    average(csend, crecv, all_spaces(crecv, cs_sem, cr_sem), mrecv, ms_sem, mr_sem)
    def turn(n, carry):
        at = pl.ds(pl.multiple_of(n * COLS, COLS), COLS)
        turned[:, at] = w_buf[at, :].T
        return carry

    lax.fori_loop(0, width // COLS, turn, 0)
    for q in range(places):
        at = slice(q * quarter, (q + 1) * quarter)
        turned_hot[at, :] = hot[:, at].astype(f32).T.astype(bf16)

    average(zsend, zrecv, all_spaces(zrecv, zs_sem, zr_sem), nrecv, ns_sem, nr_sem)

    def members_of(place):
        parts = [mrecv[place, :, j * LANES:(j + 1) * LANES] for j in range(locals_ - 1)] + [nrecv[place]]
        return jnp.concatenate(parts, axis=0).astype(f32).T[:variables]

    precv[mm] = psend[mm]
    truths = target[:, nodes_of(mm)]
    weight = area[:, nodes_of(mm)]
    all_members(precv, ps_sem, pr_sem).wait_recv()

    def truth_step(m, total):
        p = precv[lax.div(m, locals_), lax.rem(m, locals_)].astype(f32)
        p32[m] = p
        d = p - truths
        sq = jnp.sum(d * d, axis=0, keepdims=True) * (1.0 / variables) + epsilon
        r = lax.rsqrt(sq)
        grad[m] = d * (r * (1.0 / members))
        return total + sq * r

    def pair_step(m, total):
        pm = p32[m]
        factors = []
        for r in range(1, members // 2 + 1):
            share = 0.5 if 2 * r == members else 1.0
            d = pm - p32[lax.rem(m + r, members)]
            sq = jnp.sum(d * d, axis=0, keepdims=True) * (1.0 / variables) + epsilon
            inv = lax.rsqrt(sq)
            total = total + share * (sq * inv)
            factors.append(inv * (share * pair_scale))
        mine = grad[m]
        for r in range(1, members // 2 + 1):
            k = lax.rem(m + r, members)
            part = (pm - p32[k]) * factors[r - 1]
            mine = mine - part
            grad[k] = grad[k] + part
        grad[m] = mine
        return total

    zero = jnp.zeros((1, quarter), f32)
    truth_total = lax.fori_loop(0, members, truth_step, zero)
    pair_total = lax.fori_loop(0, members, pair_step, zero)
    fine_loss = weight * (truth_total * (1.0 / members) - pair_total * pair_scale)
    scale = weight * (1.0 / variables)

    def send_grads(o):
        peer = member_peer(o)
        for j in range(locals_):
            gsend[peer, j] = (grad[peer * locals_ + j] * scale).astype(bf16)
        to_member(gsend.at[peer], grecv, gs_sem, gr_sem.at[mm], o).start()

    send_grads(1)
    for j in range(locals_):
        grecv[mm, j] = (grad[mm * locals_ + j] * scale).astype(bf16)

    if places > 2:
        send_grads(2)

    own = members_of(mm)
    all_members(mrecv, ms_sem, mr_sem).wait_recv()
    all_members(nrecv, ns_sem, nr_sem).wait_recv()
    d = own - cell_target
    sq = jnp.sum(d * d, axis=0, keepdims=True) * (1.0 / variables) + epsilon
    inv = lax.rsqrt(sq)
    coarse = d * (inv * (1.0 / members))
    coarse_dist = sq * inv * (1.0 / members)
    for o in range(places):
        theirs = members_of(member_peer(o)) if o else own
        for r in range(locals_):
            if o == 0 and r == 0:
                continue
            d = own - (pltpu.roll(theirs, r * CELL_DEV, 1) if r else theirs)
            sq = jnp.sum(d * d, axis=0, keepdims=True) * (1.0 / variables) + epsilon
            inv = lax.rsqrt(sq)
            coarse = coarse - d * (inv * pair_scale)
            coarse_dist = coarse_dist - sq * inv * (0.5 * pair_scale)
    per_cell = coarse * (cell_weight * (1.0 / variables)) / lane_divisor
    per_cell = jnp.concatenate([per_cell, jnp.zeros((spare, locals_ * CELL_DEV), f32)], axis=0).T.astype(bf16)
    for j in range(locals_):
        dsend[:, j * LANES:(j + 1) * LANES] = per_cell[j * CELL_DEV:(j + 1) * CELL_DEV]
    for o in range(1, spaces):
        to_space(dsend, drecv, ds_sem, dr_sem, o).start()
    drecv[ms] = dsend[...]
    coarse_loss = jnp.sum(cell_weight * coarse_dist, axis=1, keepdims=True)

    row = lax.broadcasted_iota(jnp.int32, (8, LANES), 0)
    lspace[ms] = jnp.where(row == 0, jnp.sum(fine_loss, axis=1, keepdims=True), coarse_loss)
    for o in range(1, spaces):
        to_space(lspace.at[ms], lspace, ts_sem, tr_sem, o).start()
    for o in range(3, places):
        send_grads(o)
    lax.fori_loop(0, locals_ * (units // SLIM), slopes, 0)

    all_spaces(drecv, ds_sem, dr_sem).wait_recv()
    factor = scaling / all_area

    def upstream(i):
        q = lax.rem(mm + 1 + i, places)
        pieces = drecv[...].reshape(cells, locals_ * LANES)
        coarse_part = jnp.dot(turned_hot[nodes_of(q), :], pieces, preferred_element_type=f32)
        blank = jnp.zeros((spare, quarter), f32)
        for j in range(locals_):
            fine = jnp.concatenate([grecv[q, j].astype(f32), blank], axis=0).T
            up_buf[j * quarter:(j + 1) * quarter, :] = (
                fine + coarse_part[:, j * LANES:(j + 1) * LANES]).astype(bf16)

    def hidden_to(pg, i):
        h = jnp.dot(up_buf[...], w_out[...], preferred_element_type=f32)
        slope = slope_buf[:, nodes_of(lax.rem(mm + 1 + i, places)), :].reshape(rows, units)
        pg[...] = (h * slope.astype(f32)).astype(bf16)

    def finish(i):
        upstream(i)
        hidden_to(act, i)
        g = jnp.dot(act[...], turned[...], preferred_element_type=f32)
        early[i - 1] = (g * factor).astype(bf16).reshape(locals_, quarter, width)

    finish(places - 1)
    all_spaces(lspace, ts_sem, tr_sem).wait_recv()
    loss = lspace[0]
    for s in range(1, spaces):
        loss = loss + lspace[s]
    lmem[mm] = loss
    for o in range(1, places):
        to_member(lmem.at[mm], lmem, ls_sem, lr_sem, o).start()

    def arrived(n, carry):
        i = places - 2 - n
        from_member(grecv, gs_sem, gr_sem, i + 1).wait_recv()
        finish(i)
        return carry

    lax.fori_loop(0, places - 2, arrived, 0)
    from_member(grecv, gs_sem, gr_sem, 1).wait_recv()
    upstream(0)
    hidden_to(pg_out, 0)

    all_members(lmem, ls_sem, lr_sem).wait_recv()
    loss = lmem[0]
    for m in range(1, places):
        loss = loss + lmem[m]
    stats_out[...] = jnp.where(row == 2, all_area, loss)

    all_members(psend, ps_sem, pr_sem).wait_send()
    all_members(mrecv, ms_sem, mr_sem).wait_send()
    all_members(nrecv, ns_sem, nr_sem).wait_send()
    all_members(gsend, gs_sem, gr_sem.at[mm]).wait_send()
    all_members(lmem, ls_sem, lr_sem).wait_send()
    all_spaces(qsend, qs_sem, qr_sem).wait_send()
    all_spaces(csend, cs_sem, cr_sem).wait_send()
    all_spaces(zsend, zs_sem, zr_sem).wait_send()
    all_spaces(drecv, ds_sem, dr_sem).wait_send()
    all_spaces(lspace, ts_sem, tr_sem).wait_send()


def backward(places, scaling, early, pg, turned, stats, latent_grad, scores_out, last, scores, store_sem):
    locals_, quarter, width = last.shape
    mm = lax.axis_index("member")

    def nodes_of(i):
        q = lax.rem(mm + 1 + i, places)
        return pl.ds(pl.multiple_of(q * quarter, quarter), quarter)

    def store(i):
        return pltpu.make_async_copy(early.at[i - 1], latent_grad.at[:, nodes_of(i), :], store_sem.at[i - 1])

    def store_last(n):
        at = pl.ds(pl.multiple_of(n * COLS, COLS), COLS)
        return pltpu.make_async_copy(
            last.at[:, :, at], latent_grad.at[:, nodes_of(0), at], store_sem.at[places - 1 + n])

    for i in range(1, places):
        store(i).start()
    all_area = stats[2:3, 0:1]
    factor = scaling / all_area
    both = stats[...] / all_area
    scores[0] = both[0, 0]
    scores[1] = both[1, 0]
    score_copy = pltpu.make_async_copy(scores, scores_out, store_sem.at[places - 1 + width // COLS])
    score_copy.start()

    def outputs(n, carry):
        at = pl.ds(pl.multiple_of(n * COLS, COLS), COLS)
        g = jnp.dot(pg[...], turned[:, at], preferred_element_type=f32)
        last[:, :, at] = (g * factor).astype(bf16).reshape(locals_, quarter, COLS)
        store_last(n).start()
        return carry

    lax.fori_loop(0, width // COLS, outputs, 0)
    score_copy.wait()
    for i in range(1, places):
        store(i).wait()
    for n in range(width // COLS):
        store_last(n).wait()


def solution(mesh):
    spaces, places = mesh.shape["space"], mesh.shape["member"]

    def shards(latent, w_in, b_in, w_out, b_out, target, area, cell_of):
        locals_, nodes, width = latent.shape
        units, variables = w_out.shape
        quarter = nodes // places
        cells = CELL_DEV * spaces
        members = locals_ * places
        anywhere = pl.BlockSpec(memory_space=pl.ANY)
        inside = pl.BlockSpec(memory_space=pltpu.VMEM)
        single = pltpu.SemaphoreType.DMA
        rows = locals_ * quarter
        scaling = loss_scale * (nodes * spaces)
        early, pg, turned, stats = pl.pallas_call(
            functools.partial(exchange, spaces, places, scaling),
            out_shape=(
                pltpu.VMEM((places - 1, locals_, quarter, width), bf16),
                pltpu.VMEM((rows, units), bf16),
                pltpu.VMEM((units, width), bf16),
                pltpu.VMEM((8, LANES), f32),
            ),
            in_specs=[anywhere] * 8,
            out_specs=(inside, inside, inside, inside),
            scratch_shapes=[
                pltpu.VMEM((1, units), f32),
                pltpu.VMEM((LANES, units), bf16),
                pltpu.VMEM((1, variables), f32),
                pltpu.VMEM((variables, nodes), f32),
                pltpu.VMEM((1, nodes), f32),
                pltpu.VMEM((1, nodes), jnp.int32),
                pltpu.VMEM((locals_, nodes, width), bf16),
                pltpu.VMEM((width, units), bf16),
                pltpu.VMEM((locals_, nodes, units), bf16),
                pltpu.VMEM((rows, units), bf16),
                pltpu.VMEM((places, locals_, variables, quarter), bf16),
                pltpu.VMEM((places, locals_, variables, quarter), bf16),
                pltpu.VMEM((members, variables, quarter), f32),
                pltpu.VMEM((members, variables, quarter), f32),
                pltpu.VMEM((places, locals_, variables, quarter), bf16),
                pltpu.VMEM((places, locals_, variables, quarter), bf16),
                pltpu.VMEM((cells, nodes), bf16),
                pltpu.VMEM((nodes, cells), bf16),
                pltpu.VMEM((nodes, locals_ * LANES), bf16),
                pltpu.VMEM((spaces, CELL_DEV, LANES), bf16),
                pltpu.VMEM((spaces, CELL_DEV, LANES), bf16),
                pltpu.VMEM((spaces, CELL_DEV, (locals_ - 1) * LANES), bf16),
                pltpu.VMEM((spaces, CELL_DEV, (locals_ - 1) * LANES), bf16),
                pltpu.VMEM((spaces, CELL_DEV, LANES), bf16),
                pltpu.VMEM((spaces, CELL_DEV, LANES), bf16),
                pltpu.VMEM((places, CELL_DEV, (locals_ - 1) * LANES), bf16),
                pltpu.VMEM((places, CELL_DEV, LANES), bf16),
                pltpu.VMEM((CELL_DEV, locals_ * LANES), bf16),
                pltpu.VMEM((spaces, CELL_DEV, locals_ * LANES), bf16),
                pltpu.VMEM((rows, LANES), bf16),
                pltpu.VMEM((places, 8, LANES), f32),
                pltpu.VMEM((spaces, 8, LANES), f32),
                pltpu.SemaphoreType.DMA((locals_ + 1,)),
                pltpu.SemaphoreType.DMA((6,)),
                single, single, single, pltpu.SemaphoreType.DMA((places,)),
            ]
            + [single] * 16,
            compiler_params=pltpu.CompilerParams(
                collective_id=0, has_side_effects=True, vmem_limit_bytes=36 * 2**20
            ),
            name="exchange",
        )(*map(in_hbm, (latent, w_in, b_in[None], w_out.T, b_out[None], target.T, area[None], cell_of[None])))

        latent_grad, scores = pl.pallas_call(
            functools.partial(backward, places, scaling),
            out_shape=(
                jax.ShapeDtypeStruct((locals_, nodes, width), bf16),
                jax.ShapeDtypeStruct((2,), f32),
            ),
            in_specs=[inside] * 4,
            out_specs=(anywhere, anywhere),
            scratch_shapes=[
                pltpu.VMEM((locals_, quarter, width), bf16),
                pltpu.SMEM((2,), f32),
                pltpu.SemaphoreType.DMA((places + width // COLS,)),
            ],
            compiler_params=pltpu.CompilerParams(vmem_limit_bytes=16 * 2**20),
            name="backward",
        )(early, pg, turned, stats)
        return latent_grad, scores

    in_specs = (
        P("member", "space", None),
        P(),
        P(),
        P(),
        P(),
        P("space", None),
        P("space"),
        P("space"),
    )
    out_specs = (P("member", "space", None), P())
    return jax.shard_map(shards, mesh=mesh, in_specs=in_specs, out_specs=out_specs, check_vma=False)
```

```python
import functools

import jax
import jax.numpy as jnp
from jax import lax
from jax.experimental import pallas as pl
from jax.experimental.pallas import tpu as pltpu
from jax.sharding import PartitionSpec as P

CELL_DEV = 32
COLS = 512
SLIM = 256
LANES = 128

epsilon = 1e-05
loss_scale = 4096.0
bf16, f32 = jnp.bfloat16, jnp.float32
MESH = pl.DeviceIdType.MESH


def in_hbm(value):
    return pltpu.with_memory_space_constraint(value, pltpu.HBM)


def dot_t(a, b):
    return lax.dot_general(a, b, (((1,), (1,)), ((), ())), preferred_element_type=f32)


def halves(value):
    high = value.astype(bf16).astype(f32)
    return high, value - high


def exchange(spaces, places, scaling, latent, w_in, b_in_far, w_out_far, b_out_far, target_far, area_far,
             cell_of_far,
             early, pg_out, turned, stats_out,
             b_in, w_out, b_out, target, area, cell_of, lat_buf, w_buf, slope_buf, act,
             psend, precv, p32, grad, gsend, grecv, hot, turned_hot, pcat, qsend, qrecv, csend, crecv,
             zsend, zrecv, mrecv, nrecv, dsend, drecv, up_buf, lmem, lspace,
             load_sem, small_sem, ps_sem, pr_sem, gs_sem, gr_sem, qs_sem, qr_sem, cs_sem, cr_sem,
             zs_sem, zr_sem, ms_sem, mr_sem, ns_sem, nr_sem, ds_sem, dr_sem, ls_sem, lr_sem, ts_sem, tr_sem):
    ms = lax.axis_index("space")
    mm = lax.axis_index("member")
    locals_, nodes, width = lat_buf.shape
    quarter = nodes // places
    units = w_buf.shape[1]
    variables = target.shape[0]
    members = locals_ * places
    rows = locals_ * quarter
    cells = CELL_DEV * spaces
    pair_scale = 1.0 / (members * (members - 1))

    def member_peer(o):
        return lax.rem(mm + o, places)

    def space_peer(o):
        return lax.rem(ms + o, spaces)

    def to_member(src, dst, ss, rs, o):
        return pltpu.make_async_remote_copy(
            src_ref=src, dst_ref=dst.at[mm], send_sem=ss, recv_sem=rs,
            device_id={"member": member_peer(o)}, device_id_type=MESH)

    def to_space(src, dst, ss, rs, o):
        return pltpu.make_async_remote_copy(
            src_ref=src, dst_ref=dst.at[ms], send_sem=ss, recv_sem=rs,
            device_id={"space": space_peer(o)}, device_id_type=MESH)

    def all_members(dst, ss, rs):
        part = dst.at[pl.ds(0, places - 1)]
        return pltpu.make_async_remote_copy(
            src_ref=part, dst_ref=part, send_sem=ss, recv_sem=rs,
            device_id={"member": member_peer(1)}, device_id_type=MESH)

    def all_spaces(dst, ss, rs):
        part = dst.at[pl.ds(0, spaces - 1)]
        return pltpu.make_async_remote_copy(
            src_ref=part, dst_ref=part, send_sem=ss, recv_sem=rs,
            device_id={"space": space_peer(1)}, device_id_type=MESH)

    def from_member(dst, ss, rs, o):
        peer = member_peer(o)
        return pltpu.make_async_remote_copy(
            src_ref=dst.at[peer], dst_ref=dst.at[peer], send_sem=ss, recv_sem=rs.at[peer],
            device_id={"member": peer}, device_id_type=MESH)

    def nodes_of(q):
        return pl.ds(pl.multiple_of(q * quarter, quarter), quarter)

    def load_chunk(j):
        return pltpu.make_async_copy(latent.at[j], lat_buf.at[j], load_sem.at[j])

    w_copy = pltpu.make_async_copy(w_in, w_buf, load_sem.at[locals_])
    small = [
        pltpu.make_async_copy(src, dst, small_sem.at[n])
        for n, (src, dst) in enumerate((
            (cell_of_far, cell_of), (area_far, area), (target_far, target),
            (b_in_far, b_in), (w_out_far, w_out.at[pl.ds(0, variables)]), (b_out_far, b_out)))
    ]
    for copy in small[:3]:
        copy.start()
    w_copy.start()
    load_chunk(0).start()
    for copy in small[3:]:
        copy.start()
    for j in range(1, locals_):
        load_chunk(j).start()
    barrier = pltpu.get_barrier_semaphore()
    for o in range(1, places):
        pl.semaphore_signal(barrier, inc=1, device_id={"member": member_peer(o)}, device_id_type=MESH)
    for o in range(1, spaces):
        pl.semaphore_signal(barrier, inc=1, device_id={"space": space_peer(o)}, device_id_type=MESH)

    for copy in small[:3]:
        copy.wait()
    spare = LANES - variables
    match = lax.broadcasted_iota(jnp.int32, (cells, nodes), 0) == cell_of[...]
    hot[...] = jnp.where(match, 1.0, 0.0).astype(bf16)
    row = lax.broadcasted_iota(jnp.int32, (spare, nodes), 0)
    t_high, t_low = halves(target[...])
    a_high, a_low = halves(area[...])
    firsts = jnp.where(row == 0, 1.0, jnp.where(row == 1, a_high, 0.0))
    seconds = jnp.where(row == 1, a_low, 0.0)
    sums = dot_t(hot[...], jnp.concatenate([t_high, firsts, t_low, seconds], axis=0).astype(bf16))
    sums = sums[:, :LANES] + sums[:, LANES:]
    lane = lax.broadcasted_iota(jnp.int32, (cells, LANES), 1)
    lows = pltpu.roll(halves(sums)[1], 2, 1)
    meta = jnp.where(lane < variables + 2, sums, lows)
    for n, value in enumerate(halves(jnp.sum(area[...], axis=1, keepdims=True))):
        meta = jnp.where(lane == variables + 4 + n, value, meta)
    for s in range(spaces):
        qsend[s] = meta[s * CELL_DEV:(s + 1) * CELL_DEV].astype(bf16)
    w_out[variables:, :] = jnp.zeros((spare, units), bf16)

    for copy in small[3:]:
        copy.wait()
    w_copy.wait()

    def forward(j, carry):
        load_chunk(j).wait()
        x = jnp.dot(lat_buf[j], w_buf[...], preferred_element_type=f32) + b_in[...]
        x = x.astype(bf16)
        slope_buf[j] = x
        x = x * 0.5
        act[...] = x * jnp.tanh(x) + x
        bias = jnp.concatenate([b_out[...], jnp.zeros((1, spare), f32)], axis=1)
        rounded = (dot_t(act[...], w_out[...]) + bias).astype(bf16)
        pcat[:, pl.ds(pl.multiple_of(j * LANES, LANES), LANES)] = rounded
        for q in range(places):
            psend[q, j] = rounded[q * quarter:(q + 1) * quarter].astype(f32).T[:variables].astype(bf16)

        @pl.when(j == 0)
        def _():
            pl.semaphore_wait(barrier, places + spaces - 2)

        for o in range(1, places):
            pltpu.make_async_remote_copy(
                src_ref=psend.at[member_peer(o), j], dst_ref=precv.at[mm, j], send_sem=ps_sem, recv_sem=pr_sem,
                device_id={"member": member_peer(o)}, device_id_type=MESH).start()

        @pl.when(j == 0)
        def _():
            for o in range(1, spaces):
                to_space(qsend.at[space_peer(o)], qrecv, qs_sem, qr_sem, o).start()

        return carry

    def spread(src, dst, ss, rs, lanes):
        sums = jnp.dot(hot[...], pcat[:, lanes], preferred_element_type=f32).astype(bf16)
        for s in range(spaces):
            src[s] = sums[s * CELL_DEV:(s + 1) * CELL_DEV]
        for o in range(1, spaces):
            to_space(src.at[space_peer(o)], dst, ss, rs, o).start()

    ahead = (locals_ - 1) * LANES
    lax.fori_loop(0, locals_ - 1, forward, 0)
    spread(csend, crecv, cs_sem, cr_sem, slice(0, ahead))
    forward(locals_ - 1, 0)
    spread(zsend, zrecv, zs_sem, zr_sem, slice(ahead, ahead + LANES))

    qrecv[ms] = qsend[ms]
    all_spaces(qrecv, qs_sem, qr_sem).wait_recv()
    meta = qrecv[0].astype(f32)
    for s in range(1, spaces):
        meta = meta + qrecv[s].astype(f32)
    cell_count = meta[:, variables:variables + 1] + meta[:, variables + 2:variables + 3]
    cell_area = meta[:, variables + 1:variables + 2] + meta[:, variables + 3:variables + 4]
    all_area = meta[0:1, variables + 4:variables + 5] + meta[0:1, variables + 5:variables + 6]
    divisor = jnp.maximum(cell_count, 1.0)
    cell_lane = lax.broadcasted_iota(jnp.int32, (CELL_DEV, LANES), 1)
    facts = jnp.where(cell_lane < variables, meta / divisor, jnp.where(cell_lane == variables, divisor, cell_area))
    facts = jnp.concatenate([facts] * locals_, axis=0).T
    cell_target = facts[:variables]
    lane_divisor = facts[variables:variables + 1]
    cell_weight = facts[variables + 1:variables + 2]

    def slopes(n, carry):
        j, at = lax.div(n, units // SLIM), pl.ds(pl.multiple_of(lax.rem(n, units // SLIM) * SLIM, SLIM), SLIM)
        x = slope_buf[j, :, at].astype(f32)
        s = 0.5 * jnp.tanh(0.5 * x) + 0.5
        slope_buf[j, :, at] = (s + x * s * (1.0 - s)).astype(bf16)
        return carry

    def average(src, near, far, count, rest, means_buf, ss, rs):
        near[ms] = src[ms]
        far.wait_recv()
        total = near[0].astype(f32)
        for s in range(1, spaces):
            total = total + near[s].astype(f32)
        means = (total / divisor).astype(bf16).astype(f32)
        packed = jnp.concatenate(rest + [means[:, j * LANES:j * LANES + variables] for j in range(count)], axis=1)
        sent = means_buf.shape[2]
        means_buf[mm] = packed[:, :sent].astype(bf16)
        for o in range(1, places):
            to_member(means_buf.at[mm], means_buf, ss, rs, o).start()
        return packed[:, sent:] if sent < packed.shape[1] else None

    rest = average(csend, crecv, all_spaces(crecv, cs_sem, cr_sem), locals_ - 1, [], mrecv, ms_sem, mr_sem)
    def turn(n, carry):
        at = pl.ds(pl.multiple_of(n * COLS, COLS), COLS)
        turned[:, at] = w_buf[at, :].T
        return carry

    lax.fori_loop(0, width // COLS, turn, 0)
    for q in range(places):
        at = slice(q * quarter, (q + 1) * quarter)
        turned_hot[at, :] = hot[:, at].astype(f32).T.astype(bf16)

    average(zsend, zrecv, all_spaces(zrecv, zs_sem, zr_sem), 1, [rest], nrecv, ns_sem, nr_sem)

    def members_of(place):
        packed = jnp.concatenate([mrecv[place].astype(f32), nrecv[place].astype(f32)], axis=1)
        parts = [packed[:, j * variables:(j + 1) * variables] for j in range(locals_)]
        return jnp.concatenate(parts, axis=0).T

    precv[mm] = psend[mm]
    truths = target[:, nodes_of(mm)]
    weight = area[:, nodes_of(mm)]
    all_members(precv, ps_sem, pr_sem).wait_recv()

    def truth_step(m, total):
        p = precv[lax.div(m, locals_), lax.rem(m, locals_)].astype(f32)
        p32[m] = p
        d = p - truths
        sq = jnp.sum(d * d, axis=0, keepdims=True) * (1.0 / variables) + epsilon
        r = lax.rsqrt(sq)
        grad[m] = d * (r * (1.0 / members))
        return total + sq * r

    def pair_step(m, total):
        pm = p32[m]
        factors = []
        for r in range(1, members // 2 + 1):
            share = 0.5 if 2 * r == members else 1.0
            d = pm - p32[lax.rem(m + r, members)]
            sq = jnp.sum(d * d, axis=0, keepdims=True) * (1.0 / variables) + epsilon
            inv = lax.rsqrt(sq)
            total = total + share * (sq * inv)
            factors.append(inv * (share * pair_scale))
        mine = grad[m]
        for r in range(1, members // 2 + 1):
            k = lax.rem(m + r, members)
            part = (pm - p32[k]) * factors[r - 1]
            mine = mine - part
            grad[k] = grad[k] + part
        grad[m] = mine
        return total

    zero = jnp.zeros((1, quarter), f32)
    truth_total = lax.fori_loop(0, members, truth_step, zero)
    pair_total = lax.fori_loop(0, members, pair_step, zero)
    fine_loss = weight * (truth_total * (1.0 / members) - pair_total * pair_scale)
    scale = weight * (1.0 / variables)

    def send_grads(o):
        peer = member_peer(o)
        for j in range(locals_):
            gsend[peer, j] = (grad[peer * locals_ + j] * scale).astype(bf16)
        to_member(gsend.at[peer], grecv, gs_sem, gr_sem.at[mm], o).start()

    send_grads(1)
    for j in range(locals_):
        grecv[mm, j] = (grad[mm * locals_ + j] * scale).astype(bf16)

    if places > 2:
        send_grads(2)

    own = members_of(mm)
    all_members(mrecv, ms_sem, mr_sem).wait_recv()
    all_members(nrecv, ns_sem, nr_sem).wait_recv()
    d = own - cell_target
    sq = jnp.sum(d * d, axis=0, keepdims=True) * (1.0 / variables) + epsilon
    inv = lax.rsqrt(sq)
    coarse = d * (inv * (1.0 / members))
    coarse_dist = sq * inv * (1.0 / members)
    for o in range(places):
        theirs = members_of(member_peer(o)) if o else own
        for r in range(locals_):
            if o == 0 and r == 0:
                continue
            d = own - (pltpu.roll(theirs, r * CELL_DEV, 1) if r else theirs)
            sq = jnp.sum(d * d, axis=0, keepdims=True) * (1.0 / variables) + epsilon
            inv = lax.rsqrt(sq)
            coarse = coarse - d * (inv * pair_scale)
            coarse_dist = coarse_dist - sq * inv * (0.5 * pair_scale)
    per_cell = coarse * (cell_weight * (1.0 / variables)) / lane_divisor
    per_cell = jnp.concatenate([per_cell, jnp.zeros((spare, locals_ * CELL_DEV), f32)], axis=0).T.astype(bf16)
    for j in range(locals_):
        dsend[:, j * LANES:(j + 1) * LANES] = per_cell[j * CELL_DEV:(j + 1) * CELL_DEV]
    for o in range(1, spaces):
        to_space(dsend, drecv, ds_sem, dr_sem, o).start()
    drecv[ms] = dsend[...]
    coarse_loss = jnp.sum(cell_weight * coarse_dist, axis=1, keepdims=True)

    row = lax.broadcasted_iota(jnp.int32, (8, LANES), 0)
    lspace[ms] = jnp.where(row == 0, jnp.sum(fine_loss, axis=1, keepdims=True), coarse_loss)
    for o in range(1, spaces):
        to_space(lspace.at[ms], lspace, ts_sem, tr_sem, o).start()
    for o in range(3, places):
        send_grads(o)
    lax.fori_loop(0, locals_ * (units // SLIM), slopes, 0)

    all_spaces(drecv, ds_sem, dr_sem).wait_recv()
    factor = scaling / all_area

    def upstream(i):
        q = lax.rem(mm + 1 + i, places)
        pieces = drecv[...].reshape(cells, locals_ * LANES)
        coarse_part = jnp.dot(turned_hot[nodes_of(q), :], pieces, preferred_element_type=f32)
        blank = jnp.zeros((spare, quarter), f32)
        for j in range(locals_):
            fine = jnp.concatenate([grecv[q, j].astype(f32), blank], axis=0).T
            up_buf[j * quarter:(j + 1) * quarter, :] = (
                fine + coarse_part[:, j * LANES:(j + 1) * LANES]).astype(bf16)

    def hidden_to(pg, i):
        h = jnp.dot(up_buf[...], w_out[...], preferred_element_type=f32)
        slope = slope_buf[:, nodes_of(lax.rem(mm + 1 + i, places)), :].reshape(rows, units)
        pg[...] = (h * slope.astype(f32)).astype(bf16)

    def finish(i):
        upstream(i)
        hidden_to(act, i)
        g = jnp.dot(act[...], turned[...], preferred_element_type=f32)
        early[i - 1] = (g * factor).astype(bf16).reshape(locals_, quarter, width)

    finish(places - 1)
    all_spaces(lspace, ts_sem, tr_sem).wait_recv()
    loss = lspace[0]
    for s in range(1, spaces):
        loss = loss + lspace[s]
    lmem[mm] = loss
    for o in range(1, places):
        to_member(lmem.at[mm], lmem, ls_sem, lr_sem, o).start()

    def arrived(n, carry):
        i = places - 2 - n
        from_member(grecv, gs_sem, gr_sem, i + 1).wait_recv()
        finish(i)
        return carry

    lax.fori_loop(0, places - 2, arrived, 0)
    from_member(grecv, gs_sem, gr_sem, 1).wait_recv()
    upstream(0)
    hidden_to(pg_out, 0)

    all_members(lmem, ls_sem, lr_sem).wait_recv()
    loss = lmem[0]
    for m in range(1, places):
        loss = loss + lmem[m]
    stats_out[...] = jnp.where(row == 2, all_area, loss)

    all_members(psend, ps_sem, pr_sem).wait_send()
    all_members(mrecv, ms_sem, mr_sem).wait_send()
    all_members(nrecv, ns_sem, nr_sem).wait_send()
    all_members(gsend, gs_sem, gr_sem.at[mm]).wait_send()
    all_members(lmem, ls_sem, lr_sem).wait_send()
    all_spaces(qsend, qs_sem, qr_sem).wait_send()
    all_spaces(csend, cs_sem, cr_sem).wait_send()
    all_spaces(zsend, zs_sem, zr_sem).wait_send()
    all_spaces(drecv, ds_sem, dr_sem).wait_send()
    all_spaces(lspace, ts_sem, tr_sem).wait_send()


def backward(places, scaling, early, pg, turned, stats, latent_grad, scores_out, last, scores, store_sem):
    locals_, quarter, width = last.shape
    mm = lax.axis_index("member")

    def nodes_of(i):
        q = lax.rem(mm + 1 + i, places)
        return pl.ds(pl.multiple_of(q * quarter, quarter), quarter)

    def store(i):
        return pltpu.make_async_copy(early.at[i - 1], latent_grad.at[:, nodes_of(i), :], store_sem.at[i - 1])

    def store_last(n):
        at = pl.ds(pl.multiple_of(n * COLS, COLS), COLS)
        return pltpu.make_async_copy(
            last.at[:, :, at], latent_grad.at[:, nodes_of(0), at], store_sem.at[places - 1 + n])

    for i in range(1, places):
        store(i).start()
    all_area = stats[2:3, 0:1]
    factor = scaling / all_area
    both = stats[...] / all_area
    scores[0] = both[0, 0]
    scores[1] = both[1, 0]
    score_copy = pltpu.make_async_copy(scores, scores_out, store_sem.at[places - 1 + width // COLS])
    score_copy.start()

    def outputs(n, carry):
        at = pl.ds(pl.multiple_of(n * COLS, COLS), COLS)
        g = jnp.dot(pg[...], turned[:, at], preferred_element_type=f32)
        last[:, :, at] = (g * factor).astype(bf16).reshape(locals_, quarter, COLS)
        store_last(n).start()
        return carry

    lax.fori_loop(0, width // COLS, outputs, 0)
    score_copy.wait()
    for i in range(1, places):
        store(i).wait()
    for n in range(width // COLS):
        store_last(n).wait()


def solution(mesh):
    spaces, places = mesh.shape["space"], mesh.shape["member"]

    def shards(latent, w_in, b_in, w_out, b_out, target, area, cell_of):
        locals_, nodes, width = latent.shape
        units, variables = w_out.shape
        quarter = nodes // places
        cells = CELL_DEV * spaces
        members = locals_ * places
        anywhere = pl.BlockSpec(memory_space=pl.ANY)
        inside = pl.BlockSpec(memory_space=pltpu.VMEM)
        single = pltpu.SemaphoreType.DMA
        rows = locals_ * quarter
        first = (locals_ - 1) * variables // LANES * LANES
        scaling = loss_scale * (nodes * spaces)
        early, pg, turned, stats = pl.pallas_call(
            functools.partial(exchange, spaces, places, scaling),
            out_shape=(
                pltpu.VMEM((places - 1, locals_, quarter, width), bf16),
                pltpu.VMEM((rows, units), bf16),
                pltpu.VMEM((units, width), bf16),
                pltpu.VMEM((8, LANES), f32),
            ),
            in_specs=[anywhere] * 8,
            out_specs=(inside, inside, inside, inside),
            scratch_shapes=[
                pltpu.VMEM((1, units), f32),
                pltpu.VMEM((LANES, units), bf16),
                pltpu.VMEM((1, variables), f32),
                pltpu.VMEM((variables, nodes), f32),
                pltpu.VMEM((1, nodes), f32),
                pltpu.VMEM((1, nodes), jnp.int32),
                pltpu.VMEM((locals_, nodes, width), bf16),
                pltpu.VMEM((width, units), bf16),
                pltpu.VMEM((locals_, nodes, units), bf16),
                pltpu.VMEM((rows, units), bf16),
                pltpu.VMEM((places, locals_, variables, quarter), bf16),
                pltpu.VMEM((places, locals_, variables, quarter), bf16),
                pltpu.VMEM((members, variables, quarter), f32),
                pltpu.VMEM((members, variables, quarter), f32),
                pltpu.VMEM((places, locals_, variables, quarter), bf16),
                pltpu.VMEM((places, locals_, variables, quarter), bf16),
                pltpu.VMEM((cells, nodes), bf16),
                pltpu.VMEM((nodes, cells), bf16),
                pltpu.VMEM((nodes, locals_ * LANES), bf16),
                pltpu.VMEM((spaces, CELL_DEV, LANES), bf16),
                pltpu.VMEM((spaces, CELL_DEV, LANES), bf16),
                pltpu.VMEM((spaces, CELL_DEV, (locals_ - 1) * LANES), bf16),
                pltpu.VMEM((spaces, CELL_DEV, (locals_ - 1) * LANES), bf16),
                pltpu.VMEM((spaces, CELL_DEV, LANES), bf16),
                pltpu.VMEM((spaces, CELL_DEV, LANES), bf16),
                pltpu.VMEM((places, CELL_DEV, first), bf16),
                pltpu.VMEM((places, CELL_DEV, locals_ * variables - first), bf16),
                pltpu.VMEM((CELL_DEV, locals_ * LANES), bf16),
                pltpu.VMEM((spaces, CELL_DEV, locals_ * LANES), bf16),
                pltpu.VMEM((rows, LANES), bf16),
                pltpu.VMEM((places, 8, LANES), f32),
                pltpu.VMEM((spaces, 8, LANES), f32),
                pltpu.SemaphoreType.DMA((locals_ + 1,)),
                pltpu.SemaphoreType.DMA((6,)),
                single, single, single, pltpu.SemaphoreType.DMA((places,)),
            ]
            + [single] * 16,
            compiler_params=pltpu.CompilerParams(
                collective_id=0, has_side_effects=True, vmem_limit_bytes=36 * 2**20
            ),
            name="exchange",
        )(*map(in_hbm, (latent, w_in, b_in[None], w_out.T, b_out[None], target.T, area[None], cell_of[None])))

        latent_grad, scores = pl.pallas_call(
            functools.partial(backward, places, scaling),
            out_shape=(
                jax.ShapeDtypeStruct((locals_, nodes, width), bf16),
                jax.ShapeDtypeStruct((2,), f32),
            ),
            in_specs=[inside] * 4,
            out_specs=(anywhere, anywhere),
            scratch_shapes=[
                pltpu.VMEM((locals_, quarter, width), bf16),
                pltpu.SMEM((2,), f32),
                pltpu.SemaphoreType.DMA((places + width // COLS,)),
            ],
            compiler_params=pltpu.CompilerParams(vmem_limit_bytes=16 * 2**20),
            name="backward",
        )(early, pg, turned, stats)
        return latent_grad, scores

    in_specs = (
        P("member", "space", None),
        P(),
        P(),
        P(),
        P(),
        P("space", None),
        P("space"),
        P("space"),
    )
    out_specs = (P("member", "space", None), P())
    return jax.shard_map(shards, mesh=mesh, in_specs=in_specs, out_specs=out_specs, check_vma=False)
```

```python
import functools

import jax
import jax.numpy as jnp
from jax import lax
from jax.experimental import pallas as pl
from jax.experimental.pallas import tpu as pltpu
from jax.sharding import PartitionSpec as P

CELL_DEV = 32
COLS = 512
SLIM = 256
LANES = 128

epsilon = 1e-05
loss_scale = 4096.0
bf16, f32 = jnp.bfloat16, jnp.float32
MESH = pl.DeviceIdType.MESH


def in_hbm(value):
    return pltpu.with_memory_space_constraint(value, pltpu.HBM)


def dot_t(a, b):
    return lax.dot_general(a, b, (((1,), (1,)), ((), ())), preferred_element_type=f32)


def halves(value):
    high = value.astype(bf16).astype(f32)
    return high, value - high


def exchange(spaces, places, scaling, latent, w_in, b_in_far, w_out_far, b_out_far, target_far, area_far,
             cell_of_far,
             early, pg_out, turned, stats_out,
             b_in, w_out, b_out, target, area, cell_of, lat_buf, w_buf, slope_buf, act,
             psend, precv, p32, grad, gsend, grecv, hot, turned_hot, pcat, qsend, qrecv, csend, crecv,
             zsend, zrecv, mrecv, nrecv, dsend, drecv, up_buf, lmem, lspace,
             load_sem, small_sem, ps_sem, pr_sem, gs_sem, gr_sem, qs_sem, qr_sem, cs_sem, cr_sem,
             zs_sem, zr_sem, ms_sem, mr_sem, ns_sem, nr_sem, ds_sem, dr_sem, ls_sem, lr_sem, ts_sem, tr_sem):
    ms = lax.axis_index("space")
    mm = lax.axis_index("member")
    locals_, nodes, width = lat_buf.shape
    quarter = nodes // places
    units = w_buf.shape[1]
    variables = target.shape[0]
    members = locals_ * places
    rows = locals_ * quarter
    cells = CELL_DEV * spaces
    pair_scale = 1.0 / (members * (members - 1))

    def member_peer(o):
        return lax.rem(mm + o, places)

    def space_peer(o):
        return lax.rem(ms + o, spaces)

    def to_member(src, dst, ss, rs, o):
        return pltpu.make_async_remote_copy(
            src_ref=src, dst_ref=dst.at[mm], send_sem=ss, recv_sem=rs,
            device_id={"member": member_peer(o)}, device_id_type=MESH)

    def to_space(src, dst, ss, rs, o):
        return pltpu.make_async_remote_copy(
            src_ref=src, dst_ref=dst.at[ms], send_sem=ss, recv_sem=rs,
            device_id={"space": space_peer(o)}, device_id_type=MESH)

    def all_members(dst, ss, rs):
        part = dst.at[pl.ds(0, places - 1)]
        return pltpu.make_async_remote_copy(
            src_ref=part, dst_ref=part, send_sem=ss, recv_sem=rs,
            device_id={"member": member_peer(1)}, device_id_type=MESH)

    def all_spaces(dst, ss, rs):
        part = dst.at[pl.ds(0, spaces - 1)]
        return pltpu.make_async_remote_copy(
            src_ref=part, dst_ref=part, send_sem=ss, recv_sem=rs,
            device_id={"space": space_peer(1)}, device_id_type=MESH)

    def from_member(dst, ss, rs, o):
        peer = member_peer(o)
        return pltpu.make_async_remote_copy(
            src_ref=dst.at[peer], dst_ref=dst.at[peer], send_sem=ss, recv_sem=rs.at[peer],
            device_id={"member": peer}, device_id_type=MESH)

    def nodes_of(q):
        return pl.ds(pl.multiple_of(q * quarter, quarter), quarter)

    def load_chunk(j):
        return pltpu.make_async_copy(latent.at[j], lat_buf.at[j], load_sem.at[j])

    w_copy = pltpu.make_async_copy(w_in, w_buf, load_sem.at[locals_])
    small = [
        pltpu.make_async_copy(src, dst, small_sem.at[n])
        for n, (src, dst) in enumerate((
            (cell_of_far, cell_of), (area_far, area), (target_far, target),
            (b_in_far, b_in), (w_out_far, w_out.at[pl.ds(0, variables)]), (b_out_far, b_out)))
    ]
    for copy in small[:3]:
        copy.start()
    w_copy.start()
    load_chunk(0).start()
    for copy in small[3:]:
        copy.start()
    for j in range(1, locals_):
        load_chunk(j).start()
    barrier = pltpu.get_barrier_semaphore()
    for o in range(1, places):
        pl.semaphore_signal(barrier, inc=1, device_id={"member": member_peer(o)}, device_id_type=MESH)
    for o in range(1, spaces):
        pl.semaphore_signal(barrier, inc=1, device_id={"space": space_peer(o)}, device_id_type=MESH)

    for copy in small[:3]:
        copy.wait()
    spare = LANES - variables
    match = lax.broadcasted_iota(jnp.int32, (cells, nodes), 0) == cell_of[...]
    hot[...] = jnp.where(match, 1.0, 0.0).astype(bf16)
    row = lax.broadcasted_iota(jnp.int32, (spare, nodes), 0)
    t_high, t_low = halves(target[...])
    a_high, a_low = halves(area[...])
    firsts = jnp.where(row == 0, 1.0, jnp.where(row == 1, a_high, 0.0))
    seconds = jnp.where(row == 1, a_low, 0.0)
    sums = dot_t(hot[...], jnp.concatenate([t_high, firsts, t_low, seconds], axis=0).astype(bf16))
    sums = sums[:, :LANES] + sums[:, LANES:]
    lane = lax.broadcasted_iota(jnp.int32, (cells, LANES), 1)
    lows = pltpu.roll(halves(sums)[1], 2, 1)
    meta = jnp.where(lane < variables + 2, sums, lows)
    for n, value in enumerate(halves(jnp.sum(area[...], axis=1, keepdims=True))):
        meta = jnp.where(lane == variables + 4 + n, value, meta)
    for s in range(spaces):
        qsend[s] = meta[s * CELL_DEV:(s + 1) * CELL_DEV].astype(bf16)
    w_out[variables:, :] = jnp.zeros((spare, units), bf16)

    for copy in small[3:]:
        copy.wait()
    w_copy.wait()

    def forward(j, carry):
        load_chunk(j).wait()
        x = jnp.dot(lat_buf[j], w_buf[...], preferred_element_type=f32) + b_in[...]
        x = x.astype(bf16)
        slope_buf[j] = x
        x = x * 0.5
        act[...] = x * jnp.tanh(x) + x
        bias = jnp.concatenate([b_out[...], jnp.zeros((1, spare), f32)], axis=1)
        rounded = (dot_t(act[...], w_out[...]) + bias).astype(bf16)
        pcat[:, pl.ds(pl.multiple_of(j * LANES, LANES), LANES)] = rounded
        for q in range(places):
            psend[q, j] = rounded[q * quarter:(q + 1) * quarter].astype(f32).T[:variables].astype(bf16)

        @pl.when(j == 0)
        def _():
            pl.semaphore_wait(barrier, places + spaces - 2)

        for o in range(1, places):
            pltpu.make_async_remote_copy(
                src_ref=psend.at[member_peer(o), j], dst_ref=precv.at[mm, j], send_sem=ps_sem, recv_sem=pr_sem,
                device_id={"member": member_peer(o)}, device_id_type=MESH).start()

        @pl.when(j == 0)
        def _():
            for o in range(1, spaces):
                to_space(qsend.at[space_peer(o)], qrecv, qs_sem, qr_sem, o).start()

        return carry

    def spread(src, dst, ss, rs, lanes):
        sums = jnp.dot(hot[...], pcat[:, lanes], preferred_element_type=f32).astype(bf16)
        for s in range(spaces):
            src[s] = sums[s * CELL_DEV:(s + 1) * CELL_DEV]
        for o in range(1, spaces):
            to_space(src.at[space_peer(o)], dst, ss, rs, o).start()

    ahead = (locals_ - 1) * LANES
    lax.fori_loop(0, locals_ - 1, forward, 0)
    spread(csend, crecv, cs_sem, cr_sem, slice(0, ahead))
    forward(locals_ - 1, 0)
    spread(zsend, zrecv, zs_sem, zr_sem, slice(ahead, ahead + LANES))

    qrecv[ms] = qsend[ms]
    all_spaces(qrecv, qs_sem, qr_sem).wait_recv()
    meta = qrecv[0].astype(f32)
    for s in range(1, spaces):
        meta = meta + qrecv[s].astype(f32)
    cell_count = meta[:, variables:variables + 1] + meta[:, variables + 2:variables + 3]
    cell_area = meta[:, variables + 1:variables + 2] + meta[:, variables + 3:variables + 4]
    all_area = meta[0:1, variables + 4:variables + 5] + meta[0:1, variables + 5:variables + 6]
    divisor = jnp.maximum(cell_count, 1.0)
    cell_lane = lax.broadcasted_iota(jnp.int32, (CELL_DEV, LANES), 1)
    facts = jnp.where(cell_lane < variables, meta / divisor, jnp.where(cell_lane == variables, divisor, cell_area))
    facts = jnp.concatenate([facts] * locals_, axis=0).T
    cell_target = facts[:variables]
    lane_divisor = facts[variables:variables + 1]
    cell_weight = facts[variables + 1:variables + 2]

    def slopes(n, carry):
        j, at = lax.div(n, units // SLIM), pl.ds(pl.multiple_of(lax.rem(n, units // SLIM) * SLIM, SLIM), SLIM)
        x = slope_buf[j, :, at].astype(f32)
        s = 0.5 * jnp.tanh(0.5 * x) + 0.5
        slope_buf[j, :, at] = (s + x * s * (1.0 - s)).astype(bf16)
        return carry

    def average(src, near, far, means_buf, ss, rs):
        near[ms] = src[ms]
        far.wait_recv()
        total = near[0].astype(f32)
        for s in range(1, spaces):
            total = total + near[s].astype(f32)
        means_buf[mm] = (total / divisor).astype(bf16)
        for o in range(1, places):
            to_member(means_buf.at[mm], means_buf, ss, rs, o).start()

    average(csend, crecv, all_spaces(crecv, cs_sem, cr_sem), mrecv, ms_sem, mr_sem)
    def turn(n, carry):
        at = pl.ds(pl.multiple_of(n * COLS, COLS), COLS)
        turned[:, at] = w_buf[at, :].T
        return carry

    lax.fori_loop(0, width // COLS, turn, 0)
    for q in range(places):
        at = slice(q * quarter, (q + 1) * quarter)
        turned_hot[at, :] = hot[:, at].astype(f32).T.astype(bf16)

    average(zsend, zrecv, all_spaces(zrecv, zs_sem, zr_sem), nrecv, ns_sem, nr_sem)

    def members_of(place):
        parts = [mrecv[place, :, j * LANES:(j + 1) * LANES] for j in range(locals_ - 1)] + [nrecv[place]]
        return jnp.concatenate(parts, axis=0).astype(f32).T[:variables]

    precv[mm] = psend[mm]
    truths = target[:, nodes_of(mm)]
    weight = area[:, nodes_of(mm)]
    all_members(precv, ps_sem, pr_sem).wait_recv()

    def truth_step(m, total):
        p = precv[lax.div(m, locals_), lax.rem(m, locals_)].astype(f32)
        p32[m] = p
        d = p - truths
        sq = jnp.sum(d * d, axis=0, keepdims=True) * (1.0 / variables) + epsilon
        r = lax.rsqrt(sq)
        grad[m] = d * (r * (1.0 / members))
        return total + sq * r

    def pair_step(m, total):
        pm = p32[m]
        factors = []
        for r in range(1, members // 2 + 1):
            share = 0.5 if 2 * r == members else 1.0
            d = pm - p32[lax.rem(m + r, members)]
            sq = jnp.sum(d * d, axis=0, keepdims=True) * (1.0 / variables) + epsilon
            inv = lax.rsqrt(sq)
            total = total + share * (sq * inv)
            factors.append(inv * (share * pair_scale))
        mine = grad[m]
        for r in range(1, members // 2 + 1):
            k = lax.rem(m + r, members)
            part = (pm - p32[k]) * factors[r - 1]
            mine = mine - part
            grad[k] = grad[k] + part
        grad[m] = mine
        return total

    zero = jnp.zeros((1, quarter), f32)
    truth_total = lax.fori_loop(0, members, truth_step, zero)
    pair_total = lax.fori_loop(0, members, pair_step, zero)
    fine_loss = weight * (truth_total * (1.0 / members) - pair_total * pair_scale)
    scale = weight * (1.0 / variables)

    def send_grads(o):
        peer = member_peer(o)
        for j in range(locals_):
            gsend[peer, j] = (grad[peer * locals_ + j] * scale).astype(bf16)
        to_member(gsend.at[peer], grecv, gs_sem, gr_sem.at[mm], o).start()

    send_grads(1)
    for j in range(locals_):
        grecv[mm, j] = (grad[mm * locals_ + j] * scale).astype(bf16)

    for o in range(2, places):
        send_grads(o)

    own = members_of(mm)
    all_members(mrecv, ms_sem, mr_sem).wait_recv()
    all_members(nrecv, ns_sem, nr_sem).wait_recv()
    d = own - cell_target
    sq = jnp.sum(d * d, axis=0, keepdims=True) * (1.0 / variables) + epsilon
    inv = lax.rsqrt(sq)
    coarse = d * (inv * (1.0 / members))
    coarse_dist = sq * inv * (1.0 / members)
    for o in range(places):
        theirs = members_of(member_peer(o)) if o else own
        for r in range(locals_):
            if o == 0 and r == 0:
                continue
            d = own - (pltpu.roll(theirs, r * CELL_DEV, 1) if r else theirs)
            sq = jnp.sum(d * d, axis=0, keepdims=True) * (1.0 / variables) + epsilon
            inv = lax.rsqrt(sq)
            coarse = coarse - d * (inv * pair_scale)
            coarse_dist = coarse_dist - sq * inv * (0.5 * pair_scale)
    per_cell = coarse * (cell_weight * (1.0 / variables)) / lane_divisor
    per_cell = jnp.concatenate([per_cell, jnp.zeros((spare, locals_ * CELL_DEV), f32)], axis=0).T.astype(bf16)
    for j in range(locals_):
        dsend[:, j * LANES:(j + 1) * LANES] = per_cell[j * CELL_DEV:(j + 1) * CELL_DEV]
    for o in range(1, spaces):
        to_space(dsend, drecv, ds_sem, dr_sem, o).start()
    drecv[ms] = dsend[...]
    coarse_loss = jnp.sum(cell_weight * coarse_dist, axis=1, keepdims=True)

    row = lax.broadcasted_iota(jnp.int32, (8, LANES), 0)
    lspace[ms] = jnp.where(row == 0, jnp.sum(fine_loss, axis=1, keepdims=True), coarse_loss)
    for o in range(1, spaces):
        to_space(lspace.at[ms], lspace, ts_sem, tr_sem, o).start()
    lax.fori_loop(0, locals_ * (units // SLIM), slopes, 0)

    all_spaces(drecv, ds_sem, dr_sem).wait_recv()
    factor = scaling / all_area

    def upstream(i):
        q = lax.rem(mm + 1 + i, places)
        pieces = drecv[...].reshape(cells, locals_ * LANES)
        coarse_part = jnp.dot(turned_hot[nodes_of(q), :], pieces, preferred_element_type=f32)
        blank = jnp.zeros((spare, quarter), f32)
        for j in range(locals_):
            fine = jnp.concatenate([grecv[q, j].astype(f32), blank], axis=0).T
            up_buf[j * quarter:(j + 1) * quarter, :] = (
                fine + coarse_part[:, j * LANES:(j + 1) * LANES]).astype(bf16)

    def hidden_to(pg, i):
        h = jnp.dot(up_buf[...], w_out[...], preferred_element_type=f32)
        slope = slope_buf[:, nodes_of(lax.rem(mm + 1 + i, places)), :].reshape(rows, units)
        pg[...] = (h * slope.astype(f32)).astype(bf16)

    def finish(i):
        upstream(i)
        hidden_to(act, i)
        g = jnp.dot(act[...], turned[...], preferred_element_type=f32)
        early[i - 1] = (g * factor).astype(bf16).reshape(locals_, quarter, width)

    finish(places - 1)
    all_spaces(lspace, ts_sem, tr_sem).wait_recv()
    loss = lspace[0]
    for s in range(1, spaces):
        loss = loss + lspace[s]
    lmem[mm] = loss
    for o in range(1, places):
        to_member(lmem.at[mm], lmem, ls_sem, lr_sem, o).start()

    def arrived(n, carry):
        i = places - 2 - n
        from_member(grecv, gs_sem, gr_sem, i + 1).wait_recv()
        finish(i)
        return carry

    lax.fori_loop(0, places - 2, arrived, 0)
    from_member(grecv, gs_sem, gr_sem, 1).wait_recv()
    upstream(0)
    hidden_to(pg_out, 0)

    all_members(lmem, ls_sem, lr_sem).wait_recv()
    loss = lmem[0]
    for m in range(1, places):
        loss = loss + lmem[m]
    stats_out[...] = jnp.where(row == 2, all_area, loss)

    all_members(psend, ps_sem, pr_sem).wait_send()
    all_members(mrecv, ms_sem, mr_sem).wait_send()
    all_members(nrecv, ns_sem, nr_sem).wait_send()
    all_members(gsend, gs_sem, gr_sem.at[mm]).wait_send()
    all_members(lmem, ls_sem, lr_sem).wait_send()
    all_spaces(qsend, qs_sem, qr_sem).wait_send()
    all_spaces(csend, cs_sem, cr_sem).wait_send()
    all_spaces(zsend, zs_sem, zr_sem).wait_send()
    all_spaces(drecv, ds_sem, dr_sem).wait_send()
    all_spaces(lspace, ts_sem, tr_sem).wait_send()


def backward(places, scaling, early, pg, turned, stats, latent_grad, scores_out, last, scores, store_sem):
    locals_, quarter, width = last.shape
    mm = lax.axis_index("member")

    def nodes_of(i):
        q = lax.rem(mm + 1 + i, places)
        return pl.ds(pl.multiple_of(q * quarter, quarter), quarter)

    def store(i):
        return pltpu.make_async_copy(early.at[i - 1], latent_grad.at[:, nodes_of(i), :], store_sem.at[i - 1])

    def store_last(n):
        at = pl.ds(pl.multiple_of(n * COLS, COLS), COLS)
        return pltpu.make_async_copy(
            last.at[:, :, at], latent_grad.at[:, nodes_of(0), at], store_sem.at[places - 1 + n])

    for i in range(1, places):
        store(i).start()
    all_area = stats[2:3, 0:1]
    factor = scaling / all_area
    both = stats[...] / all_area
    scores[0] = both[0, 0]
    scores[1] = both[1, 0]
    score_copy = pltpu.make_async_copy(scores, scores_out, store_sem.at[places - 1 + width // COLS])
    score_copy.start()

    def outputs(n, carry):
        at = pl.ds(pl.multiple_of(n * COLS, COLS), COLS)
        g = jnp.dot(pg[...], turned[:, at], preferred_element_type=f32)
        last[:, :, at] = (g * factor).astype(bf16).reshape(locals_, quarter, COLS)
        store_last(n).start()
        return carry

    lax.fori_loop(0, width // COLS, outputs, 0)
    score_copy.wait()
    for i in range(1, places):
        store(i).wait()
    for n in range(width // COLS):
        store_last(n).wait()


def solution(mesh):
    spaces, places = mesh.shape["space"], mesh.shape["member"]

    def shards(latent, w_in, b_in, w_out, b_out, target, area, cell_of):
        locals_, nodes, width = latent.shape
        units, variables = w_out.shape
        quarter = nodes // places
        cells = CELL_DEV * spaces
        members = locals_ * places
        anywhere = pl.BlockSpec(memory_space=pl.ANY)
        inside = pl.BlockSpec(memory_space=pltpu.VMEM)
        single = pltpu.SemaphoreType.DMA
        rows = locals_ * quarter
        scaling = loss_scale * (nodes * spaces)
        early, pg, turned, stats = pl.pallas_call(
            functools.partial(exchange, spaces, places, scaling),
            out_shape=(
                pltpu.VMEM((places - 1, locals_, quarter, width), bf16),
                pltpu.VMEM((rows, units), bf16),
                pltpu.VMEM((units, width), bf16),
                pltpu.VMEM((8, LANES), f32),
            ),
            in_specs=[anywhere] * 8,
            out_specs=(inside, inside, inside, inside),
            scratch_shapes=[
                pltpu.VMEM((1, units), f32),
                pltpu.VMEM((LANES, units), bf16),
                pltpu.VMEM((1, variables), f32),
                pltpu.VMEM((variables, nodes), f32),
                pltpu.VMEM((1, nodes), f32),
                pltpu.VMEM((1, nodes), jnp.int32),
                pltpu.VMEM((locals_, nodes, width), bf16),
                pltpu.VMEM((width, units), bf16),
                pltpu.VMEM((locals_, nodes, units), bf16),
                pltpu.VMEM((rows, units), bf16),
                pltpu.VMEM((places, locals_, variables, quarter), bf16),
                pltpu.VMEM((places, locals_, variables, quarter), bf16),
                pltpu.VMEM((members, variables, quarter), f32),
                pltpu.VMEM((members, variables, quarter), f32),
                pltpu.VMEM((places, locals_, variables, quarter), bf16),
                pltpu.VMEM((places, locals_, variables, quarter), bf16),
                pltpu.VMEM((cells, nodes), bf16),
                pltpu.VMEM((nodes, cells), bf16),
                pltpu.VMEM((nodes, locals_ * LANES), bf16),
                pltpu.VMEM((spaces, CELL_DEV, LANES), bf16),
                pltpu.VMEM((spaces, CELL_DEV, LANES), bf16),
                pltpu.VMEM((spaces, CELL_DEV, (locals_ - 1) * LANES), bf16),
                pltpu.VMEM((spaces, CELL_DEV, (locals_ - 1) * LANES), bf16),
                pltpu.VMEM((spaces, CELL_DEV, LANES), bf16),
                pltpu.VMEM((spaces, CELL_DEV, LANES), bf16),
                pltpu.VMEM((places, CELL_DEV, (locals_ - 1) * LANES), bf16),
                pltpu.VMEM((places, CELL_DEV, LANES), bf16),
                pltpu.VMEM((CELL_DEV, locals_ * LANES), bf16),
                pltpu.VMEM((spaces, CELL_DEV, locals_ * LANES), bf16),
                pltpu.VMEM((rows, LANES), bf16),
                pltpu.VMEM((places, 8, LANES), f32),
                pltpu.VMEM((spaces, 8, LANES), f32),
                pltpu.SemaphoreType.DMA((locals_ + 1,)),
                pltpu.SemaphoreType.DMA((6,)),
                single, single, single, pltpu.SemaphoreType.DMA((places,)),
            ]
            + [single] * 16,
            compiler_params=pltpu.CompilerParams(
                collective_id=0, has_side_effects=True, vmem_limit_bytes=36 * 2**20
            ),
            name="exchange",
        )(*map(in_hbm, (latent, w_in, b_in[None], w_out.T, b_out[None], target.T, area[None], cell_of[None])))

        latent_grad, scores = pl.pallas_call(
            functools.partial(backward, places, scaling),
            out_shape=(
                jax.ShapeDtypeStruct((locals_, nodes, width), bf16),
                jax.ShapeDtypeStruct((2,), f32),
            ),
            in_specs=[inside] * 4,
            out_specs=(anywhere, anywhere),
            scratch_shapes=[
                pltpu.VMEM((locals_, quarter, width), bf16),
                pltpu.SMEM((2,), f32),
                pltpu.SemaphoreType.DMA((places + width // COLS,)),
            ],
            compiler_params=pltpu.CompilerParams(vmem_limit_bytes=16 * 2**20),
            name="backward",
        )(early, pg, turned, stats)
        return latent_grad, scores

    in_specs = (
        P("member", "space", None),
        P(),
        P(),
        P(),
        P(),
        P("space", None),
        P("space"),
        P("space"),
    )
    out_specs = (P("member", "space", None), P())
    return jax.shard_map(shards, mesh=mesh, in_specs=in_specs, out_specs=out_specs, check_vma=False)
```
